32 devices in a mesh: dp: 4 (over y, x), expert: 4 (over z), tensor: 2 (over core).
Axes of the slice: x: 2, y: 2, z: 4, core: 2. Of those that a mesh axis runs over, the one named last changes fastest.
Arguments:
- block_input: bfloat16 [2048, 2048], P(('dp', 'expert')), may hold values from -24 to 24
- attn_gain: bfloat16 [2048], P(('dp', 'expert')), may hold values from 0.5 to 1.5
- query_weight: bfloat16 [2048, 2048], P(('dp', 'expert'), 'tensor'), may hold values from -1 to 1
- key_weight: bfloat16 [2048, 2048], P(('dp', 'expert'), 'tensor'), may hold values from -16 to 16
- value_weight: bfloat16 [2048, 2048], P(('dp', 'expert'), 'tensor'), may hold values from -0.125 to 0.125
- output_weight: bfloat16 [2048, 2048], P('tensor', ('dp', 'expert')), may hold values from -0.75 to 0.75
- ffn_gain: bfloat16 [2048], P(('dp', 'expert')), may hold values from 0.5 to 1.5
- router_weight: bfloat16 [2048, 16], P(('dp', 'expert')), may hold values from -8 to 8
- expert_gate: bfloat16 [16, 2048, 1408], P('expert', 'dp', 'tensor'), may hold values from -0.125 to 0.125
- expert_up: bfloat16 [16, 2048, 1408], P('expert', 'dp', 'tensor'), may hold values from -0.125 to 0.125
- expert_down: bfloat16 [16, 1408, 2048], P('expert', 'tensor', 'dp'), may hold values from -1.25 to 1.25
- shared_gate: bfloat16 [2048, 2816], P(('dp', 'expert'), 'tensor'), may hold values from -0.125 to 0.125
- shared_up: bfloat16 [2048, 2816], P(('dp', 'expert'), 'tensor'), may hold values from -0.125 to 0.125
- shared_down: bfloat16 [2816, 2048], P('tensor', ('dp', 'expert')), may hold values from -0.109375 to 0.109375
- segments: int32 [16, 128], P(('dp', 'expert')), may hold values from 0 to 2, never falling along the last dimension, each value on 1 to 64 neighbouring positions
- routes: int32 [2048, 6], P(('dp', 'expert')), may hold values from 0 to 15, all different within a row; in each aligned block of 128 rows (0 to 127, 128 to 255, ...) at most 96 rows name the same one
- cotangent: bfloat16 [2048, 2048], P(('dp', 'expert')), may hold values from -6 to 6
Outputs:
- block_output: bfloat16 [2048, 2048], P(('dp', 'expert'))
- input_grad: float32 [2048, 2048], P(('dp', 'expert'))
- attn_gain_grad: float32 [2048], P(('dp', 'expert'))
- query_grad: float32 [2048, 2048], P(('dp', 'expert'), 'tensor')
- key_grad: float32 [2048, 2048], P(('dp', 'expert'), 'tensor')
- value_grad: float32 [2048, 2048], P(('dp', 'expert'), 'tensor')
- output_grad: float32 [2048, 2048], P('tensor', ('dp', 'expert'))
- ffn_gain_grad: float32 [2048], P(('dp', 'expert'))
- router_grad: float32 [2048, 16], P(('dp', 'expert'))
- expert_gate_grad: float32 [16, 2048, 1408], P('expert', 'dp', 'tensor')
- expert_up_grad: float32 [16, 2048, 1408], P('expert', 'dp', 'tensor')
- expert_down_grad: float32 [16, 1408, 2048], P('expert', 'tensor', 'dp')
- shared_gate_grad: float32 [2048, 2816], P(('dp', 'expert'), 'tensor')
- shared_up_grad: float32 [2048, 2816], P(('dp', 'expert'), 'tensor')
- shared_down_grad: float32 [2816, 2048], P('tensor', ('dp', 'expert'))
The draws below stay inside these ranges and needn't reach their ends.
Inputs may be any that keep to these rules, and one draw needn't show every extreme that they name: `segments`: within each row the numbers never fall; each document holds 1 to 64 positions, one exactly 64. `routes`: each token names 6 different experts; among the 128 rows of one device no expert is named by more than 96 rows, a bound that some block reaches.
All inputs are finite; a program needn't handle non-finite values.
Results may differ from the reference program's by a relative error of at most 0.019.
The reference program's roundings to bfloat16 on the way count: a program that leaves them out, or rounds other values in their place, can miss the bound.
Values may be sent and summed in bfloat16 or wider, within the bound.
A program may use at most 320 MiB of HBM per device.

```python
import math
import jax
import jax.numpy as jnp
import numpy as np
from jax import lax

D = 2048
HEADS = 16
HD = 128
FFE = 1408
TOPK = 6
SEQ = 128
FS = 2816
EXPERTS = 16
NSEQ = 16
TOKENS = 2048
CAP = 96
N_DP = 4
N_EXPERT = 4
N_TENSOR = 2


def query_base(key):
    return jax.random.normal(jax.random.fold_in(key, 21), (D, D), jnp.float32) / math.sqrt(D)


def draw_block_input(key, part):
    drawn = jax.random.normal(jax.random.fold_in(key, 50), (TOKENS, D), jnp.float32)
    return jnp.clip(drawn, -6.0, 6.0).astype(jnp.bfloat16)


def draw_query_weight(key, part):
    bound = 4.0 / math.sqrt(D)
    return jnp.clip(query_base(key), -bound, bound).astype(jnp.bfloat16)


def draw_key_weight(key, part):
    own = jax.random.normal(jax.random.fold_in(key, 22), (D, D), jnp.float32) / math.sqrt(D)
    return jnp.clip(own, -16.0, 16.0).astype(jnp.bfloat16)


def draw_router_weight(key, part):
    own = jax.random.normal(jax.random.fold_in(key, 31), (D, EXPERTS), jnp.float32) / math.sqrt(D)
    return jnp.clip(own, -8.0, 8.0).astype(jnp.bfloat16)


def raised(array, own_key, source, target, parts, factor):
    owner, partner = [(jnp.arange(array.shape[dim]) // (array.shape[dim] // parts)).reshape([-1 if axis == dim else 1 for axis in range(array.ndim)]) for dim in (source, target)]
    chosen = jax.random.permutation(own_key, parts)[partner]
    strong = (owner == chosen) | (owner == (partner + parts // 2) % parts)
    return jnp.where(strong, factor * array, array)


def level_of(rng, dims, cuts, low, top_value):
    loudness = 1.0
    for dim, blocks in cuts:
        heights = jax.random.uniform(jax.random.fold_in(jax.random.fold_in(rng, 6), dim), (blocks,), jnp.float32, low / len(cuts), top_value / len(cuts))
        loudness = loudness * jnp.repeat(jnp.exp(heights), dims[dim] // blocks).reshape((-1,) + (1,) * (len(dims) - 1 - dim))
    return loudness


def profile(number_of, total, reach, lean):
    portions = [(1 << 20) // math.isqrt(grade ** lean) + 1 for grade in range(2, number_of + 1)]
    rest, given = total - reach - (number_of - 1), [1] * (number_of - 1)
    while rest > 0:
        movable = [i for i in range(number_of - 1) if given[i] < reach]
        pool, remaining = sum([portions[i] for i in movable]), rest
        for i in movable:
            addition = min(reach - given[i], max(1, remaining * portions[i] // pool), rest)
            given[i] = given[i] + addition
            rest = rest - addition
    return np.array([reach] + given)


def ragged_sizes(own_key, number_of, total, reach, skew):
    if number_of == 2:
        one = jax.random.randint(own_key, (), max(1, total - reach), min(reach, total - 1) + 1)
        return jnp.stack([one, total - one])
    tallies = jnp.asarray(profile(number_of, total, reach, skew), jnp.int32)
    twos = (number_of - 1) // 2
    source_of, taker = tallies[1:1 + 2 * twos:2], tallies[2:2 + 2 * twos:2]
    room = jnp.minimum(source_of - 1, reach - taker)
    shifted = jax.random.randint(jax.random.fold_in(own_key, 1), (twos,), 0, 1 << 20) % (room + 1)
    tallies = tallies.at[1:1 + 2 * twos:2].set(source_of - shifted).at[2:2 + 2 * twos:2].set(taker + shifted)
    return tallies[jax.random.permutation(jax.random.fold_in(own_key, 2), number_of)]


def assign_block(key, own, number, rows, amount, top, most, lean):
    order = jax.random.permutation(key, amount)
    packed, ordinary = shares(amount, rows * top, most, lean, True), shares(amount, rows * top, most, lean, False)
    places = jnp.arange(amount)

    def named(lengths, offset_by):
        used = int((lengths > 0).sum())
        fixed = max(1, used // 4)
        passed = fixed + (places - fixed + offset_by * (used - fixed)) % max(1, amount - fixed)
        return jnp.zeros((amount,), jnp.int32).at[order[jnp.where(places < fixed, places, passed)]].set(jnp.asarray(lengths, jnp.int32))

    lengths = jnp.where(number % 4 == 0, named(packed, number // 4), named(ordinary, number - number // 4 - 1))
    mixed = jax.random.permutation(jax.random.fold_in(own, 3), amount)
    source_of, taker = mixed[0:amount // 2 * 2:2], mixed[1:amount // 2 * 2:2]
    room = jnp.minimum(lengths[source_of] - 1, most - lengths[taker]) // 2
    room = jnp.where((source_of == order[0]) | (taker == order[0]) | (lengths[taker] == 0), 0, jnp.maximum(room, 0))
    passed = jax.random.randint(jax.random.fold_in(own, 4), (amount // 2,), 0, 1 << 20) % (room + 1)
    lengths = lengths.at[source_of].add(-passed).at[taker].add(passed)
    members = jnp.searchsorted(jnp.cumsum(lengths), jnp.arange(rows * top), side="right").astype(jnp.int32)
    listing = members.reshape(top, rows).T
    listing = listing[jax.random.permutation(jax.random.fold_in(own, 1), rows)]
    offset_by = jax.random.randint(jax.random.fold_in(own, 2), (rows, 1), 0, top)
    return jnp.take_along_axis(listing, (jnp.arange(top)[None, :] + offset_by) % top, axis=1)


def shares(amount, total, most, lean, full):
    portions = [(1 << 20) // math.isqrt(rank ** lean) + 1 for rank in range(1, amount + 1)]
    largest = most if full else min(most, max(-(-total // amount), total * portions[0] // sum(portions)))
    least = 1 if total - largest >= amount - 1 else 0
    given, rest = [largest] + [least] * (amount - 1), total - largest - least * (amount - 1)
    while rest > 0:
        free = [i for i in range(1, amount) if given[i] < largest] or [i for i in range(1, amount) if given[i] < most]
        whole, remaining = sum([portions[i] for i in free]), rest
        for i in free:
            more = min(most - given[i], max(1, remaining * portions[i] // whole), rest)
            given[i] = given[i] + more
            rest = rest - more
    return np.array(given)


def centred(own_key, shape, scale, reach, split=(), kind=jnp.bfloat16):
    loudness = level_of(own_key, shape, split, -0.22, 0.18) if split else 1.0
    values = jax.random.normal(own_key, shape, jnp.float32) * scale * loudness
    return jnp.minimum(jnp.maximum(values, -reach), reach).astype(kind)


def noise_with(rng, dims, scale, most, shards, heavy, held_as=jnp.bfloat16):
    entries = scale * jax.random.normal(rng, dims, jnp.float32)
    if shards:
        entries = entries * level_of(rng, dims, shards, -0.22, 0.18)
    return jnp.clip(raised(entries, jax.random.fold_in(rng, 3), *heavy), -most, most).astype(held_as)


def setup_inputs(seed: int = 0) -> dict:
    seeds = jax.random.split(jax.random.key(seed), 18)
    block_input = draw_block_input(jax.random.fold_in(seeds[17], 71), 0)
    attn_gain = jnp.clip(1.0 + 0.1 * jax.random.normal(seeds[1], (D,), jnp.float32), 0.5, 1.5).astype(jnp.bfloat16)
    query_weight = draw_query_weight(jax.random.fold_in(seeds[17], 71), 0)
    key_weight = draw_key_weight(jax.random.fold_in(seeds[17], 71), 0)
    value_weight = centred(seeds[4], (D, D), D ** -0.5, 0.125, ((0, 16), (1, 2)))
    output_weight = centred(seeds[5], (D, D), (D // 32) ** -0.5, 0.75, ((0, 2), (1, 16)))
    ffn_gain = jnp.clip(1.0 + 0.1 * jax.random.normal(seeds[6], (D,), jnp.float32), 0.5, 1.5).astype(jnp.bfloat16)
    router_weight = draw_router_weight(jax.random.fold_in(seeds[17], 71), 0)
    expert_gate = centred(seeds[8], (EXPERTS, D, FFE), D ** -0.5, 0.125, ((0, 4), (1, 4), (2, 2)))
    expert_up = centred(seeds[9], (EXPERTS, D, FFE), D ** -0.5, 0.125, ((0, 4), (1, 4), (2, 2)))
    expert_down = centred(seeds[10], (EXPERTS, FFE, D), (max(FFE // 64, 1)) ** -0.5, 1.25, ((0, 4), (1, 2), (2, 4)))
    shared_gate = centred(seeds[11], (D, FS), D ** -0.5, 0.125, ((0, 16), (1, 2)))
    shared_up = centred(seeds[12], (D, FS), D ** -0.5, 0.125, ((0, 16), (1, 2)))
    shared_down = centred(seeds[13], (FS, D), FS ** -0.5, 0.109375, ((0, 2), (1, 16)))
    segments = jax.vmap(lambda own: jnp.searchsorted(jnp.cumsum(ragged_sizes(own, 3, SEQ, SEQ // 2, 0)), jnp.arange(SEQ), side="right"))(jax.random.split(seeds[14], NSEQ)).reshape((NSEQ, SEQ)).astype(jnp.int32)
    routes_keys = jax.random.split(jax.random.fold_in(seeds[15], 1), TOKENS // SEQ)
    routes_turns = jax.random.permutation(jax.random.fold_in(seeds[15], 3), TOKENS // SEQ)
    routes = jax.vmap(lambda own, number: assign_block(jax.random.fold_in(seeds[15], 2), own, number, SEQ, EXPERTS, TOPK, CAP, 2))(routes_keys, routes_turns).reshape((TOKENS, TOPK))
    cotangent = noise_with(seeds[16], (TOKENS, D), 1.0, 6.0, ((0, 16),), (0, 1, 16, 2.0))
    return dict(block_input=block_input, attn_gain=attn_gain, query_weight=query_weight, key_weight=key_weight, value_weight=value_weight, output_weight=output_weight, ffn_gain=ffn_gain, router_weight=router_weight, expert_gate=expert_gate, expert_up=expert_up, expert_down=expert_down, shared_gate=shared_gate, shared_up=shared_up, shared_down=shared_down, segments=segments, routes=routes, cotangent=cotangent)


epsilon = 1e-06
rope_base = 10000.0
masked_score = -1e+30

@jax.custom_vjp
def low(v):
    return lax.optimization_barrier(v.astype(jnp.bfloat16)).astype(jnp.float32)

@jax.custom_vjp
def low_back(v):
    return v

def low_keep(v):
    return (low(v), None)

def low_pass(kept, grad):
    return (grad,)

def back_keep(v):
    return (v, None)

def back_low(kept, grad):
    return (low(grad),)
low.defvjp(low_keep, low_pass)
low_back.defvjp(back_keep, back_low)

def matmul(left, right):
    return jnp.dot(left, right, preferred_element_type=jnp.float32, precision=lax.Precision.HIGHEST)

def rms_scale(vector):
    return lax.rsqrt(lax.optimization_barrier(jnp.mean(vector * vector, axis=-1, keepdims=True)) + epsilon)

def rope_tables(positions, width):
    half_width = width // 2
    frequency = rope_base ** (-jnp.arange(half_width, dtype=jnp.float32) / half_width)
    angles = positions[:, None] * frequency[None, :]
    return (jnp.cos(angles)[:, None, :], jnp.sin(angles)[:, None, :])

def rotate(vector, cosine, sine_table):
    half_width = vector.shape[-1] // 2
    first_half = vector[..., :half_width]
    second_half = vector[..., half_width:]
    return jnp.concatenate([first_half * cosine - second_half * sine_table, first_half * sine_table + second_half * cosine], axis=-1)

def attend(block_data):
    query_rot, key_rot, value_rows, segment_ids = block_data
    scores = jnp.einsum('bqhd,bkhd->bhqk', query_rot, key_rot, precision=lax.Precision.HIGHEST) / math.sqrt(HD)
    scores = low_back(scores)
    position = jnp.arange(SEQ)
    causal = (position[:, None] >= position[None, :])[None, None]
    allowed = causal & (segment_ids[:, None, :, None] == segment_ids[:, None, None, :])
    scores = jnp.where(allowed, scores, masked_score)
    prob_rows = jax.nn.softmax(scores, axis=-1)
    mixed_rows = jnp.einsum('bhqk,bkhd->bqhd', low(prob_rows), value_rows, precision=lax.Precision.HIGHEST)
    return low(low_back(mixed_rows))

def expert(block_data):
    gathered, gate_weight, up_weight, down_weight = block_data
    gate_pre = low_back(matmul(gathered, gate_weight))
    up_pre = low_back(matmul(gathered, up_weight))
    act_rows = low(jax.nn.silu(gate_pre) * up_pre)
    piece_width = FFE // N_TENSOR
    pieces = jnp.einsum('rjf,jfd->jrd', act_rows.reshape(-1, N_TENSOR, piece_width), down_weight.reshape(N_TENSOR, piece_width, D), precision=lax.Precision.HIGHEST)
    return lax.optimization_barrier(jnp.sum(low(low_back(pieces)), axis=0))

def forward_layer(input_f, attn_gain, query_weight, key_weight, value_weight, output_weight, ffn_gain, router_weight, expert_gate, expert_up, expert_down, shared_gate, shared_up, shared_down, segments, routes):
    scale_one = rms_scale(input_f)
    normed_one = low(input_f * scale_one * attn_gain)
    positions = (jnp.arange(TOKENS) % SEQ).astype(jnp.float32)
    cosine, sine_table = rope_tables(positions, HD)
    query_pre = low_back(matmul(normed_one, query_weight)).reshape(TOKENS, HEADS, HD)
    key_pre = low_back(matmul(normed_one, key_weight)).reshape(TOKENS, HEADS, HD)
    value_pre = low_back(matmul(normed_one, value_weight)).reshape(TOKENS, HEADS, HD)
    query_rot = low(rotate(query_pre, cosine, sine_table))
    key_rot = low(rotate(key_pre, cosine, sine_table))
    value_rows = low(value_pre)
    group_size = math.gcd(NSEQ, max(1, 4096 // SEQ))

    def grouped(stacked):
        return stacked.reshape((NSEQ // group_size, group_size, SEQ) + stacked.shape[1:])
    segment_ids = segments.reshape(NSEQ // group_size, group_size, SEQ)
    mixed_rows = lax.map(jax.checkpoint(attend), (grouped(query_rot), grouped(key_rot), grouped(value_rows), segment_ids))
    mixed_rows = mixed_rows.reshape(TOKENS, HEADS * HD)
    attn_out = low_back(matmul(mixed_rows, output_weight))
    hidden_one = input_f + attn_out
    scale_two = rms_scale(hidden_one)
    normed_two = low(hidden_one * scale_two * ffn_gain)
    logits = low_back(matmul(normed_two, router_weight))
    router_probs = jax.nn.softmax(logits, axis=-1)
    gate_probs = jnp.take_along_axis(router_probs, routes, axis=1)
    room_rows = N_DP * N_EXPERT * CAP
    expert_ids = jnp.arange(EXPERTS, dtype=jnp.int32)
    per_token = lax.optimization_barrier(jnp.sum((routes[:, :, None] == expert_ids[None, None, :]).astype(jnp.int32), axis=1))
    rank_table = jnp.cumsum(per_token, axis=0) - 1
    position_of = jnp.take_along_axis(rank_table, routes, axis=1).astype(jnp.int32)
    token_ids = jnp.broadcast_to(jnp.arange(TOKENS, dtype=jnp.int32)[:, None], (TOKENS, TOPK))
    row_table = jnp.zeros((EXPERTS, room_rows), jnp.int32).at[routes, position_of].set(token_ids)
    gathered = normed_two[row_table]
    expert_out = lax.map(jax.checkpoint(expert), (gathered, expert_gate, expert_up, expert_down))
    picked = expert_out[routes, position_of]
    routed = lax.optimization_barrier(jnp.sum(gate_probs[:, :, None] * picked, axis=1))
    shared_gpre = low_back(matmul(normed_two, shared_gate))
    shared_upre = low_back(matmul(normed_two, shared_up))
    shared_act = low(jax.nn.silu(shared_gpre) * shared_upre)
    shared_out = low_back(matmul(shared_act, shared_down))
    return hidden_one + shared_out + routed

def reference(block_input, attn_gain, query_weight, key_weight, value_weight, output_weight, ffn_gain, router_weight, expert_gate, expert_up, expert_down, shared_gate, shared_up, shared_down, segments, routes, cotangent):
    floats = tuple((weight_in.astype(jnp.float32) for weight_in in (block_input, attn_gain, query_weight, key_weight, value_weight, output_weight, ffn_gain, router_weight, expert_gate, expert_up, expert_down, shared_gate, shared_up, shared_down)))

    def wrapped(*weights):
        return forward_layer(*weights, segments, routes)
    result, pullback = jax.vjp(wrapped, *floats)
    gradients = pullback(cotangent.astype(jnp.float32))
    return (result.astype(jnp.bfloat16), gradients[0], gradients[1], gradients[2], gradients[3], gradients[4], gradients[5], gradients[6], gradients[7], gradients[8], gradients[9], gradients[10], gradients[11], gradients[12], gradients[13])
```

```python
import functools
import math

import jax
import jax.numpy as jnp
from jax import lax
from jax.experimental import pallas as pl
from jax.experimental.pallas import tpu as pltpu
from jax.sharding import PartitionSpec as P

MESH = pl.DeviceIdType.MESH
F32 = jnp.float32

D = 2048
HD = 128
TOPK = 6


epsilon = 1e-06
rope_base = 10000.0
scatter_order = (46, 68, 63, 64, 18, 10, 11, 84, 88, 89, 19, 54, 9, 74, 45, 36, 38, 73, 70, 20, 83, 90, 28, 55, 37, 12, 48, 30, 65, 56, 78, 27, 47, 66, 39, 79, 91, 14, 0, 29, 13, 76, 69, 1, 21, 41, 16, 57, 75, 40, 49, 86, 3, 71, 58, 23, 43, 2, 92, 31, 42, 85, 67, 51, 32, 59, 77, 22, 25, 50, 33, 87, 5, 44, 61, 4, 15, 60, 24, 52, 34, 80, 81, 6, 17, 26, 72, 53, 62, 35, 7, 82, 8)
gather_starts = (2.97, 4.29, 2.32, 3.19, 2.3, 2.4, 5.08, 6.72, 5.91, 6.5, 6.76, 5.24)
masked_score = -1e30


class Leaf:
    def __init__(self, shape, dtype, form, first, n):
        self.shape, self.dtype, self.form, self.first, self.n = shape, dtype, form, first, n
        rows = shape[-2]
        if form == "rows":
            self.out = (4 * n * rows, shape[1])
        elif form == "cols":
            self.out = (shape[0], 4 * n * shape[1])
        elif form == "expert":
            self.out = (shape[0], shape[1], 4 * shape[2])
        elif form == "tokens":
            self.out = (n * rows, shape[1])

    def view(self, ref, d, e, half=None):
        if self.form == "rows":
            r = self.shape[0]
            s, k = (d * self.n + e) * r, r
            if half is not None:
                k = r // 2
                s = s + half * k
            return ref.at[pl.ds(pl.multiple_of(s, k), k), :]
        if self.form == "cols":
            c = self.shape[1]
            s = pl.multiple_of((d * self.n + e) * c, c)
            k = self.shape[0] // 2
            rows = slice(None) if half is None else pl.ds(half * k, k)
            return ref.at[rows, pl.ds(s, c)]
        if self.form == "tokens":
            r = self.shape[0]
            s = pl.multiple_of(e * r, r)
            if half is None:
                return ref.at[pl.ds(s, r), :]
            c = self.shape[1] // 2
            return ref.at[pl.ds(s, r), pl.ds(pl.multiple_of(half * c, c), c)]
        c = self.shape[2]
        k = self.shape[0] // 2
        heads = slice(None) if half is None else pl.ds(half * k, k)
        return ref.at[heads, :, pl.ds(pl.multiple_of(d * c, c), c)]

    def own(self, ref, half=None):
        if half is None:
            return ref
        if self.form == "tokens":
            c = self.shape[1] // 2
            return ref.at[:, pl.ds(pl.multiple_of(half * c, c), c)]
        k = self.shape[0] // 2
        return ref.at[pl.ds(half * k, k)]


def gather_kernel(leaves, n, starts, *refs):
    m = len(leaves)
    ins, outs = refs[:m], refs[m : 2 * m]
    stages = refs[2 * m : 3 * m]
    in_sem, out_sem, send_sem, recv_sem = refs[3 * m :]
    d, e, t = lax.axis_index("dp"), lax.axis_index("expert"), lax.axis_index("tensor")
    dx = d + 1 - 2 * lax.rem(d, 2)
    dy = lax.rem(d + 2, 4)
    dd = lax.rem(dx + 2, 4)
    near = {"x": {"dp": dx}, "y": {"dp": dy}, "r": {"expert": e + 1}, "l": {"expert": e - 1},
            "c": {"tensor": 1 - t}}
    has = {"r": e < n - 1, "l": e > 0}

    barrier = pltpu.get_barrier_semaphore()
    for side in ("x", "y", "c"):
        pl.semaphore_signal(barrier, inc=1, device_id=near[side], device_id_type=MESH)
    for side in ("r", "l"):
        @pl.when(has[side])
        def _():
            pl.semaphore_signal(barrier, inc=1, device_id=near[side], device_id_type=MESH)
    pl.semaphore_wait(barrier, 3 + has["r"].astype(jnp.int32) + has["l"].astype(jnp.int32))

    for i in range(m):
        pltpu.make_async_copy(ins[i], stages[i], in_sem.at[i]).start()

    count = [0]
    table = {}

    def slot(key):
        if key not in table:
            table[key] = len(table)
        return table[key]

    def copy(src, dst, side, key):
        k = slot(key)
        return pltpu.make_async_remote_copy(
            src_ref=src, dst_ref=dst, send_sem=send_sem.at[k], recv_sem=recv_sem.at[k],
            device_id=near[side], device_id_type=MESH)

    sends = []

    def send(i, dd_, ee_, half, side, key, own=False, cond=None):
        leaf = leaves[i]
        dst = leaf.view(outs[i], dd_, ee_, half)
        src = leaf.own(ins[i], half) if own else dst
        c = copy(src, dst, side, key)
        if cond is None:
            c.start()
        else:
            pl.when(cond)(c.start)
        sends.append((c, cond))

    def arrive(i, dd_, ee_, half, key, cond=None):
        leaf = leaves[i]
        dst = leaf.view(outs[i], dd_, ee_, half)
        c = copy(dst, dst, "x", key)
        if cond is None:
            c.wait_recv()
        else:
            pl.when(cond)(c.wait_recv)

    work = []

    def plane(i, ee_, at, tag, cond, own):
        def s0():
            for half, side in ((0, "x"), (1, "y"), (1, "x"), (0, "y")):
                send(i, d, ee_, half, side, (i, tag, half, side), own=own, cond=cond)
        def s1():
            arrive(i, dx, ee_, 0, (i, tag, 0, "x"), cond)
            send(i, dx, ee_, 0, "y", (i, tag, 0, "fy"), cond=cond)
            arrive(i, dy, ee_, 1, (i, tag, 1, "y"), cond)
            send(i, dy, ee_, 1, "x", (i, tag, 1, "fx"), cond=cond)
        def s2():
            arrive(i, dx, ee_, 1, (i, tag, 1, "x"), cond)
            arrive(i, dy, ee_, 0, (i, tag, 0, "y"), cond)
        def s3():
            arrive(i, dd, ee_, 0, (i, tag, 0, "fy"), cond)
            arrive(i, dd, ee_, 1, (i, tag, 1, "fx"), cond)
        for k, f in enumerate((s0, s1, s2, s3)):
            work.append((at + k, f))

    def line(i, dd_, at, tag, own, then=None):
        def s0():
            for side in ("r", "l"):
                send(i, dd_, e, None, side, (i, tag, side, 1), own=own, cond=has[side])
        work.append((at, s0))
        for k in range(1, n):
            def step(k=k):
                for side, o, there in (("r", e - k, e >= k), ("l", e + k, e + k < n)):
                    arrive(i, dd_, o, None, (i, tag, side, k), there)
                    if k < n - 1:
                        go = jnp.logical_and(there, has[side])
                        send(i, dd_, o, None, side, (i, tag, side, k + 1), cond=go)
            work.append((at + k, step))

    def tokens(i, at):
        def s0():
            for side in ("r", "l"):
                send(i, d, e, t, side, (i, side, 1), own=True, cond=has[side])
        work.append((at, s0))
        for k in range(1, n):
            def step(k=k):
                for side, o, there in (("r", e - k, e >= k), ("l", e + k, e + k < n)):
                    arrive(i, d, o, t, (i, side, k), there)
                    if k < n - 1:
                        go = jnp.logical_and(there, has[side])
                        send(i, d, o, t, side, (i, side, k + 1), cond=go)
                    send(i, d, o, t, "c", (i, "c", side, k), cond=there)
            def last(k=k):
                for side, o, there in (("r", e - k, e >= k), ("l", e + k, e + k < n)):
                    arrive(i, d, o, 1 - t, (i, "c", side, k), there)
            work.append((at + k, step))
            work.append((at + k + 1, last))

    for i, leaf in enumerate(leaves):
        at = starts[i]
        if leaf.form == "tokens":
            tokens(i, at)
            continue
        if leaf.form == "expert":
            plane(i, 0, at, "p", None, True)
        elif leaf.first == "xy":
            plane(i, e, at, "p", None, True)
            line(i, d, at, "z0", True)
            line(i, dx, at + 2.2, "zx", False)
            line(i, dy, at + 2.2, "zy", False)
            line(i, dd, at + 3.2, "zd", False)
        else:
            plane(i, e, at, "p", None, True)
            line(i, d, at, "z0", True)
            for k in range(1, n):
                plane(i, e - k, at + k + 0.5, ("pr", k), e >= k, False)
                plane(i, e + k, at + k + 0.5, ("pl", k), e + k < n, False)

    def settle():
        for i in range(m):
            pltpu.make_async_copy(ins[i], stages[i], in_sem.at[i]).wait()
            pltpu.make_async_copy(stages[i], leaves[i].view(outs[i], d, e), out_sem.at[i]).start()
    work.append((1.2, settle))
    for _, f in sorted(work, key=lambda w: w[0]):
        f()
    for c, cond in sends:
        if cond is None:
            c.wait_send()
        else:
            pl.when(cond)(c.wait_send)
    for i in range(m):
        pltpu.make_async_copy(stages[i], leaves[i].view(outs[i], d, e), out_sem.at[i]).wait()
    assert len(table) <= recv_sem.shape[0], len(table)


def gather(arrays, forms, firsts, n, starts):
    leaves = [Leaf(a.shape, a.dtype, f, o, n) for a, f, o in zip(arrays, forms, firsts)]
    total = 0
    for leaf in leaves:
        plane, line = 6, 2 * (n - 1)
        if leaf.form == "tokens":
            total += 2 * line
            continue
        total += plane if leaf.form == "expert" else plane + 4 * line if leaf.first == "xy" else plane * (2 * n - 1) + line
    m = len(leaves)
    anyspace = pl.BlockSpec(memory_space=pl.ANY)
    return pl.pallas_call(
        functools.partial(gather_kernel, leaves, n, starts),
        out_shape=[jax.ShapeDtypeStruct(leaf.out, leaf.dtype) for leaf in leaves],
        in_specs=[anyspace] * m,
        out_specs=[anyspace] * m,
        scratch_shapes=[pltpu.VMEM(leaf.shape, leaf.dtype) for leaf in leaves] + [
            pltpu.SemaphoreType.DMA((m,)), pltpu.SemaphoreType.DMA((m,)),
            pltpu.SemaphoreType.DMA((total,)), pltpu.SemaphoreType.DMA((total,))],
        compiler_params=pltpu.CompilerParams(
            collective_id=0, has_side_effects=True, vmem_limit_bytes=40 << 20),
    )(*arrays)


message_rows = 5632
ring_slots = {"x": 3, "y": 3, "z": 4}


def scatter_items(dense, units, n):
    ends = [k // 2 if k % 2 == 0 else n - 1 - k // 2 for k in range(n)]
    items = []
    for i, (_, first) in enumerate(dense):
        names = [("z", t) for t in ends] if first == "z" else []
        names += [("p", s) for s in ("y1", "x1", "x2", "y2")]
        names += [("z", t) for t in ends] if first != "z" else []
        items += [("d", i) + name for name in names] + [("d", i, "out", 0)]
    for u in range(units):
        items += [("e", u, "p", s) for s in ("y1", "x1", "x2", "y2")] + [("e", u, "out", 0)]
    return items


def scatter_kernel(dense, units, n, order, *refs):
    m = len(dense)
    lefts, rights = refs[:m], refs[m : 2 * m]
    exp_left = refs[2 * m : 2 * m + 3]
    rows_all, grads_in = refs[2 * m + 3 : 2 * m + 5]
    refs = refs[2 * m + 5 :]
    outs, refs = refs[: m + 3], refs[m + 3 :]
    landed, refs = refs[: 3 * m + 2], refs[3 * m + 2 :]
    bufs = dict(zip("xyz", refs[:3]))
    held, tall, wide = refs[3:6]
    stage_sem, load_sem, recv_sem = refs[6:9]
    send_sems = dict(zip("xyz", refs[9:12]))
    d, e = lax.axis_index("dp"), lax.axis_index("expert")
    dx = d + 1 - 2 * lax.rem(d, 2)
    dy = lax.rem(d + 2, 4)
    dd = lax.rem(dx + 2, 4)
    after, before = e < n - 1, e > 0

    barrier = pltpu.get_barrier_semaphore()
    for dev in ({"dp": dx}, {"dp": dy}):
        pl.semaphore_signal(barrier, inc=1, device_id=dev, device_id_type=MESH)
    for cond, dev in ((after, {"expert": e + 1}), (before, {"expert": e - 1})):
        @pl.when(cond)
        def _():
            pl.semaphore_signal(barrier, inc=1, device_id=dev, device_id_type=MESH)
    pl.semaphore_wait(barrier, 2 + after.astype(jnp.int32) + before.astype(jnp.int32))
    held[...] = jnp.zeros_like(held)

    def when(cond, f):
        if cond is None:
            f()
        else:
            pl.when(cond)(f)

    sems = {}

    def sem_of(key, count=1):
        if key not in sems:
            sems[key] = sum(c for _, c in sems.values()), count
        return sems[key][0]

    turns = {"x": 0, "y": 0, "z": 0}
    pending = {}

    def slot(side):
        k = turns[side] % ring_slots[side]
        turns[side] += 1
        if (side, k) in pending:
            c, cond = pending.pop((side, k))
            when(cond, c.wait_send)
        return k

    def send(side, k, rows, dst, sem, dev, cond=None):
        c = pltpu.make_async_remote_copy(
            src_ref=bufs[side].at[k, pl.ds(0, rows)], dst_ref=dst,
            send_sem=send_sems[side].at[k], recv_sem=recv_sem.at[sem],
            device_id=dev, device_id_type=MESH)
        when(cond, c.start)
        pending[(side, k)] = (c, cond)

    seen = set()

    def arrived(key, view, sem, cond=None):
        if key in seen:
            return
        seen.add(key)
        c = pltpu.make_async_remote_copy(
            src_ref=view, dst_ref=view, send_sem=recv_sem.at[sem], recv_sem=recv_sem.at[sem],
            device_id={"dp": dx}, device_id_type=MESH)
        when(cond, c.wait_recv)

    class Loads:
        def __init__(self):
            self.list = []

        def add(self, src, k, off, cond=None):
            rows = src.shape[0]
            c = pltpu.make_async_copy(src, held.at[k, pl.ds(off, rows)], load_sem.at[len(self.list)])
            when(cond, c.start)
            self.list.append((c, cond))

        def wait(self):
            for c, cond in self.list:
                when(cond, c.wait)

    def dense_piece(i, d_, e_, half, put):
        kind = dense[i][0]
        block = d_ * n + e_
        if kind == "rows":
            width = rights[i].shape[1]
            r = lefts[i].shape[0] // (4 * n)
            left = lefts[i][pl.ds(pl.multiple_of(block * r + half * (r // 2), r // 2), r // 2), :]
            for c in range(0, width, 256):
                w = min(256, width - c)
                res = jnp.dot(left, rights[i][:, c : c + w], preferred_element_type=F32)
                for k in range(0, w, 128):
                    put((c + k) // 128 * (r // 2), res[:, k : k + 128], c + k)
        else:
            half_rows = lefts[i].shape[0] // 2
            right = rights[i][:, pl.ds(pl.multiple_of(block * 128, 128), 128)]
            step = half_rows // 2
            for r in range(0, half_rows, step):
                left = lefts[i][pl.ds(pl.multiple_of(half * half_rows + r, 16), step), :]
                put(r, jnp.dot(left, right, preferred_element_type=F32), 0)

    def half_rows_of(i):
        if dense[i][0] == "rows":
            return lefts[i].shape[0] // (8 * n) * rights[i].shape[1] // 128
        return lefts[i].shape[0] // 2

    def total(value, row, adds):
        rows = value.shape[0]
        for k, off, flag in adds:
            more = held[k, pl.ds(pl.multiple_of(off + row, 16), rows), :].astype(F32)
            value = value + (more if flag is None else jnp.where(flag, more, 0.0))
        return value

    def into(side, k, base, adds):
        def put(row, value, col):
            value = total(value, row, adds)
            start = pl.multiple_of(base + row, 16)
            bufs[side][k, pl.ds(start, value.shape[0]), :] = value.astype(jnp.bfloat16)
        return put

    out_busy = {}

    def out_wait(which):
        if which in out_busy:
            out_busy.pop(which).wait()

    def dense_step(i, stage, arg):
        z_land, first_land, second_land = landed[3 * i : 3 * i + 3]
        z_first = dense[i][1] == "z"
        hb = half_rows_of(i)
        z_rows = (8 if z_first else 2) * hb
        z_sem = sem_of(("z", i), 2 * n)
        groups = 1 if z_first else n
        p_sem = {s: sem_of((s, i)) for s in ("y1", "x1", "x2", "y2")}
        place = {"y1": (first_land, 0, 2), "x1": (first_land, 1, 2), "x2": (second_land, 0, 1), "y2": (second_land, 1, 1)}

        def view(s, g0, gs, sub):
            land, which, pieces = place[s]
            if sub is None:
                return land.at[which, pl.ds(0, groups * pieces * hb)]
            return land.at[which, pl.ds(pl.multiple_of((g0 * pieces + sub) * hb, hb), gs * hb)]

        def plane_arrived(s):
            arrived((s, i), view(s, 0, 0, None), p_sem[s])

        def own_line(ld, k, off, d_, half, rows):
            for side, there in ((0, after), (1, before)):
                arrived(("own", i, side), z_land.at[side, e], z_sem + side * n + e, there)
                src = z_land.at[side, e, pl.ds(pl.multiple_of((2 * d_ + half) * hb, hb), rows)]
                ld.add(src, k + side, off, there)

        def plane_out(ld, g):
            for s in ("y1", "x1", "x2", "y2"):
                plane_arrived(s)
            ld.add(view("y1", g, 1, 1), 2, 0)
            ld.add(view("x1", g, 1, 1), 2, hb)
            ld.add(view("x2", g, 1, 0), 3, 0)
            ld.add(view("y2", g, 1, 0), 3, hb)

        if stage == "z":
            t = arg
            side = 1 - (e + n - t) // n
            more = jnp.logical_or(jnp.logical_and(e > t, after), jnp.logical_and(e < t, before))
            cond = e != t
            k = slot("z")
            def go():
                ld = Loads()
                land = z_land.at[side, t]
                arrived(("pass", i, t), land, z_sem + side * n + t, more)
                ld.add(land, 0, 0, more)
                if not z_first:
                    plane_out(ld, t)
                ld.wait()
                if z_first:
                    def one(h, _):
                        dense_piece(i, h // 2, t, h % 2, into("z", k, h * hb, [(0, h * hb, more)]))
                        return 0
                    lax.fori_loop(0, 8, one, 0)
                else:
                    def one(h, _):
                        dense_piece(i, d, t, h, into("z", k, h * hb, [(0, h * hb, more), (2, h * hb, None), (3, h * hb, None)]))
                        return 0
                    lax.fori_loop(0, 2, one, 0)
            if not z_first:
                for s in ("y1", "x1", "x2", "y2"):
                    plane_arrived(s)
            pl.when(cond)(go)
            send("z", k, z_rows, z_land.at[side, t], z_sem + side * n + t, {"expert": e - 1 + 2 * side}, cond)
        elif stage == "p":
            s = arg
            link = s[0]
            dev = {"dp": dy if link == "y" else dx}
            half = 0 if s in ("y1", "x2") else 1
            k = slot(link)
            ld = Loads()
            if s in ("y1", "x1"):
                owners = (dd, dy if link == "y" else dx)
                if z_first:
                    for q, o in enumerate(owners):
                        own_line(ld, 0, q * hb, o, half, hb)
                    ld.wait()
                    for q, o in enumerate(owners):
                        dense_piece(i, o, e, half, into(link, k, q * hb, [(0, q * hb, after), (1, q * hb, before)]))
                else:
                    def one(g, _):
                        for q, o in enumerate(owners):
                            dense_piece(i, o, g, half, into(link, k, (2 * g + q) * hb, []))
                        return 0
                    lax.fori_loop(0, n, one, 0)
                send(link, k, groups * 2 * hb, view(s, 0, 0, None), p_sem[s], dev)
            else:
                o = dx if link == "x" else dy
                prior = "y1" if s == "x2" else "x1"
                plane_arrived(prior)
                if z_first:
                    own_line(ld, 0, 0, o, half, hb)
                    ld.add(view(prior, 0, 1, 0), 2, 0)
                    ld.wait()
                    dense_piece(i, o, e, half, into(link, k, 0, [(0, 0, after), (1, 0, before), (2, 0, None)]))
                else:
                    ld.add(view(prior, 0, 0, None), 2, 0)
                    ld.wait()
                    def one(g, _):
                        dense_piece(i, o, g, half, into(link, k, g * hb, [(2, 2 * g * hb, None)]))
                        return 0
                    lax.fori_loop(0, n, one, 0)
                send(link, k, groups * hb, view(s, 0, 0, None), p_sem[s], dev)
        else:
            ld = Loads()
            if z_first:
                own_line(ld, 0, 0, d, 0, 2 * hb)
                plane_out(ld, 0)
            else:
                for side, there in ((0, after), (1, before)):
                    arrived(("own", i, side), z_land.at[side, e], z_sem + side * n + e, there)
                    ld.add(z_land.at[side, e], side, 0, there)
                plane_out(ld, e)
            rows = dense[i][0] == "rows"
            which = "wide" if rows else "tall"
            out_wait(which)
            ld.wait()
            def one(h, _):
                adds = [(0, h * hb, after), (1, h * hb, before), (2, h * hb, None), (3, h * hb, None)]
                def put(row, value, col):
                    value = total(value, row, adds)
                    if rows:
                        r = value.shape[0]
                        wide[pl.ds(pl.multiple_of(h * r, r), r), col : col + 128] = value
                    else:
                        tall[0, pl.ds(pl.multiple_of(h * hb + row, 16), value.shape[0]), 0:128] = value
                dense_piece(i, d, e, h, put)
                return 0
            lax.fori_loop(0, 2, one, 0)
            if rows:
                src = wide.at[:, pl.ds(0, outs[i].shape[1])]
            else:
                src = tall.at[0, pl.ds(0, outs[i].shape[0]), pl.ds(0, 128)]
            c = pltpu.make_async_copy(src, outs[i], stage_sem.at[0 if rows else 1])
            c.start()
            out_busy[which] = c

    first_exp, second_exp = landed[3 * m], landed[3 * m + 1]

    def expert_step(u, stage, s):
        a, q = u // 2, u % 2
        rows, width = exp_left[a].shape[1], outs[m + a].shape[2]
        tiles = width // 128
        piece = rows * tiles
        step = rows // 4
        sem = {s_: sem_of((s_, "e", u)) for s_ in ("y1", "x1", "x2", "y2")}
        place = {"y1": (first_exp, 0, 2), "x1": (first_exp, 1, 2), "x2": (second_exp, 0, 1), "y2": (second_exp, 1, 1)}

        def view(s_, sub=None):
            land, which, pieces = place[s_]
            if sub is None:
                return land.at[u, which]
            return land.at[u, which, pl.ds(sub * piece, piece)]

        def one_piece(j, d_, put):
            def body(r, _):
                left = exp_left[a][j, pl.ds(pl.multiple_of(r * step, 16), step), :]
                cols = pl.ds(pl.multiple_of(d_ * width, 128), width)
                right = grads_in[j, :, cols] if a == 2 else rows_all[:, cols]
                res = jnp.dot(left, right, preferred_element_type=F32)
                for c in range(tiles):
                    put(c * rows + r * step, res[:, c * 128 : (c + 1) * 128], (r * step, c * 128))
                return 0
            lax.fori_loop(0, 4, body, 0)

        def get(s_):
            arrived((s_, "e", u), view(s_), sem[s_])

        ld = Loads()
        if stage == "p":
            link = s[0]
            dev = {"dp": dy if link == "y" else dx}
            j = q if s in ("y1", "x2") else q + 2
            k = slot(link)
            if s in ("y1", "x1"):
                for b, o in enumerate((dd, dy if link == "y" else dx)):
                    one_piece(j, o, into(link, k, b * piece, []))
                send(link, k, 2 * piece, view(s), sem[s], dev)
            else:
                prior = "y1" if s == "x2" else "x1"
                get(prior)
                ld.add(view(prior, 0), 0, 0)
                ld.wait()
                one_piece(j, dx if link == "x" else dy, into(link, k, 0, [(0, 0, None)]))
                send(link, k, piece, view(s), sem[s], dev)
        else:
            for b, (j, one, two) in enumerate(((q, "y1", "x2"), (q + 2, "x1", "y2"))):
                get(one)
                get(two)
                ld.add(view(one, 1), 2 * b, 0)
                ld.add(view(two, 0), 2 * b + 1, 0)
            out_wait("tall")
            ld.wait()
            for b, j in enumerate((q, q + 2)):
                adds = [(2 * b, 0, None), (2 * b + 1, 0, None)]
                def put(row, value, at):
                    value = total(value, row, adds)
                    r, c = at
                    tall[b, pl.ds(pl.multiple_of(r, 16), value.shape[0]), c : c + 128] = value
                one_piece(j, d, put)
            cs = [pltpu.make_async_copy(tall.at[b, pl.ds(0, rows), pl.ds(0, width)], outs[m + a].at[q + 2 * b], stage_sem.at[1 + b]) for b in range(2)]
            for c in cs:
                c.start()
            class Both:
                def wait(self):
                    for c in cs:
                        c.wait()
            out_busy["tall"] = Both()

    items = scatter_items(dense, units, n)
    for kind, i, stage, arg in [items[k] for k in order] if order else items:
        (dense_step if kind == "d" else expert_step)(i, stage, arg)
    for c, cond in pending.values():
        when(cond, c.wait_send)
    for which in list(out_busy):
        out_wait(which)
    assert sum(c for _, c in sems.values()) <= recv_sem.shape[0]


def scatter(dense, lefts, rights, exp_left, rows_all, grads_in, n, order, cid):
    m, units = len(dense), 6
    bf = jnp.bfloat16
    outs, landed = [], []
    for (kind, first), a, b in zip(dense, lefts, rights):
        if kind == "rows":
            r = a.shape[0] // (4 * n)
            shape, hb = (r, b.shape[1]), r // 2 * b.shape[1] // 128
        else:
            shape, hb = (a.shape[0], 128), a.shape[0] // 2
        outs.append(jax.ShapeDtypeStruct(shape, F32))
        g, z = (1, 8) if first == "z" else (n, 2)
        landed += [jax.ShapeDtypeStruct((2, n, z * hb, 128), bf),
                   jax.ShapeDtypeStruct((2, g * 2 * hb, 128), bf),
                   jax.ShapeDtypeStruct((2, g * hb, 128), bf)]
    here, rows = exp_left[0].shape[:2]
    width = rows_all.shape[1] // 4
    outs += [jax.ShapeDtypeStruct((here, rows, width), F32)] * 3
    piece = rows * width // 128
    landed += [jax.ShapeDtypeStruct((units, 2, 2 * piece, 128), bf),
               jax.ShapeDtypeStruct((units, 2, piece, 128), bf)]
    anyspace, vmem = pl.BlockSpec(memory_space=pl.ANY), pl.BlockSpec(memory_space=pltpu.VMEM)
    count = m * (2 * n + 4) + 4 * units
    res = pl.pallas_call(
        functools.partial(scatter_kernel, dense, units, n, order),
        out_shape=outs + landed,
        in_specs=[vmem] * (2 * m + 5),
        out_specs=[anyspace] * (len(outs) + len(landed)),
        scratch_shapes=[pltpu.VMEM((ring_slots[s], message_rows, 128), bf) for s in "xyz"] + [
            pltpu.VMEM((4, message_rows, 128), bf),
            pltpu.VMEM((2, max(rows, max(o.shape[0] for o in outs[:m])), width), F32),
            pltpu.VMEM((128, max(o.shape[1] for o in outs[:m])), F32),
            pltpu.SemaphoreType.DMA((3,)), pltpu.SemaphoreType.DMA((8,)),
            pltpu.SemaphoreType.DMA((count,)),
        ] + [pltpu.SemaphoreType.DMA((ring_slots[s],)) for s in "xyz"],
        compiler_params=pltpu.CompilerParams(
            collective_id=cid, has_side_effects=True, vmem_limit_bytes=60 << 20),
    )(*lefts, *rights, *exp_left, rows_all, grads_in)
    return res[: m + 3]


def rms_scale(vector):
    return lax.rsqrt(jnp.mean(vector * vector, axis=-1, keepdims=True) + epsilon)


def rope_tables(count, width):
    half_width = width // 2
    frequency = rope_base ** (-jnp.arange(half_width, dtype=jnp.float32) / half_width)
    angles = jnp.arange(count, dtype=jnp.float32)[:, None] * frequency[None, :]
    return (jnp.cos(angles)[:, None, :], jnp.sin(angles)[:, None, :])


def rotate(vector, cosine, sine_table):
    half_width = vector.shape[-1] // 2
    first_half = vector[..., :half_width]
    second_half = vector[..., half_width:]
    return jnp.concatenate(
        [
            first_half * cosine - second_half * sine_table,
            first_half * sine_table + second_half * cosine,
        ],
        axis=-1,
    )


def unrotate(vector, cosine, sine_table):
    half_width = vector.shape[-1] // 2
    first_half = vector[..., :half_width]
    second_half = vector[..., half_width:]
    return jnp.concatenate(
        [
            first_half * cosine + second_half * sine_table,
            second_half * cosine - first_half * sine_table,
        ],
        axis=-1,
    )


def dots(left, right, *dims):
    return lax.dot_general(left, right, dims, preferred_element_type=F32)


def silu_parts(before):
    sigmoid_val = jax.nn.sigmoid(before)
    return (before * sigmoid_val, sigmoid_val * (1.0 + before * (1.0 - sigmoid_val)))


def masked_scores(query_rot, key_rot, allowed):
    scores = dots(query_rot, key_rot, ((2,), (2,)), ((1,), (1,))) / math.sqrt(query_rot.shape[-1])
    return jnp.where(allowed[None], scores, masked_score)


def body(
    block_input,
    attn_gain,
    query_weight,
    key_weight,
    value_weight,
    output_weight,
    ffn_gain,
    router_weight,
    expert_gate,
    expert_up,
    expert_down,
    shared_gate,
    shared_up,
    shared_down,
    segments,
    routes,
    cotangent,
):
    both = ("dp", "expert")
    small = jnp.concatenate([router_weight, attn_gain[:, None], ffn_gain[:, None]], axis=1).T
    flip_gate, flip_up = jnp.swapaxes(expert_gate, 1, 2), jnp.swapaxes(expert_up, 1, 2)
    kernels = output_weight.shape[1] % 128 == 0 and lax.axis_size("dp") == 4
    if kernels:
        small = jnp.pad(small, ((0, -small.shape[0] % 32), (0, 0)))
        arrays = (query_weight, key_weight, value_weight, output_weight, small, cotangent,
                  shared_gate, shared_up, shared_down, flip_gate, flip_up, expert_down)
        forms = ("rows",) * 3 + ("cols", "cols", "tokens", "rows", "rows", "cols") + ("expert",) * 3
        firsts = ("xy",) * 7 + ("z",) * 2 + ("xy",) * 3
        (full_query, full_key, full_value, full_output, full_small, grads_all,
         full_sgate, full_sup, full_sdown, local_gate, local_up, local_down) = gather(
            arrays, forms, firsts, lax.axis_size("expert"), gather_starts)
    else:
        full_small = lax.all_gather(small, both, axis=1, tiled=True)
        full_query = lax.all_gather(query_weight, both, axis=0, tiled=True)
        full_key = lax.all_gather(key_weight, both, axis=0, tiled=True)
        full_value = lax.all_gather(value_weight, both, axis=0, tiled=True)
        full_output = lax.all_gather(output_weight, both, axis=1, tiled=True)
        full_sgate = lax.all_gather(shared_gate, both, axis=0, tiled=True)
        full_sup = lax.all_gather(shared_up, both, axis=0, tiled=True)
        full_sdown = lax.all_gather(shared_down, both, axis=1, tiled=True)
        grads_all = lax.all_gather(cotangent, "expert", axis=0, tiled=True)
        local_gate = lax.all_gather(flip_gate, "dp", axis=2, tiled=True)
        local_up = lax.all_gather(flip_up, "dp", axis=2, tiled=True)
        local_down = lax.all_gather(expert_down, "dp", axis=2, tiled=True)
    seq_len = block_input.shape[0]
    total_experts = router_weight.shape[1]
    experts_here = expert_gate.shape[0]
    owners = lax.axis_size("expert")
    here = lax.axis_index("expert")
    all_rows = owners * seq_len
    router_rows = full_small[:total_experts]
    gain_attn = full_small[total_experts]
    gain_ffn = full_small[total_experts + 1]
    routes_all = lax.all_gather(routes, "expert", axis=0, tiled=True)
    heads_here = full_query.shape[1] // HD
    gain_one = gain_attn.astype(jnp.float32)
    gain_two = gain_ffn.astype(jnp.float32)
    input_f = block_input.astype(jnp.float32)
    scale_one = rms_scale(input_f)
    normed_one = (input_f * scale_one * gain_one).astype(jnp.bfloat16)
    cosine, sine_table = rope_tables(seq_len, HD)
    query_pre = jnp.dot(normed_one, full_query, preferred_element_type=jnp.float32).reshape(
        seq_len, heads_here, HD
    )
    key_pre = jnp.dot(normed_one, full_key, preferred_element_type=jnp.float32).reshape(
        seq_len, heads_here, HD
    )
    query_rot = rotate(query_pre, cosine, sine_table).astype(jnp.bfloat16)
    key_rot = rotate(key_pre, cosine, sine_table).astype(jnp.bfloat16)
    value_rows = (
        jnp.dot(normed_one, full_value, preferred_element_type=jnp.float32)
        .astype(jnp.bfloat16)
        .reshape(seq_len, heads_here, HD)
    )
    position = jnp.arange(seq_len)
    segment_row = segments[0]
    allowed = (position[:, None] >= position[None, :]) & (
        segment_row[:, None] == segment_row[None, :]
    )
    scores = masked_scores(query_rot, key_rot, allowed)
    top_score = jnp.max(scores, axis=-1, keepdims=True)
    shifted = jnp.exp(scores - top_score)
    row_total = jnp.sum(shifted, axis=-1, keepdims=True)
    log_total = top_score + jnp.log(row_total)
    prob_low = (shifted / row_total).astype(jnp.bfloat16)
    mixed_rows = (
        jnp.transpose(dots(prob_low, value_rows, ((2,), (0,)), ((0,), (1,))), (1, 0, 2))
        .astype(jnp.bfloat16)
        .reshape(seq_len, heads_here * HD)
    )
    attn_part = jnp.dot(mixed_rows, full_output, preferred_element_type=jnp.float32)
    attn_total = lax.psum(attn_part, "tensor")
    hidden_one = input_f + attn_total
    scale_two = rms_scale(hidden_one)
    normed_two = (hidden_one * scale_two * gain_two).astype(jnp.bfloat16)
    rows_all = lax.all_gather(normed_two, "expert", axis=0, tiled=True)
    logits = dots(rows_all, router_rows, ((1,), (1,)), ((), ()))
    probs_all = jax.nn.softmax(logits, axis=-1)
    expert_ids = jnp.arange(total_experts, dtype=jnp.int32)
    named = jnp.any(routes_all[:, :, None] == expert_ids[None, None, :], axis=1)
    gates_all = jnp.where(named, probs_all, 0.0)
    gates_here = lax.dynamic_slice_in_dim(gates_all, here * experts_here, experts_here, axis=1)
    gate_pre = jnp.transpose(dots(rows_all, local_gate, ((1,), (2,)), ((), ())), (1, 0, 2))
    up_pre = jnp.transpose(dots(rows_all, local_up, ((1,), (2,)), ((), ())), (1, 0, 2))
    silu_gate, slope_gate = silu_parts(gate_pre)
    act_rows = (silu_gate * up_pre).astype(jnp.bfloat16)
    part_rows = dots(act_rows, local_down, ((2,), (1,)), ((0,), (0,))).astype(jnp.bfloat16)
    routed_all = sum(
        gates_here[:, j : j + 1] * part_rows[j].astype(F32) for j in range(experts_here)
    )
    shared_gpre = jnp.dot(normed_two, full_sgate, preferred_element_type=jnp.float32)
    shared_upre = jnp.dot(normed_two, full_sup, preferred_element_type=jnp.float32)
    silu_shared, slope_shared = silu_parts(shared_gpre)
    shared_act = (silu_shared * shared_upre).astype(jnp.bfloat16)
    shared_part = jnp.dot(shared_act, full_sdown, preferred_element_type=jnp.float32)
    routed_part = lax.psum_scatter(routed_all, "expert", scatter_dimension=0, tiled=True)
    ffn_total = lax.psum(shared_part + routed_part, "tensor")
    block_output = (hidden_one + ffn_total).astype(jnp.bfloat16)
    grad_out = cotangent.astype(jnp.float32)
    grad_sact = dots(cotangent, full_sdown, ((1,), (1,)), ((), ()))
    grad_sgate = (grad_sact * shared_upre * slope_shared).astype(jnp.bfloat16)
    grad_sup = (grad_sact * silu_shared).astype(jnp.bfloat16)
    grad_normed_two = dots(grad_sgate, full_sgate, ((1,), (1,)), ((), ()))
    grad_normed_two = grad_normed_two + dots(grad_sup, full_sup, ((1,), (1,)), ((), ()))
    grads_wide = grads_all.astype(jnp.float32)
    owner_grads = (jnp.transpose(gates_here)[:, :, None] * grads_wide[None]).astype(jnp.bfloat16)
    grad_act = dots(owner_grads, local_down, ((2,), (2,)), ((0,), (0,)))
    grad_gate_pre = (grad_act * up_pre * slope_gate).astype(jnp.bfloat16)
    grad_up_pre = (grad_act * silu_gate).astype(jnp.bfloat16)
    grad_rows = dots(grad_gate_pre, local_gate, ((0, 2), (0, 1)), ((), ()))
    grad_rows = grad_rows + dots(grad_up_pre, local_up, ((0, 2), (0, 1)), ((), ()))
    gate_dots = jnp.sum(part_rows.astype(jnp.float32) * grads_wide[None], axis=-1)
    dots_wide = jnp.zeros((all_rows, total_experts), jnp.float32)
    dots_wide = lax.dynamic_update_slice(
        dots_wide, jnp.transpose(gate_dots), (0, here * experts_here)
    )
    rows_back = lax.psum_scatter(
        jnp.concatenate([grad_rows, dots_wide], axis=1),
        "expert", scatter_dimension=0, tiled=True,
    )
    rows_back = jnp.concatenate(
        [rows_back[:, :D] + grad_normed_two, rows_back[:, D:]], axis=1)
    rows_back = lax.psum(rows_back, "tensor")
    grad_normed_two = rows_back[:, :D]
    named_own = jnp.any(routes[:, :, None] == expert_ids[None, None, :], axis=1)
    grad_rprobs = jnp.where(named_own, rows_back[:, D:], 0.0)
    router_probs = lax.dynamic_slice_in_dim(probs_all, here * seq_len, seq_len, axis=0)
    grad_logits = (
        router_probs * (grad_rprobs - jnp.sum(grad_rprobs * router_probs, axis=-1, keepdims=True))
    ).astype(jnp.bfloat16)
    router_full = dots(normed_two, grad_logits, ((0,), (0,)), ((), ()))
    grad_normed_two = grad_normed_two + dots(grad_logits, router_rows, ((1,), (0,)), ((), ()))
    ffn_gain_full = jnp.sum(grad_normed_two * hidden_one * scale_two, axis=0)
    weighted_two = grad_normed_two * gain_two
    cube_two = scale_two * scale_two * scale_two
    grad_hidden = (
        grad_out
        + scale_two * weighted_two
        - hidden_one * cube_two * jnp.mean(hidden_one * weighted_two, axis=-1, keepdims=True)
    )
    grad_attn = grad_hidden.astype(jnp.bfloat16)
    grad_mixed = (
        dots(grad_attn, full_output, ((1,), (1,)), ((), ()))
        .astype(jnp.bfloat16)
        .reshape(seq_len, heads_here, HD)
    )
    prob_again = jnp.exp(masked_scores(query_rot, key_rot, allowed) - log_total)
    grad_probs = dots(grad_mixed, value_rows, ((2,), (2,)), ((1,), (1,)))
    grad_scores = (
        prob_again * (grad_probs - jnp.sum(prob_again * grad_probs, axis=-1, keepdims=True))
    ).astype(jnp.bfloat16)
    value_grad_rows = (
        jnp.transpose(dots(prob_again.astype(jnp.bfloat16), grad_mixed, ((1,), (0,)), ((0,), (1,))), (1, 0, 2))
        .astype(jnp.bfloat16)
        .reshape(seq_len, heads_here * HD)
    )
    inverse_root = 1.0 / math.sqrt(HD)
    grad_qrot = (
        jnp.transpose(dots(grad_scores, key_rot, ((2,), (0,)), ((0,), (1,))), (1, 0, 2))
        * inverse_root
    )
    grad_krot = (
        jnp.transpose(dots(grad_scores, query_rot, ((1,), (0,)), ((0,), (1,))), (1, 0, 2))
        * inverse_root
    )
    grad_qpre = (
        unrotate(grad_qrot, cosine, sine_table)
        .astype(jnp.bfloat16)
        .reshape(seq_len, heads_here * HD)
    )
    grad_kpre = (
        unrotate(grad_krot, cosine, sine_table)
        .astype(jnp.bfloat16)
        .reshape(seq_len, heads_here * HD)
    )
    grad_normed_one = dots(grad_qpre, full_query, ((1,), (1,)), ((), ()))
    grad_normed_one = grad_normed_one + dots(grad_kpre, full_key, ((1,), (1,)), ((), ()))
    grad_normed_one = grad_normed_one + dots(value_grad_rows, full_value, ((1,), (1,)), ((), ()))
    grad_normed_one = lax.psum(grad_normed_one.astype(jnp.bfloat16), "tensor").astype(jnp.float32)
    attn_gain_full = jnp.sum(grad_normed_one * input_f * scale_one, axis=0)
    weighted_one = grad_normed_one * gain_one
    cube_one = scale_one * scale_one * scale_one
    input_grad = (
        grad_hidden
        + scale_one * weighted_one
        - input_f * cube_one * jnp.mean(input_f * weighted_one, axis=-1, keepdims=True)
    )
    small_full = jnp.concatenate(
        [router_full, attn_gain_full[:, None], ffn_gain_full[:, None]], axis=1)
    small_grad = lax.psum_scatter(small_full, both, scatter_dimension=0, tiled=True)
    router_grad = small_grad[:, :total_experts]
    attn_gain_grad = small_grad[:, total_experts]
    ffn_gain_grad = small_grad[:, total_experts + 1]
    one_t, two_t = normed_one.T, normed_two.T
    lefts = (one_t, one_t, one_t, mixed_rows.T, two_t, two_t, shared_act.T)
    rights = (grad_qpre, grad_kpre, value_grad_rows, grad_attn, grad_sgate, grad_sup, cotangent)
    exp_left = tuple(jnp.swapaxes(v, 1, 2) for v in (grad_gate_pre, grad_up_pre, act_rows))
    dense = (("rows", "z"),) * 3 + (("cols", "z"), ("rows", "z"), ("rows", "p"), ("cols", "p"))
    if kernels:
        (query_grad, key_grad, value_grad, output_grad, shared_gate_grad, shared_up_grad,
         shared_down_grad, expert_gate_grad, expert_up_grad, expert_down_grad) = scatter(
            dense, lefts, rights, exp_left, rows_all, owner_grads, owners, scatter_order, 1)
    else:
        sums = []
        for (kind, _), left, right in zip(dense, lefts, rights):
            part = jnp.dot(left, right, preferred_element_type=F32)
            dim = 0 if kind == "rows" else 1
            sums.append(lax.psum_scatter(part, both, scatter_dimension=dim, tiled=True))
        for left, right in zip(exp_left, (rows_all, rows_all, owner_grads)):
            dims = (((2,), (0,)), ((), ())) if right.ndim == 2 else (((2,), (1,)), ((0,), (0,)))
            part = lax.dot_general(left, right, dims, preferred_element_type=F32)
            part = lax.psum_scatter(
                part.astype(jnp.bfloat16), "dp", scatter_dimension=2, tiled=True)
            sums.append(part.astype(F32))
        (query_grad, key_grad, value_grad, output_grad, shared_gate_grad, shared_up_grad,
         shared_down_grad, expert_gate_grad, expert_up_grad, expert_down_grad) = sums
    return (
        block_output,
        input_grad,
        attn_gain_grad,
        query_grad,
        key_grad,
        value_grad,
        output_grad,
        ffn_gain_grad,
        router_grad,
        jnp.swapaxes(expert_gate_grad, 1, 2),
        jnp.swapaxes(expert_up_grad, 1, 2),
        expert_down_grad,
        shared_gate_grad,
        shared_up_grad,
        shared_down_grad,
    )


def solution(mesh):
    return jax.shard_map(
        body,
        mesh=mesh,
        in_specs=(
            P(("dp", "expert"), None),
            P(("dp", "expert")),
            P(("dp", "expert"), "tensor"),
            P(("dp", "expert"), "tensor"),
            P(("dp", "expert"), "tensor"),
            P("tensor", ("dp", "expert")),
            P(("dp", "expert")),
            P(("dp", "expert"), None),
            P("expert", "dp", "tensor"),
            P("expert", "dp", "tensor"),
            P("expert", "tensor", "dp"),
            P(("dp", "expert"), "tensor"),
            P(("dp", "expert"), "tensor"),
            P("tensor", ("dp", "expert")),
            P(("dp", "expert"), None),
            P(("dp", "expert"), None),
            P(("dp", "expert"), None),
        ),
        out_specs=(
            P(("dp", "expert"), None),
            P(("dp", "expert"), None),
            P(("dp", "expert")),
            P(("dp", "expert"), "tensor"),
            P(("dp", "expert"), "tensor"),
            P(("dp", "expert"), "tensor"),
            P("tensor", ("dp", "expert")),
            P(("dp", "expert")),
            P(("dp", "expert"), None),
            P("expert", "dp", "tensor"),
            P("expert", "dp", "tensor"),
            P("expert", "tensor", "dp"),
            P(("dp", "expert"), "tensor"),
            P(("dp", "expert"), "tensor"),
            P("tensor", ("dp", "expert")),
        ),
        check_vma=False,
    )
```

```python
import functools
import math

import jax
import jax.numpy as jnp
from jax import lax
from jax.experimental import pallas as pl
from jax.experimental.pallas import tpu as pltpu
from jax.sharding import PartitionSpec as P

MESH = pl.DeviceIdType.MESH
F32, BF = jnp.float32, jnp.bfloat16
DP, EXPERT, TENSOR = "dp", "expert", "tensor"
BOTH = (DP, EXPERT)
D = 2048
HD = 128


epsilon = 1e-06
rope_base = 10000.0
masked_score = -1e30
gather_starts = (1.91, 2.48, 3.88, 2.78, 2.0, 1.0, 1.1)
scatter_order = (46, 77, 72, 73, 18, 10, 11, 93, 97, 98, 19, 54, 9, 83, 45, 36, 38, 82, 79, 20, 92, 99, 28, 55, 37, 12, 48, 30, 74, 56, 87, 27, 47, 75, 39, 88, 100, 14, 0, 63, 29, 13, 85, 78, 1, 64, 21, 41, 16, 57, 84, 40, 49, 95, 3, 66, 80, 58, 23, 43, 2, 65, 101, 31, 42, 94, 76, 51, 32, 59, 86, 22, 25, 50, 33, 96, 5, 68, 44, 61, 4, 67, 15, 60, 24, 52, 34, 89, 90, 6, 69, 17, 26, 81, 53, 62, 35, 7, 70, 91, 8, 71)
middle_order = (49, 25, 26, 27, 33, 37, 45, 46, 5, 34, 50, 6, 35, 99, 7, 8, 21, 47, 53, 48, 57, 84, 100, 101, 13, 69, 17, 18, 70, 80, 88, 0, 1, 36, 102, 73, 51, 52, 38, 39, 89, 29, 30, 65, 61, 74, 114, 28, 41, 42, 43, 66, 129, 85, 81, 82, 9, 10, 11, 12, 95, 71, 72, 103, 40, 31, 32, 90, 91, 22, 19, 20, 44, 115, 23, 24, 75, 76, 62, 2, 118, 67, 68, 77, 3, 4, 78, 79, 54, 55, 56, 86, 87, 63, 64, 96, 97, 104, 110, 14, 15, 83, 92, 93, 94, 16, 119, 58, 59, 60, 105, 106, 116, 111, 98, 107, 108, 109, 125, 117, 112, 120, 113, 121, 122, 123, 124, 126, 130, 127, 131, 128, 132, 133)


class Leaf:
    def __init__(self, shape, dtype, form, first, n):
        self.shape, self.dtype, self.form, self.first, self.n = shape, dtype, form, first, n
        rows = shape[-2]
        if form == "rows":
            self.out = (4 * n * rows, shape[1])
        elif form == "cols":
            self.out = (shape[0], 4 * n * shape[1])
        elif form == "expert":
            self.out = (shape[0], shape[1], 4 * shape[2])
        elif form == "tokens":
            self.out = (n * rows, shape[1])

    def view(self, ref, d, e, half=None):
        if self.form == "rows":
            r = self.shape[0]
            s, k = (d * self.n + e) * r, r
            if half is not None:
                k = r // 2
                s = s + half * k
            return ref.at[pl.ds(pl.multiple_of(s, k), k), :]
        if self.form == "cols":
            c = self.shape[1]
            s = pl.multiple_of((d * self.n + e) * c, c)
            k = self.shape[0] // 2
            rows = slice(None) if half is None else pl.ds(half * k, k)
            return ref.at[rows, pl.ds(s, c)]
        if self.form == "tokens":
            r = self.shape[0]
            s = pl.multiple_of(e * r, r)
            if half is None:
                return ref.at[pl.ds(s, r), :]
            c = self.shape[1] // 2
            return ref.at[pl.ds(s, r), pl.ds(pl.multiple_of(half * c, c), c)]
        c = self.shape[2]
        k = self.shape[0] // 2
        heads = slice(None) if half is None else pl.ds(half * k, k)
        return ref.at[heads, :, pl.ds(pl.multiple_of(d * c, c), c)]

    def own(self, ref, half=None):
        if half is None:
            return ref
        if self.form == "tokens":
            c = self.shape[1] // 2
            return ref.at[:, pl.ds(pl.multiple_of(half * c, c), c)]
        k = self.shape[0] // 2
        return ref.at[pl.ds(half * k, k)]


def gather_kernel(leaves, n, starts, *refs):
    m = len(leaves)
    ins, outs = refs[:m], refs[m : 2 * m]
    stages = refs[2 * m : 3 * m]
    in_sem, out_sem, send_sem, recv_sem = refs[3 * m :]
    d, e, t = lax.axis_index(DP), lax.axis_index(EXPERT), lax.axis_index(TENSOR)
    dx = d + 1 - 2 * lax.rem(d, 2)
    dy = lax.rem(d + 2, 4)
    dd = lax.rem(dx + 2, 4)
    near = {"x": {DP: dx}, "y": {DP: dy}, "r": {EXPERT: e + 1}, "l": {EXPERT: e - 1},
            "c": {TENSOR: 1 - t}}
    has = {"r": e < n - 1, "l": e > 0}

    barrier = pltpu.get_barrier_semaphore()
    for side in ("x", "y", "c"):
        pl.semaphore_signal(barrier, inc=1, device_id=near[side], device_id_type=MESH)
    for side in ("r", "l"):
        @pl.when(has[side])
        def _():
            pl.semaphore_signal(barrier, inc=1, device_id=near[side], device_id_type=MESH)
    pl.semaphore_wait(barrier, 3 + has["r"].astype(jnp.int32) + has["l"].astype(jnp.int32))

    for i in range(m):
        pltpu.make_async_copy(ins[i], stages[i], in_sem.at[i]).start()

    count = [0]
    table = {}

    def slot(key):
        if key not in table:
            table[key] = len(table)
        return table[key]

    def copy(src, dst, side, key):
        k = slot(key)
        return pltpu.make_async_remote_copy(
            src_ref=src, dst_ref=dst, send_sem=send_sem.at[k], recv_sem=recv_sem.at[k],
            device_id=near[side], device_id_type=MESH)

    sends = []

    def send(i, dd_, ee_, half, side, key, own=False, cond=None):
        leaf = leaves[i]
        dst = leaf.view(outs[i], dd_, ee_, half)
        src = leaf.own(ins[i], half) if own else dst
        c = copy(src, dst, side, key)
        if cond is None:
            c.start()
        else:
            pl.when(cond)(c.start)
        sends.append((c, cond))

    def arrive(i, dd_, ee_, half, key, cond=None):
        leaf = leaves[i]
        dst = leaf.view(outs[i], dd_, ee_, half)
        c = copy(dst, dst, "x", key)
        if cond is None:
            c.wait_recv()
        else:
            pl.when(cond)(c.wait_recv)

    work = []

    def plane(i, ee_, at, tag, cond, own):
        def s0():
            for half, side in ((0, "x"), (1, "y"), (1, "x"), (0, "y")):
                send(i, d, ee_, half, side, (i, tag, half, side), own=own, cond=cond)
        def s1():
            arrive(i, dx, ee_, 0, (i, tag, 0, "x"), cond)
            send(i, dx, ee_, 0, "y", (i, tag, 0, "fy"), cond=cond)
            arrive(i, dy, ee_, 1, (i, tag, 1, "y"), cond)
            send(i, dy, ee_, 1, "x", (i, tag, 1, "fx"), cond=cond)
        def s2():
            arrive(i, dx, ee_, 1, (i, tag, 1, "x"), cond)
            arrive(i, dy, ee_, 0, (i, tag, 0, "y"), cond)
        def s3():
            arrive(i, dd, ee_, 0, (i, tag, 0, "fy"), cond)
            arrive(i, dd, ee_, 1, (i, tag, 1, "fx"), cond)
        for k, f in enumerate((s0, s1, s2, s3)):
            work.append((at + k, f))

    def line(i, dd_, at, tag, own, then=None):
        def s0():
            for side in ("r", "l"):
                send(i, dd_, e, None, side, (i, tag, side, 1), own=own, cond=has[side])
        work.append((at, s0))
        for k in range(1, n):
            def step(k=k):
                for side, o, there in (("r", e - k, e >= k), ("l", e + k, e + k < n)):
                    arrive(i, dd_, o, None, (i, tag, side, k), there)
                    if k < n - 1:
                        go = jnp.logical_and(there, has[side])
                        send(i, dd_, o, None, side, (i, tag, side, k + 1), cond=go)
            work.append((at + k, step))

    def tokens(i, at):
        def s0():
            for side in ("r", "l"):
                send(i, d, e, t, side, (i, side, 1), own=True, cond=has[side])
        work.append((at, s0))
        for k in range(1, n):
            def step(k=k):
                for side, o, there in (("r", e - k, e >= k), ("l", e + k, e + k < n)):
                    arrive(i, d, o, t, (i, side, k), there)
                    if k < n - 1:
                        go = jnp.logical_and(there, has[side])
                        send(i, d, o, t, side, (i, side, k + 1), cond=go)
                    send(i, d, o, t, "c", (i, "c", side, k), cond=there)
            def last(k=k):
                for side, o, there in (("r", e - k, e >= k), ("l", e + k, e + k < n)):
                    arrive(i, d, o, 1 - t, (i, "c", side, k), there)
            work.append((at + k, step))
            work.append((at + k + 1, last))

    for i, leaf in enumerate(leaves):
        at = starts[i]
        if leaf.form == "tokens":
            tokens(i, at)
            continue
        if leaf.form == "expert":
            plane(i, 0, at, "p", None, True)
        elif leaf.first == "xy":
            plane(i, e, at, "p", None, True)
            line(i, d, at, "z0", True)
            line(i, dx, at + 2.2, "zx", False)
            line(i, dy, at + 2.2, "zy", False)
            line(i, dd, at + 3.2, "zd", False)
        else:
            plane(i, e, at, "p", None, True)
            line(i, d, at, "z0", True)
            for k in range(1, n):
                plane(i, e - k, at + k + 0.5, ("pr", k), e >= k, False)
                plane(i, e + k, at + k + 0.5, ("pl", k), e + k < n, False)

    def settle():
        for i in range(m):
            pltpu.make_async_copy(ins[i], stages[i], in_sem.at[i]).wait()
            pltpu.make_async_copy(stages[i], leaves[i].view(outs[i], d, e), out_sem.at[i]).start()
    work.append((1.2, settle))
    for _, f in sorted(work, key=lambda w: w[0]):
        f()
    for c, cond in sends:
        if cond is None:
            c.wait_send()
        else:
            pl.when(cond)(c.wait_send)
    for i in range(m):
        pltpu.make_async_copy(stages[i], leaves[i].view(outs[i], d, e), out_sem.at[i]).wait()
    assert len(table) <= recv_sem.shape[0], len(table)


def gather(arrays, forms, firsts, n, starts):
    leaves = [Leaf(a.shape, a.dtype, f, o, n) for a, f, o in zip(arrays, forms, firsts)]
    total = 0
    for leaf in leaves:
        plane, line = 6, 2 * (n - 1)
        if leaf.form == "tokens":
            total += 2 * line
            continue
        total += plane if leaf.form == "expert" else plane + 4 * line if leaf.first == "xy" else plane * (2 * n - 1) + line
    m = len(leaves)
    anyspace = pl.BlockSpec(memory_space=pl.ANY)
    return pl.pallas_call(
        functools.partial(gather_kernel, leaves, n, starts),
        out_shape=[jax.ShapeDtypeStruct(leaf.out, leaf.dtype) for leaf in leaves],
        in_specs=[anyspace] * m,
        out_specs=[anyspace] * m,
        scratch_shapes=[pltpu.VMEM(leaf.shape, leaf.dtype) for leaf in leaves] + [
            pltpu.SemaphoreType.DMA((m,)), pltpu.SemaphoreType.DMA((m,)),
            pltpu.SemaphoreType.DMA((total,)), pltpu.SemaphoreType.DMA((total,))],
        compiler_params=pltpu.CompilerParams(
            collective_id=0, has_side_effects=True, vmem_limit_bytes=60 << 20),
    )(*arrays)


message_rows = 5632
ring_slots = {"x": 3, "y": 3, "z": 4}


def scatter_items(dense, units, n):
    ends = [k // 2 if k % 2 == 0 else n - 1 - k // 2 for k in range(n)]
    items = []
    for i, (_, first) in enumerate(dense):
        names = [("z", t) for t in ends] if first == "z" else []
        names += [("p", s) for s in ("y1", "x1", "x2", "y2")]
        names += [("z", t) for t in ends] if first != "z" else []
        items += [("d", i) + name for name in names] + [("d", i, "out", 0)]
    for u in range(units):
        items += [("e", u, "p", s) for s in ("y1", "x1", "x2", "y2")] + [("e", u, "out", 0)]
    return items


def scatter_kernel(dense, units, n, order, *refs):
    m = len(dense)
    lefts, rights = refs[:m], refs[m : 2 * m]
    exp_left = refs[2 * m : 2 * m + 3]
    rows_all, grads_in, extra = refs[2 * m + 3 : 2 * m + 6]
    refs = refs[2 * m + 6 :]
    outs, refs = refs[: m + 3], refs[m + 3 :]
    landed, refs = refs[: 3 * m + 2], refs[3 * m + 2 :]
    bufs = dict(zip("xyz", refs[:3]))
    held, tall, wide = refs[3:6]
    stage_sem, load_sem, recv_sem = refs[6:9]
    send_sems = dict(zip("xyz", refs[9:12]))
    d, e = lax.axis_index(DP), lax.axis_index(EXPERT)
    dx = d + 1 - 2 * lax.rem(d, 2)
    dy = lax.rem(d + 2, 4)
    dd = lax.rem(dx + 2, 4)
    after, before = e < n - 1, e > 0

    barrier = pltpu.get_barrier_semaphore()
    for dev in ({DP: dx}, {DP: dy}):
        pl.semaphore_signal(barrier, inc=1, device_id=dev, device_id_type=MESH)
    for cond, dev in ((after, {EXPERT: e + 1}), (before, {EXPERT: e - 1})):
        @pl.when(cond)
        def _():
            pl.semaphore_signal(barrier, inc=1, device_id=dev, device_id_type=MESH)
    pl.semaphore_wait(barrier, 2 + after.astype(jnp.int32) + before.astype(jnp.int32))
    held[...] = jnp.zeros_like(held)

    def when(cond, f):
        if cond is None:
            f()
        else:
            pl.when(cond)(f)

    sems = {}

    def sem_of(key, count=1):
        if key not in sems:
            sems[key] = sum(c for _, c in sems.values()), count
        return sems[key][0]

    turns = {"x": 0, "y": 0, "z": 0}
    pending = {}

    def slot(side):
        k = turns[side] % ring_slots[side]
        turns[side] += 1
        if (side, k) in pending:
            c, cond = pending.pop((side, k))
            when(cond, c.wait_send)
        return k

    def send(side, k, rows, dst, sem, dev, cond=None):
        c = pltpu.make_async_remote_copy(
            src_ref=bufs[side].at[k, pl.ds(0, rows)], dst_ref=dst,
            send_sem=send_sems[side].at[k], recv_sem=recv_sem.at[sem],
            device_id=dev, device_id_type=MESH)
        when(cond, c.start)
        pending[(side, k)] = (c, cond)

    seen = set()

    def arrived(key, view, sem, cond=None):
        if key in seen:
            return
        seen.add(key)
        c = pltpu.make_async_remote_copy(
            src_ref=view, dst_ref=view, send_sem=recv_sem.at[sem], recv_sem=recv_sem.at[sem],
            device_id={DP: dx}, device_id_type=MESH)
        when(cond, c.wait_recv)

    class Loads:
        def __init__(self):
            self.list = []

        def add(self, src, k, off, cond=None):
            rows = src.shape[0]
            c = pltpu.make_async_copy(src, held.at[k, pl.ds(off, rows)], load_sem.at[len(self.list)])
            when(cond, c.start)
            self.list.append((c, cond))

        def wait(self):
            for c, cond in self.list:
                when(cond, c.wait)

    def dense_piece(i, d_, e_, half, put):
        kind = dense[i][0]
        block = d_ * n + e_
        if kind == "rows":
            width = rights[i].shape[1]
            r = lefts[i].shape[0] // (4 * n)
            left = lefts[i][pl.ds(pl.multiple_of(block * r + half * (r // 2), r // 2), r // 2), :]
            for c in range(0, width, 256):
                w = min(256, width - c)
                res = jnp.dot(left, rights[i][:, c : c + w], preferred_element_type=F32)
                for k in range(0, w, 128):
                    put((c + k) // 128 * (r // 2), res[:, k : k + 128], c + k)
        else:
            half_rows = lefts[i].shape[0] // 2
            right = rights[i][:, pl.ds(pl.multiple_of(block * 128, 128), 128)]
            step = half_rows // 2
            for r in range(0, half_rows, step):
                left = lefts[i][pl.ds(pl.multiple_of(half * half_rows + r, 16), step), :]
                res = jnp.dot(left, right, preferred_element_type=F32)
                if i == m - 1:
                    at = pl.ds(pl.multiple_of(half * half_rows + r, 16), step)
                    res = res + extra[at, pl.ds(pl.multiple_of(block * 128, 128), 128)]
                put(r, res, 0)

    def half_rows_of(i):
        if dense[i][0] == "rows":
            return lefts[i].shape[0] // (8 * n) * rights[i].shape[1] // 128
        return lefts[i].shape[0] // 2

    def total(value, row, adds):
        rows = value.shape[0]
        for k, off, flag in adds:
            more = held[k, pl.ds(pl.multiple_of(off + row, 16), rows), :].astype(F32)
            value = value + (more if flag is None else jnp.where(flag, more, 0.0))
        return value

    def into(side, k, base, adds):
        def put(row, value, col):
            value = total(value, row, adds)
            start = pl.multiple_of(base + row, 16)
            bufs[side][k, pl.ds(start, value.shape[0]), :] = value.astype(jnp.bfloat16)
        return put

    out_busy = {}

    def out_wait(which):
        if which in out_busy:
            out_busy.pop(which).wait()

    def dense_step(i, stage, arg):
        z_land, first_land, second_land = landed[3 * i : 3 * i + 3]
        z_first = dense[i][1] == "z"
        hb = half_rows_of(i)
        z_rows = (8 if z_first else 2) * hb
        z_sem = sem_of(("z", i), 2 * n)
        groups = 1 if z_first else n
        p_sem = {s: sem_of((s, i)) for s in ("y1", "x1", "x2", "y2")}
        place = {"y1": (first_land, 0, 2), "x1": (first_land, 1, 2), "x2": (second_land, 0, 1), "y2": (second_land, 1, 1)}

        def view(s, g0, gs, sub):
            land, which, pieces = place[s]
            if sub is None:
                return land.at[which, pl.ds(0, groups * pieces * hb)]
            return land.at[which, pl.ds(pl.multiple_of((g0 * pieces + sub) * hb, hb), gs * hb)]

        def plane_arrived(s):
            arrived((s, i), view(s, 0, 0, None), p_sem[s])

        def own_line(ld, k, off, d_, half, rows):
            for side, there in ((0, after), (1, before)):
                arrived(("own", i, side), z_land.at[side, e], z_sem + side * n + e, there)
                src = z_land.at[side, e, pl.ds(pl.multiple_of((2 * d_ + half) * hb, hb), rows)]
                ld.add(src, k + side, off, there)

        def plane_out(ld, g):
            for s in ("y1", "x1", "x2", "y2"):
                plane_arrived(s)
            ld.add(view("y1", g, 1, 1), 2, 0)
            ld.add(view("x1", g, 1, 1), 2, hb)
            ld.add(view("x2", g, 1, 0), 3, 0)
            ld.add(view("y2", g, 1, 0), 3, hb)

        if stage == "z":
            t = arg
            side = 1 - (e + n - t) // n
            more = jnp.logical_or(jnp.logical_and(e > t, after), jnp.logical_and(e < t, before))
            cond = e != t
            k = slot("z")
            def go():
                ld = Loads()
                land = z_land.at[side, t]
                arrived(("pass", i, t), land, z_sem + side * n + t, more)
                ld.add(land, 0, 0, more)
                if not z_first:
                    plane_out(ld, t)
                ld.wait()
                if z_first:
                    def one(h, _):
                        dense_piece(i, h // 2, t, h % 2, into("z", k, h * hb, [(0, h * hb, more)]))
                        return 0
                    lax.fori_loop(0, 8, one, 0)
                else:
                    def one(h, _):
                        dense_piece(i, d, t, h, into("z", k, h * hb, [(0, h * hb, more), (2, h * hb, None), (3, h * hb, None)]))
                        return 0
                    lax.fori_loop(0, 2, one, 0)
            if not z_first:
                for s in ("y1", "x1", "x2", "y2"):
                    plane_arrived(s)
            pl.when(cond)(go)
            send("z", k, z_rows, z_land.at[side, t], z_sem + side * n + t, {EXPERT: e - 1 + 2 * side}, cond)
        elif stage == "p":
            s = arg
            link = s[0]
            dev = {DP: dy if link == "y" else dx}
            half = 0 if s in ("y1", "x2") else 1
            k = slot(link)
            ld = Loads()
            if s in ("y1", "x1"):
                owners = (dd, dy if link == "y" else dx)
                if z_first:
                    for q, o in enumerate(owners):
                        own_line(ld, 0, q * hb, o, half, hb)
                    ld.wait()
                    for q, o in enumerate(owners):
                        dense_piece(i, o, e, half, into(link, k, q * hb, [(0, q * hb, after), (1, q * hb, before)]))
                else:
                    def one(g, _):
                        for q, o in enumerate(owners):
                            dense_piece(i, o, g, half, into(link, k, (2 * g + q) * hb, []))
                        return 0
                    lax.fori_loop(0, n, one, 0)
                send(link, k, groups * 2 * hb, view(s, 0, 0, None), p_sem[s], dev)
            else:
                o = dx if link == "x" else dy
                prior = "y1" if s == "x2" else "x1"
                plane_arrived(prior)
                if z_first:
                    own_line(ld, 0, 0, o, half, hb)
                    ld.add(view(prior, 0, 1, 0), 2, 0)
                    ld.wait()
                    dense_piece(i, o, e, half, into(link, k, 0, [(0, 0, after), (1, 0, before), (2, 0, None)]))
                else:
                    ld.add(view(prior, 0, 0, None), 2, 0)
                    ld.wait()
                    def one(g, _):
                        dense_piece(i, o, g, half, into(link, k, g * hb, [(2, 2 * g * hb, None)]))
                        return 0
                    lax.fori_loop(0, n, one, 0)
                send(link, k, groups * hb, view(s, 0, 0, None), p_sem[s], dev)
        else:
            ld = Loads()
            if z_first:
                own_line(ld, 0, 0, d, 0, 2 * hb)
                plane_out(ld, 0)
            else:
                for side, there in ((0, after), (1, before)):
                    arrived(("own", i, side), z_land.at[side, e], z_sem + side * n + e, there)
                    ld.add(z_land.at[side, e], side, 0, there)
                plane_out(ld, e)
            rows = dense[i][0] == "rows"
            which = "wide" if rows else "tall"
            out_wait(which)
            ld.wait()
            def one(h, _):
                adds = [(0, h * hb, after), (1, h * hb, before), (2, h * hb, None), (3, h * hb, None)]
                def put(row, value, col):
                    value = total(value, row, adds)
                    if rows:
                        r = value.shape[0]
                        wide[pl.ds(pl.multiple_of(h * r, r), r), col : col + 128] = value
                    else:
                        tall[0, pl.ds(pl.multiple_of(h * hb + row, 16), value.shape[0]), 0:128] = value
                dense_piece(i, d, e, h, put)
                return 0
            lax.fori_loop(0, 2, one, 0)
            if rows:
                src = wide.at[:, pl.ds(0, outs[i].shape[1])]
            else:
                src = tall.at[0, pl.ds(0, outs[i].shape[0]), pl.ds(0, 128)]
            c = pltpu.make_async_copy(src, outs[i], stage_sem.at[0 if rows else 1])
            c.start()
            out_busy[which] = c

    first_exp, second_exp = landed[3 * m], landed[3 * m + 1]

    def expert_step(u, stage, s):
        a, q = u // 2, u % 2
        rows, width = exp_left[a].shape[1], outs[m + a].shape[2]
        tiles = width // 128
        piece = rows * tiles
        step = rows // 4
        sem = {s_: sem_of((s_, "e", u)) for s_ in ("y1", "x1", "x2", "y2")}
        place = {"y1": (first_exp, 0, 2), "x1": (first_exp, 1, 2), "x2": (second_exp, 0, 1), "y2": (second_exp, 1, 1)}

        def view(s_, sub=None):
            land, which, pieces = place[s_]
            if sub is None:
                return land.at[u, which]
            return land.at[u, which, pl.ds(sub * piece, piece)]

        def one_piece(j, d_, put):
            def body(r, _):
                left = exp_left[a][j, pl.ds(pl.multiple_of(r * step, 16), step), :]
                cols = pl.ds(pl.multiple_of(d_ * width, 128), width)
                right = grads_in[j, :, cols] if a == 2 else rows_all[:, cols]
                res = jnp.dot(left, right, preferred_element_type=F32)
                for c in range(tiles):
                    put(c * rows + r * step, res[:, c * 128 : (c + 1) * 128], (r * step, c * 128))
                return 0
            lax.fori_loop(0, 4, body, 0)

        def get(s_):
            arrived((s_, "e", u), view(s_), sem[s_])

        ld = Loads()
        if stage == "p":
            link = s[0]
            dev = {DP: dy if link == "y" else dx}
            j = q if s in ("y1", "x2") else q + 2
            k = slot(link)
            if s in ("y1", "x1"):
                for b, o in enumerate((dd, dy if link == "y" else dx)):
                    one_piece(j, o, into(link, k, b * piece, []))
                send(link, k, 2 * piece, view(s), sem[s], dev)
            else:
                prior = "y1" if s == "x2" else "x1"
                get(prior)
                ld.add(view(prior, 0), 0, 0)
                ld.wait()
                one_piece(j, dx if link == "x" else dy, into(link, k, 0, [(0, 0, None)]))
                send(link, k, piece, view(s), sem[s], dev)
        else:
            for b, (j, one, two) in enumerate(((q, "y1", "x2"), (q + 2, "x1", "y2"))):
                get(one)
                get(two)
                ld.add(view(one, 1), 2 * b, 0)
                ld.add(view(two, 0), 2 * b + 1, 0)
            out_wait("tall")
            ld.wait()
            for b, j in enumerate((q, q + 2)):
                adds = [(2 * b, 0, None), (2 * b + 1, 0, None)]
                def put(row, value, at):
                    value = total(value, row, adds)
                    r, c = at
                    tall[b, pl.ds(pl.multiple_of(r, 16), value.shape[0]), c : c + 128] = value
                one_piece(j, d, put)
            cs = [pltpu.make_async_copy(tall.at[b, pl.ds(0, rows), pl.ds(0, width)], outs[m + a].at[q + 2 * b], stage_sem.at[1 + b]) for b in range(2)]
            for c in cs:
                c.start()
            class Both:
                def wait(self):
                    for c in cs:
                        c.wait()
            out_busy["tall"] = Both()

    items = scatter_items(dense, units, n)
    for kind, i, stage, arg in [items[k] for k in order] if order else items:
        (dense_step if kind == "d" else expert_step)(i, stage, arg)
    for c, cond in pending.values():
        when(cond, c.wait_send)
    for which in list(out_busy):
        out_wait(which)
    assert sum(c for _, c in sems.values()) <= recv_sem.shape[0]


def scatter(dense, lefts, rights, extra, exp_left, rows_all, grads_in, n, order, cid):
    m, units = len(dense), 6
    bf = jnp.bfloat16
    outs, landed = [], []
    for (kind, first), a, b in zip(dense, lefts, rights):
        if kind == "rows":
            r = a.shape[0] // (4 * n)
            shape, hb = (r, b.shape[1]), r // 2 * b.shape[1] // 128
        else:
            shape, hb = (a.shape[0], 128), a.shape[0] // 2
        outs.append(jax.ShapeDtypeStruct(shape, F32))
        g, z = (1, 8) if first == "z" else (n, 2)
        landed += [jax.ShapeDtypeStruct((2, n, z * hb, 128), bf),
                   jax.ShapeDtypeStruct((2, g * 2 * hb, 128), bf),
                   jax.ShapeDtypeStruct((2, g * hb, 128), bf)]
    here, rows = exp_left[0].shape[:2]
    width = rows_all.shape[1] // 4
    outs += [jax.ShapeDtypeStruct((here, rows, width), F32)] * 3
    piece = rows * width // 128
    landed += [jax.ShapeDtypeStruct((units, 2, 2 * piece, 128), bf),
               jax.ShapeDtypeStruct((units, 2, piece, 128), bf)]
    anyspace, vmem = pl.BlockSpec(memory_space=pl.ANY), pl.BlockSpec(memory_space=pltpu.VMEM)
    count = m * (2 * n + 4) + 4 * units
    res = pl.pallas_call(
        functools.partial(scatter_kernel, dense, units, n, order),
        out_shape=outs + landed,
        in_specs=[vmem] * (2 * m + 6),
        out_specs=[anyspace] * (len(outs) + len(landed)),
        scratch_shapes=[pltpu.VMEM((ring_slots[s], message_rows, 128), bf) for s in "xyz"] + [
            pltpu.VMEM((4, message_rows, 128), bf),
            pltpu.VMEM((2, max(rows, max(o.shape[0] for o in outs[:m])), width), F32),
            pltpu.VMEM((128, max(o.shape[1] for o in outs[:m])), F32),
            pltpu.SemaphoreType.DMA((3,)), pltpu.SemaphoreType.DMA((8,)),
            pltpu.SemaphoreType.DMA((count,)),
        ] + [pltpu.SemaphoreType.DMA((ring_slots[s],)) for s in "xyz"],
        compiler_params=pltpu.CompilerParams(
            collective_id=cid, has_side_effects=True, vmem_limit_bytes=60 << 20),
    )(*lefts, *rights, *exp_left, rows_all, grads_in, extra)
    return res[: m + 3]


def pair_kernel(part, total, other, send_sem, recv_sem):
    t = lax.axis_index(TENSOR)
    partner = {TENSOR: 1 - t}
    barrier = pltpu.get_barrier_semaphore()
    pl.semaphore_signal(barrier, inc=1, device_id=partner, device_id_type=MESH)
    pl.semaphore_wait(barrier, 1)
    rows = part.shape[0] // 4
    copies = []
    for k in range(4):
        piece = pl.ds(k * rows, rows)
        c = pltpu.make_async_remote_copy(
            src_ref=part.at[piece], dst_ref=other.at[piece], send_sem=send_sem.at[k],
            recv_sem=recv_sem.at[k], device_id=partner, device_id_type=MESH)
        c.start()
        copies.append(c)
    for k, c in enumerate(copies):
        c.wait_recv()
        piece = pl.ds(k * rows, rows)
        total[piece, :] = part[piece, :].astype(F32) + other[piece, :].astype(F32)
    for c in copies:
        c.wait_send()


def pair_sum(part, cid):
    vmem = pl.BlockSpec(memory_space=pltpu.VMEM)
    return pl.pallas_call(
        pair_kernel,
        out_shape=jax.ShapeDtypeStruct(part.shape, F32),
        in_specs=[vmem],
        out_specs=vmem,
        scratch_shapes=[pltpu.VMEM(part.shape, part.dtype),
                        pltpu.SemaphoreType.DMA((4,)), pltpu.SemaphoreType.DMA((4,))],
        compiler_params=pltpu.CompilerParams(collective_id=cid, has_side_effects=True),
    )(part)


def across(a, b):
    return lax.dot_general(a, b, (((1,), (1,)), ((), ())), preferred_element_type=F32)


def times(a, b):
    return jnp.dot(a, b, preferred_element_type=F32)


def middle_items(n, here):
    items = [("join",)]
    for k in range(1, n):
        items.append(("rows", k))
    items.append(("gates",))
    for i in range(3):
        items += [("plane", 12 + i, s) for s in range(4)]
        items += [("line", i, b, k) for b in range(4) for k in range(n)]
    for j in range(here):
        for a in range(3):
            items += [("plane", 3 * j + a, s) for s in range(4)]
        items += [("load", j), ("front", j), ("back", j)]
    items += [("shared_load", v) for v in range(2)] + [("shared", v) for v in range(2)]
    return items + [("settle",), ("fold_start",), ("fold_lines",), ("fold_shared",), ("fold_end",)]


def middle_kernel(n, order, *refs):
    (part, inp, gain, router, named, cot, gate_in, up_in, down_in, sg_in, su_in, sd_in) = refs[:12]
    refs = refs[12:]
    (hidden, normed, rows_all, probs, few, gn2, ffn, act_t, ggp_t, gup_t, copies_out,
     gsg, gsu, sact_t) = refs[:14]
    exp_land, sh_land = refs[14:17], refs[17:20]
    refs = refs[20:]
    (other, weights, gates, back, routed, gpre, upre, act, grad, copy_buf, turned, eye,
     sh_stage, dot_sums, fold_other, fold_own, fold_out, fold_in, few_other, few_out, few_in,
     ffn_own, gn_own) = refs[:23]
    (pair_send, pair_recv, row_send, row_recv, plane_send, plane_recv, line_send, line_recv,
     load_sem, out_sem, stage_sem, zsend, zrecv) = refs[23:]
    ins = (gate_in, up_in, down_in)
    sh_ins = (sg_in, su_in, sd_in)
    here, hid, width = gate_in.shape
    toks = inp.shape[0]
    alltoks = n * toks
    D_ = inp.shape[1]
    half = D_ // 2
    d, e, t = lax.axis_index(DP), lax.axis_index(EXPERT), lax.axis_index(TENSOR)
    dx = d + 1 - 2 * lax.rem(d, 2)
    dy = lax.rem(d + 2, 4)
    dd = lax.rem(dx + 2, 4)
    after, before = e < n - 1, e > 0
    near = {"x": {DP: dx}, "y": {DP: dy}, "r": {EXPERT: e + 1}, "l": {EXPERT: e - 1},
            "c": {TENSOR: 1 - t}}
    peers = [lax.rem(e + k, n) for k in range(1, n)]
    mine = pl.ds(pl.multiple_of(t * half, half), half)
    theirs = pl.ds(pl.multiple_of((1 - t) * half, half), half)

    barrier = pltpu.get_barrier_semaphore()
    for dev in [near["x"], near["y"], near["c"]] + [{EXPERT: p} for p in peers]:
        pl.semaphore_signal(barrier, inc=1, device_id=dev, device_id_type=MESH)
    pl.semaphore_wait(barrier, 3 + n - 1)

    def when(cond, f):
        if cond is None:
            f()
        else:
            pl.when(cond)(f)

    sends = []

    def remote(src, dst, ssem, rsem, dev, cond=None, start=True):
        c = pltpu.make_async_remote_copy(
            src_ref=src, dst_ref=dst, send_sem=ssem, recv_sem=rsem, device_id=dev,
            device_id_type=MESH)
        if start:
            when(cond, c.start)
            sends.append((c, cond))
        return c

    def block(p):
        return pl.ds(pl.multiple_of(p * toks, toks), toks)

    first = [remote(part.at[pl.ds(k * (toks // 2), toks // 2)], other.at[pl.ds(k * (toks // 2), toks // 2)],
                    pair_send.at[k], pair_recv.at[k], near["c"]) for k in range(2)]
    for i in range(3):
        pltpu.make_async_copy(sh_ins[i], sh_stage.at[i], stage_sem.at[i]).start()

    def join():
        for k, c in enumerate(first):
            c.wait_recv()
            p = pl.ds(k * (toks // 2), toks // 2)
            h = inp[p, :].astype(F32) + (part[p, :] + other[p, :])
            scale = lax.rsqrt(jnp.mean(h * h, axis=-1, keepdims=True) + epsilon)
            hidden[p, :] = h
            rows = (h * scale * gain[...]).astype(jnp.bfloat16)
            normed[p, :] = rows
            rows_all[pl.ds(pl.multiple_of(e * toks + k * (toks // 2), toks // 2), toks // 2), :] = rows
        for k, p in enumerate(peers):
            remote(normed.at[:, mine], rows_all.at[block(e), mine], row_send.at[k], row_recv.at[k], {EXPERT: p})

    def rows_step(k):
        o = lax.rem(e + n - k, n)
        view = rows_all.at[block(o), mine]
        remote(view, view, row_send.at[k - 1], row_recv.at[k - 1], near["c"], start=False).wait_recv()
        remote(view, view, row_send.at[n - 1 + k - 1], row_recv.at[n - 1 + k - 1], near["c"])

    def gates_step():
        for k in range(1, n):
            o = lax.rem(e + n - k, n)
            view = rows_all.at[block(o), theirs]
            remote(view, view, row_send.at[n - 1 + k - 1], row_recv.at[n - 1 + k - 1], near["c"], start=False).wait_recv()
        logits = across(rows_all[...], router[...])
        lane = lax.broadcasted_iota(jnp.int32, logits.shape, 1)
        logits = jnp.where(lane < 4 * n, logits, -1e30)
        top = jnp.max(logits, axis=-1, keepdims=True)
        ex = jnp.exp(logits - top)
        pr = ex / jnp.sum(ex, axis=-1, keepdims=True)
        gates[...] = pr * named[...].astype(F32)
        back[...] = jnp.zeros_like(back)
        routed[...] = jnp.zeros_like(routed)
        dot_sums[...] = jnp.zeros_like(dot_sums)
        ffn_own[...] = jnp.zeros_like(ffn_own)
        gn_own[...] = jnp.zeros_like(gn_own)
        r = lax.broadcasted_iota(jnp.int32, eye.shape, 0)
        c = lax.broadcasted_iota(jnp.int32, eye.shape, 1)
        eye[...] = jnp.where(r == c, 1.0, 0.0).astype(jnp.bfloat16)
        own = block(e)
        probs[...] = (across(rows_all[own, :], router[...]))

    def plane_view(i, o, h):
        if i < 12:
            k = hid // 2
            return exp_land[i % 3].at[i // 3, pl.ds(h * k, k), pl.ds(pl.multiple_of(o * width, width), width)]
        k = sh_land[i - 12].shape[0] // 2
        return sh_land[i - 12].at[pl.ds(h * k, k), pl.ds(pl.multiple_of((o * n + e) * 128, 128), 128)]

    def plane_own(i, h):
        if i < 12:
            k = hid // 2
            return ins[i % 3].at[i // 3, pl.ds(h * k, k)]
        k = sh_land[i - 12].shape[0] // 2
        return sh_ins[i - 12].at[pl.ds(h * k, k)]

    kinds = ("x0", "y1", "x1", "y0", "f0", "f1")

    def plane_copy(i, o, h, side, kind, own=False, start=True):
        s = 6 * i + kinds.index(kind)
        dst = plane_view(i, o, h)
        return remote(plane_own(i, h) if own else dst, dst, plane_send.at[s], plane_recv.at[s], near[side], start=start)

    def plane_step(i, s):
        if s == 0:
            plane_copy(i, d, 0, "x", "x0", own=True)
            plane_copy(i, d, 1, "y", "y1", own=True)
            plane_copy(i, d, 1, "x", "x1", own=True)
            plane_copy(i, d, 0, "y", "y0", own=True)
        elif s == 1:
            plane_copy(i, dx, 0, "x", "x0", start=False).wait_recv()
            plane_copy(i, dx, 0, "y", "f0")
            plane_copy(i, dy, 1, "x", "y1", start=False).wait_recv()
            plane_copy(i, dy, 1, "x", "f1")
        elif s == 2:
            plane_copy(i, dx, 1, "x", "x1", start=False).wait_recv()
            plane_copy(i, dy, 0, "x", "y0", start=False).wait_recv()
        else:
            plane_copy(i, dd, 0, "x", "f0", start=False).wait_recv()
            plane_copy(i, dd, 1, "x", "f1", start=False).wait_recv()

    def line_view(i, o, eo):
        return sh_land[i].at[:, pl.ds(pl.multiple_of((o * n + eo) * 128, 128), 128)]

    def line_step(i, b, k):
        o = (d, dx, dy, dd)[b]
        base = (i * 4 + b) * 2 * (n - 1)

        def copy(eo, side, hop, own=False, cond=None, start=True):
            s = base + (0 if side == "r" else n - 1) + hop - 1
            dst = line_view(i, o, eo)
            return remote(sh_ins[i] if own else dst, dst, line_send.at[s], line_recv.at[s], near[side], cond, start)

        if k == 0:
            copy(e, "r", 1, b == 0, after)
            copy(e, "l", 1, b == 0, before)
            return
        for side, eo, there, has in (("r", e - k, e >= k, after), ("l", e + k, e + k < n, before)):
            when(there, copy(eo, side, k, start=False).wait_recv)
            if k < n - 1:
                copy(eo, side, k + 1, cond=jnp.logical_and(there, has))

    loads = {}

    def load(j):
        cs = []
        for a in range(3):
            for q, o in enumerate((d, dx, dy, dd)):
                cols = pl.ds(pl.multiple_of(o * width, width), width)
                src = ins[a].at[j] if q == 0 else exp_land[a].at[j, :, cols]
                c = pltpu.make_async_copy(src, weights.at[j % 2, a, :, cols], load_sem.at[j % 2, 4 * a + q])
                c.start()
                cs.append(c)
        loads[j] = cs

    writes = []
    waiting = {}

    def write(src, dst, k):
        c = pltpu.make_async_copy(src, dst, out_sem.at[k])
        c.start()
        waiting[k] = c

    def free(k):
        if k in waiting:
            waiting.pop(k).wait()

    def ffn_front(rows, count, w):
        step = min(256, count)
        def pre(m, _):
            r = pl.ds(pl.multiple_of(m * step, step), step)
            x = rows[r, :]
            g = across(x, w(0))
            u = across(x, w(1))
            gpre[r, :] = g
            upre[r, :] = u
            act[r, :] = (g * jax.nn.sigmoid(g) * u).astype(jnp.bfloat16)
            return 0
        lax.fori_loop(0, count // step, pre, 0)

    def front(j):
        for c in loads.pop(j):
            c.wait()
        w = lambda a: weights[j % 2, a]
        ffn_front(rows_all, alltoks, w)
        free(3)
        lane = lax.broadcasted_iota(jnp.int32, (256, 128), 1)
        def out(k, _):
            m, c = k // 4, k % 4
            r = pl.ds(pl.multiple_of(m * 256, 256), 256)
            cols = pl.ds(pl.multiple_of(c * 512, 512), 512)
            piece = times(act[r, :], weights[j % 2, 2, :, cols]).astype(jnp.bfloat16).astype(F32)
            gt = gates[r, :][:, j : j + 1]
            ct = cot[r, cols].astype(F32)
            routed[r, cols] += gt * piece
            dot = jnp.sum(piece * ct, axis=-1, keepdims=True)
            dot_sums[r, :] += jnp.where(lane == e * here + j, dot, 0.0)
            copy_buf[r, cols] = (gt * ct).astype(jnp.bfloat16)
            return 0
        lax.fori_loop(0, alltoks // 256 * 4, out, 0)
        write(copy_buf, copies_out.at[j], 3)
        free(0)
        turned[0] = across(eye[...], act[...]).astype(jnp.bfloat16)
        write(turned.at[0], act_t.at[j], 0)

    def ffn_back(rows, count, w):
        step = min(256, count)
        def pre(m, _):
            r = pl.ds(pl.multiple_of(m * step, step), step)
            ga = across(rows[r, :], w(2))
            g, u = gpre[r, :], upre[r, :]
            s = jax.nn.sigmoid(g)
            grad[0, r, :] = (ga * u * (s * (1.0 + g * (1.0 - s)))).astype(jnp.bfloat16)
            grad[1, r, :] = (ga * (g * s)).astype(jnp.bfloat16)
            return 0
        lax.fori_loop(0, count // step, pre, 0)

    def back_step(j):
        ffn_back(copy_buf, alltoks, lambda a: weights[j % 2, a])
        def out(k, _):
            m, c = k // 4, k % 4
            r = pl.ds(pl.multiple_of(m * 256, 256), 256)
            cols = pl.ds(pl.multiple_of(c * 512, 512), 512)
            back[r, cols] += (times(grad[0, r, :], weights[j % 2, 0, :, cols])
                              + times(grad[1, r, :], weights[j % 2, 1, :, cols]))
            return 0
        lax.fori_loop(0, alltoks // 256 * 4, out, 0)
        for q, dst in ((0, ggp_t), (1, gup_t)):
            free(1 + q)
            turned[1 + q] = across(eye[...], grad[q]).astype(jnp.bfloat16)
            write(turned.at[1 + q], dst.at[j], 1 + q)

    def shared_load(v):
        cs = []
        for a in range(3):
            c = pltpu.make_async_copy(sh_land[a].at[pl.ds(v * hid, hid)], weights.at[v, a], load_sem.at[v, a])
            c.start()
            cs.append(c)
        loads["s", v] = cs

    def shared(v):
        for c in loads.pop(("s", v)):
            c.wait()
        free(3)
        w = lambda a: weights[v, a]
        own = block(e)
        ffn_front(normed, toks, w)
        for c in range(4):
            ffn_own[:, c * 512 : (c + 1) * 512] += times(act[0:toks, :], weights[v, 2, :, c * 512 : (c + 1) * 512])
        sact_t[pl.ds(v * hid, hid), :] = across(eye[...], act[0:toks, :]).astype(jnp.bfloat16)
        copy_buf[0:toks, :] = cot[own, :]
        ffn_back(copy_buf, toks, w)
        for c in range(4):
            gn_own[:, c * 512 : (c + 1) * 512] += (
                times(grad[0, 0:toks, :], weights[v, 0, :, c * 512 : (c + 1) * 512])
                + times(grad[1, 0:toks, :], weights[v, 1, :, c * 512 : (c + 1) * 512]))
        gsg[v] = grad[0, 0:toks, :]
        gsu[v] = grad[1, 0:toks, :]

    def settle():
        for i in range(3):
            pltpu.make_async_copy(sh_ins[i], sh_stage.at[i], stage_sem.at[i]).wait()
            pltpu.make_async_copy(sh_stage.at[i], line_view(i, d, e), stage_sem.at[i]).start()
        for i in range(3):
            pltpu.make_async_copy(sh_stage.at[i], line_view(i, d, e), stage_sem.at[i]).wait()

    def fold_start():
        for k, p in enumerate(peers + [e]):
            remote(back.at[block(p), theirs], fold_other.at[0, block(p)], pair_send.at[2 + k], pair_recv.at[2 + k], near["c"])
            remote(dot_sums.at[block(p)], few_other.at[block(p)], pair_send.at[2 + n + k], pair_recv.at[2 + n + k], near["c"])
        base = 2 + 2 * n
        for k, p in enumerate(peers + [e]):
            remote(routed.at[block(p), theirs], fold_other.at[1, block(p)], pair_send.at[base + k], pair_recv.at[base + k], near["c"])

    def got(view, k):
        remote(view, view, pair_send.at[k], pair_recv.at[k], near["c"], start=False).wait_recv()

    def fold_shared():
        base = 2 + 3 * n
        for q, src in enumerate((gn_own, ffn_own)):
            remote(src.at[:, theirs], fold_own.at[q], pair_send.at[base + q], pair_recv.at[base + q], near["c"])

    def fold_lines():
        for k, p in enumerate(peers):
            got(fold_other.at[0, block(p)], 2 + k)
            got(few_other.at[block(p)], 2 + n + k)
            fold_out[0, k] = (back[block(p), mine] + fold_other[0, block(p), :]).astype(jnp.bfloat16)
            few_out[k] = (dot_sums[block(p), :] + few_other[block(p), :]).astype(jnp.bfloat16)
            remote(fold_out.at[0, k], fold_in.at[0, k], zsend.at[k], zrecv.at[k], {EXPERT: p})
            remote(few_out.at[k], few_in.at[k], zsend.at[n - 1 + k], zrecv.at[n - 1 + k], {EXPERT: p})
        for k, p in enumerate(peers):
            got(fold_other.at[1, block(p)], 2 + 2 * n + k)
            fold_out[1, k] = (routed[block(p), mine] + fold_other[1, block(p), :]).astype(jnp.bfloat16)
            remote(fold_out.at[1, k], fold_in.at[1, k], zsend.at[2 * (n - 1) + k], zrecv.at[2 * (n - 1) + k], {EXPERT: p})

    def fold_end():
        for src, q, base in ((back, 0, 2), (routed, 1, 2 + 2 * n)):
            got(fold_other.at[q, block(e)], base + n - 1)
            got(fold_own.at[q], 2 + 3 * n + q)
            dst, own = ((gn2, gn_own), (ffn, ffn_own))[q]
            dst[:, mine] = (src[block(e), mine] + fold_other[q, block(e), :]) + (own[:, mine] + fold_own[q])
        got(few_other.at[block(e)], 2 + n + n - 1)
        few[...] = dot_sums[block(e), :] + few_other[block(e), :]
        for k in range(n - 1):
            s = n - 1 + k
            remote(few_in.at[k], few_in.at[k], zsend.at[s], zrecv.at[s], near["c"], start=False).wait_recv()
            few[...] += few_in[k].astype(F32)
        for q, dst in ((0, gn2), (1, ffn)):
            for k in range(n - 1):
                s = 2 * (n - 1) * q + k
                remote(fold_in.at[q, k], fold_in.at[q, k], zsend.at[s], zrecv.at[s], near["c"], start=False).wait_recv()
                dst[:, mine] += fold_in[q, k].astype(F32)
            s = 2 + 3 * n + 2 + q
            remote(dst.at[:, mine], dst.at[:, mine], pair_send.at[s], pair_recv.at[s], near["c"])
        for q, dst in ((0, gn2), (1, ffn)):
            got(dst.at[:, theirs], 2 + 3 * n + 2 + q)

    steps = {"join": join, "rows": rows_step, "gates": gates_step, "plane": plane_step, "line": line_step,
             "load": load, "front": front, "back": back_step, "shared_load": shared_load, "shared": shared,
             "settle": settle, "fold_start": fold_start, "fold_shared": fold_shared, "fold_lines": fold_lines,
             "fold_end": fold_end}
    items = middle_items(n, here)
    for name, *args in [items[k] for k in order]:
        steps[name](*args)
    for k in list(waiting):
        free(k)
    for c, cond in sends:
        when(cond, c.wait_send)


def middle(part, inp, gain, router, named, cot, experts, shared_t, n, order, cid):
    bf, dma, vm = jnp.bfloat16, pltpu.SemaphoreType.DMA, pltpu.VMEM
    toks, width = inp.shape
    here, hid, cut = experts[0].shape
    al = n * toks
    sh = shared_t[0].shape[0]
    S = jax.ShapeDtypeStruct
    vmem, anyspace = pl.BlockSpec(memory_space=pltpu.VMEM), pl.BlockSpec(memory_space=pl.ANY)
    outs = [
        (S((toks, width), F32), vmem), (S((toks, width), bf), vmem), (S((al, width), bf), vmem),
        (S((toks, 128), F32), vmem), (S((toks, 128), F32), vmem), (S((toks, width), F32), vmem),
        (S((toks, width), F32), vmem), (S((here, hid, al), bf), anyspace), (S((here, hid, al), bf), anyspace),
        (S((here, hid, al), bf), anyspace), (S((here, al, width), bf), anyspace),
        (S((2, toks, hid), bf), vmem), (S((2, toks, hid), bf), vmem), (S((2 * hid, toks), bf), vmem),
    ] + [(S((here, hid, width), bf), anyspace)] * 3 + [(S((sh, width), bf), anyspace)] * 3
    scratch = [
        vm((toks, width), F32), vm((2, 3, hid, width), bf), vm((al, 128), F32), vm((al, width), F32),
        vm((al, width), F32), vm((al, hid), F32), vm((al, hid), F32), vm((al, hid), bf), vm((2, al, hid), bf),
        vm((al, width), bf), vm((3, hid, al), bf), vm((hid, hid), bf), vm((3, sh, 128), bf), vm((al, 128), F32),
        vm((2, al, width // 2), F32), vm((2, toks, width // 2), F32), vm((2, n - 1, toks, width // 2), bf),
        vm((2, n - 1, toks, width // 2), bf), vm((al, 128), F32), vm((n - 1, toks, 128), bf),
        vm((n - 1, toks, 128), bf), vm((toks, width), F32), vm((toks, width), F32),
        dma((6 + 3 * n,)), dma((6 + 3 * n,)), dma((2 * n,)), dma((2 * n,)), dma((90,)), dma((90,)),
        dma((24 * (n - 1),)), dma((24 * (n - 1),)), dma((2, 12)), dma((4,)), dma((3,)),
        dma((3 * (n - 1),)), dma((3 * (n - 1),)),
    ]
    res = pl.pallas_call(
        functools.partial(middle_kernel, n, order),
        out_shape=[s for s, _ in outs], out_specs=[b for _, b in outs],
        in_specs=[vmem] * 6 + [anyspace] * 6,
        scratch_shapes=scratch,
        compiler_params=pltpu.CompilerParams(
            collective_id=cid, has_side_effects=True, vmem_limit_bytes=67043328),
    )(part, inp, gain, router, named, cot, *experts, *shared_t)
    return res[:14]


def rms_scale(vector):
    return lax.rsqrt(jnp.mean(vector * vector, axis=-1, keepdims=True) + epsilon)


def rope_tables(count, width):
    half_width = width // 2
    frequency = rope_base ** (-jnp.arange(half_width, dtype=jnp.float32) / half_width)
    angles = jnp.arange(count, dtype=jnp.float32)[:, None] * frequency[None, :]
    return (jnp.cos(angles)[:, None, :], jnp.sin(angles)[:, None, :])


def rotate(vector, cosine, sine_table):
    half_width = vector.shape[-1] // 2
    first_half = vector[..., :half_width]
    second_half = vector[..., half_width:]
    return jnp.concatenate(
        [
            first_half * cosine - second_half * sine_table,
            first_half * sine_table + second_half * cosine,
        ],
        axis=-1,
    )


def unrotate(vector, cosine, sine_table):
    half_width = vector.shape[-1] // 2
    first_half = vector[..., :half_width]
    second_half = vector[..., half_width:]
    return jnp.concatenate(
        [
            first_half * cosine + second_half * sine_table,
            second_half * cosine - first_half * sine_table,
        ],
        axis=-1,
    )


def dots(left, right, *dims):
    return lax.dot_general(left, right, dims, preferred_element_type=F32)


def silu_parts(before):
    sigmoid_val = jax.nn.sigmoid(before)
    return (before * sigmoid_val, sigmoid_val * (1.0 + before * (1.0 - sigmoid_val)))


def masked_scores(query_rot, key_rot, allowed):
    scores = dots(query_rot, key_rot, ((2,), (2,)), ((1,), (1,))) / math.sqrt(query_rot.shape[-1])
    return jnp.where(allowed[None], scores, masked_score)


def turn(array, by, axis):
    return lax.dynamic_slice_in_dim(
        jnp.concatenate([array, array], axis=axis), by, array.shape[axis], axis=axis)


def plain_middle(attn_part, input_f, gain_two, router_rows, named_all, grads_all, cotangent,
                 expert_weights, full_sgate, full_sup, full_sdown):
    here = lax.axis_index(EXPERT)
    local_gate, local_up, local_down = expert_weights
    experts_here = local_gate.shape[0]
    hidden_one = input_f + lax.psum(attn_part, TENSOR)
    normed_two = (hidden_one * rms_scale(hidden_one) * gain_two).astype(BF)
    rows_all = lax.all_gather(normed_two, EXPERT, axis=0, tiled=True)
    probs_all = jax.nn.softmax(dots(rows_all, router_rows, ((1,), (1,)), ((), ())), axis=-1)
    gates_here = lax.dynamic_slice_in_dim(
        probs_all * named_all, here * experts_here, experts_here, axis=1)
    gate_pre = dots(local_gate, rows_all, ((2,), (1,)), ((), ()))
    up_pre = dots(local_up, rows_all, ((2,), (1,)), ((), ()))
    silu_gate, slope_gate = silu_parts(gate_pre)
    act_t = (silu_gate * up_pre).astype(BF)
    part_rows = dots(act_t, local_down, ((1,), (1,)), ((0,), (0,))).astype(BF).astype(F32)
    routed = sum(gates_here[:, j : j + 1] * part_rows[j] for j in range(experts_here))
    grads_wide = grads_all.astype(F32)
    owner_grads = (jnp.transpose(gates_here)[:, :, None] * grads_wide[None]).astype(BF)
    gate_dots = jnp.sum(part_rows * grads_wide[None], axis=-1)
    dots_wide = lax.dynamic_update_slice(
        jnp.zeros_like(probs_all), jnp.transpose(gate_dots), (0, here * experts_here))
    grad_act = dots(local_down, owner_grads, ((2,), (2,)), ((0,), (0,)))
    ggp_t = (grad_act * up_pre * slope_gate).astype(BF)
    gup_t = (grad_act * silu_gate).astype(BF)
    grad_rows = dots(ggp_t, local_gate, ((0, 1), (0, 1)), ((), ()))
    grad_rows = grad_rows + dots(gup_t, local_up, ((0, 1), (0, 1)), ((), ()))
    shared_gpre = jnp.dot(normed_two, full_sgate, preferred_element_type=F32)
    shared_upre = jnp.dot(normed_two, full_sup, preferred_element_type=F32)
    silu_shared, slope_shared = silu_parts(shared_gpre)
    shared_act = (silu_shared * shared_upre).astype(BF)
    shared_part = jnp.dot(shared_act, full_sdown, preferred_element_type=F32)
    grad_sact = dots(cotangent, full_sdown, ((1,), (1,)), ((), ()))
    grad_sgate = (grad_sact * shared_upre * slope_shared).astype(BF)
    grad_sup = (grad_sact * silu_shared).astype(BF)
    own_rows = dots(grad_sgate, full_sgate, ((1,), (1,)), ((), ()))
    own_rows = own_rows + dots(grad_sup, full_sup, ((1,), (1,)), ((), ()))
    back = [lax.psum_scatter(v, EXPERT, scatter_dimension=0, tiled=True)
            for v in (grad_rows, routed, dots_wide)]
    grad_normed_two = lax.psum(back[0] + own_rows, TENSOR)
    ffn_total = lax.psum(back[1] + shared_part, TENSOR)
    dots_sum = lax.psum(back[2], TENSOR)
    router_probs = lax.dynamic_slice_in_dim(
        probs_all, here * normed_two.shape[0], normed_two.shape[0], axis=0)
    return (hidden_one, normed_two, rows_all, router_probs, dots_sum, grad_normed_two, ffn_total,
            act_t, ggp_t, gup_t, owner_grads, grad_sgate, grad_sup, shared_act.T)


def plain_scatter(dense, lefts, rights, extra, exp_left, rows_all, owner_grads):
    sums = []
    for k, ((kind, _), left, right) in enumerate(zip(dense, lefts, rights)):
        part = jnp.dot(left, right, preferred_element_type=F32)
        if k == len(dense) - 1:
            part = part + extra
        dim = 0 if kind == "rows" else 1
        sums.append(lax.psum_scatter(part, BOTH, scatter_dimension=dim, tiled=True))
    for left, right in zip(exp_left, (rows_all, rows_all, owner_grads)):
        dims = (((2,), (0,)), ((), ())) if right.ndim == 2 else (((2,), (1,)), ((0,), (0,)))
        part = dots(left, right, *dims).astype(BF)
        sums.append(lax.psum_scatter(part, DP, scatter_dimension=2, tiled=True).astype(F32))
    return sums


def body(
    block_input,
    attn_gain,
    query_weight,
    key_weight,
    value_weight,
    output_weight,
    ffn_gain,
    router_weight,
    expert_gate,
    expert_up,
    expert_down,
    shared_gate,
    shared_up,
    shared_down,
    segments,
    routes,
    cotangent,
):
    seq_len = block_input.shape[0]
    total_experts = router_weight.shape[1]
    owners, here = lax.axis_size(EXPERT), lax.axis_index(EXPERT)
    kernels = (output_weight.shape[1] % 128 == 0 and lax.axis_size(DP) == 4
               and total_experts <= 128 and seq_len == 128)
    expert_ids = jnp.arange(total_experts, dtype=jnp.int32)
    named = jnp.any(routes[:, :, None] == expert_ids[None, None, :], axis=1)
    small = jnp.concatenate([router_weight, attn_gain[:, None], ffn_gain[:, None]], axis=1).T
    flip_gate, flip_up = jnp.swapaxes(expert_gate, 1, 2), jnp.swapaxes(expert_up, 1, 2)
    named_low = named.astype(BF)
    if kernels:
        small = jnp.pad(small, ((0, -small.shape[0] % 32), (0, 0)))
        named_low = jnp.pad(named_low, ((0, 0), (0, 256 - total_experts)))
        arrays = (query_weight, key_weight, value_weight, output_weight, small, cotangent, named_low)
        forms = ("rows",) * 3 + ("cols", "cols", "tokens", "tokens")
        firsts = ("z",) * 3 + ("xy", "z", "xy", "xy")
        (full_query, full_key, full_value, full_output, full_small, grads_all, named_all) = gather(
            arrays, forms, firsts, owners, gather_starts)
    else:
        full_small = lax.all_gather(small, BOTH, axis=1, tiled=True)
        full_query = lax.all_gather(query_weight, BOTH, axis=0, tiled=True)
        full_key = lax.all_gather(key_weight, BOTH, axis=0, tiled=True)
        full_value = lax.all_gather(value_weight, BOTH, axis=0, tiled=True)
        full_output = lax.all_gather(output_weight, BOTH, axis=1, tiled=True)
        grads_all = lax.all_gather(cotangent, EXPERT, axis=0, tiled=True)
        named_all = lax.all_gather(named_low, EXPERT, axis=0, tiled=True)
    named_all = named_all[:, :total_experts]
    router_rows = full_small[:total_experts]
    gain_one = full_small[total_experts].astype(F32)
    gain_two = full_small[total_experts + 1].astype(F32)
    heads_here = full_query.shape[1] // HD
    input_f = block_input.astype(F32)
    scale_one = rms_scale(input_f)
    normed_one = (input_f * scale_one * gain_one).astype(BF)
    cosine, sine_table = rope_tables(seq_len, HD)
    query_pre = jnp.dot(normed_one, full_query, preferred_element_type=F32).reshape(
        seq_len, heads_here, HD
    )
    key_pre = jnp.dot(normed_one, full_key, preferred_element_type=F32).reshape(
        seq_len, heads_here, HD
    )
    query_rot = rotate(query_pre, cosine, sine_table).astype(BF)
    key_rot = rotate(key_pre, cosine, sine_table).astype(BF)
    value_rows = (
        jnp.dot(normed_one, full_value, preferred_element_type=F32)
        .astype(BF)
        .reshape(seq_len, heads_here, HD)
    )
    position = jnp.arange(seq_len)
    segment_row = segments[0]
    allowed = (position[:, None] >= position[None, :]) & (
        segment_row[:, None] == segment_row[None, :]
    )
    scores = masked_scores(query_rot, key_rot, allowed)
    top_score = jnp.max(scores, axis=-1, keepdims=True)
    shifted = jnp.exp(scores - top_score)
    row_total = jnp.sum(shifted, axis=-1, keepdims=True)
    log_total = top_score + jnp.log(row_total)
    prob_low = (shifted / row_total).astype(BF)
    mixed_rows = (
        jnp.transpose(dots(prob_low, value_rows, ((2,), (0,)), ((0,), (1,))), (1, 0, 2))
        .astype(BF)
        .reshape(seq_len, heads_here * HD)
    )
    attn_part = jnp.dot(mixed_rows, full_output, preferred_element_type=F32)
    experts = (flip_gate, flip_up, expert_down)
    if kernels:
        first = here * expert_gate.shape[0]
        router_pad = jnp.pad(turn(router_rows, first, 0), ((0, 128 - total_experts), (0, 0)))
        named_pad = jnp.pad(turn(named_all, first, 1), ((0, 0), (0, 128 - total_experts)))
        (hidden_one, normed_two, rows_all, logits, dots_sum, grad_normed_two, ffn_total, act_t, ggp_t, gup_t,
         owner_grads, grad_sgate, grad_sup, shared_act_t) = middle(
            attn_part, block_input, gain_two[None], router_pad, named_pad, grads_all, experts,
            (shared_gate.T, shared_up.T, shared_down), owners, middle_order, 2)
        grad_sgate = jnp.concatenate([grad_sgate[0], grad_sgate[1]], axis=1)
        grad_sup = jnp.concatenate([grad_sup[0], grad_sup[1]], axis=1)
        router_probs = jax.nn.softmax(
            turn(logits[:, :total_experts], total_experts - first, 1), axis=-1)
        dots_sum = dots_sum[:, :total_experts]
    else:
        (hidden_one, normed_two, rows_all, router_probs, dots_sum, grad_normed_two, ffn_total, act_t, ggp_t, gup_t,
         owner_grads, grad_sgate, grad_sup, shared_act_t) = plain_middle(
            attn_part, input_f, gain_two, router_rows, named_all.astype(F32), grads_all, cotangent,
            tuple(lax.all_gather(w, DP, axis=2, tiled=True) for w in experts),
            lax.all_gather(shared_gate, BOTH, axis=0, tiled=True),
            lax.all_gather(shared_up, BOTH, axis=0, tiled=True),
            lax.all_gather(shared_down, BOTH, axis=1, tiled=True))
    scale_two = rms_scale(hidden_one)
    block_output = (hidden_one + ffn_total).astype(BF)
    grad_out = cotangent.astype(F32)
    grad_rprobs = jnp.where(named, dots_sum, 0.0)
    grad_logits = (
        router_probs * (grad_rprobs - jnp.sum(grad_rprobs * router_probs, axis=-1, keepdims=True))
    ).astype(BF)
    grad_normed_two = grad_normed_two + dots(grad_logits, router_rows, ((1,), (0,)), ((), ()))
    ffn_gain_full = jnp.sum(grad_normed_two * hidden_one * scale_two, axis=0)
    weighted_two = grad_normed_two * gain_two
    cube_two = scale_two * scale_two * scale_two
    grad_hidden = (
        grad_out
        + scale_two * weighted_two
        - hidden_one * cube_two * jnp.mean(hidden_one * weighted_two, axis=-1, keepdims=True)
    )
    grad_attn = grad_hidden.astype(BF)
    grad_mixed = (
        dots(grad_attn, full_output, ((1,), (1,)), ((), ()))
        .astype(BF)
        .reshape(seq_len, heads_here, HD)
    )
    prob_again = jnp.exp(masked_scores(query_rot, key_rot, allowed) - log_total)
    grad_probs = dots(grad_mixed, value_rows, ((2,), (2,)), ((1,), (1,)))
    grad_scores = (
        prob_again * (grad_probs - jnp.sum(prob_again * grad_probs, axis=-1, keepdims=True))
    ).astype(BF)
    value_grad_rows = (
        jnp.transpose(dots(prob_again.astype(BF), grad_mixed, ((1,), (0,)), ((0,), (1,))), (1, 0, 2))
        .astype(BF)
        .reshape(seq_len, heads_here * HD)
    )
    inverse_root = 1.0 / math.sqrt(HD)
    grad_qrot = (
        jnp.transpose(dots(grad_scores, key_rot, ((2,), (0,)), ((0,), (1,))), (1, 0, 2))
        * inverse_root
    )
    grad_krot = (
        jnp.transpose(dots(grad_scores, query_rot, ((1,), (0,)), ((0,), (1,))), (1, 0, 2))
        * inverse_root
    )
    grad_qpre = (
        unrotate(grad_qrot, cosine, sine_table).astype(BF).reshape(seq_len, heads_here * HD)
    )
    grad_kpre = (
        unrotate(grad_krot, cosine, sine_table).astype(BF).reshape(seq_len, heads_here * HD)
    )
    grad_normed_one = dots(grad_qpre, full_query, ((1,), (1,)), ((), ()))
    grad_normed_one = grad_normed_one + dots(grad_kpre, full_key, ((1,), (1,)), ((), ()))
    grad_normed_one = grad_normed_one + dots(value_grad_rows, full_value, ((1,), (1,)), ((), ()))
    grad_normed_one = (
        pair_sum(grad_normed_one, 3) if kernels else lax.psum(grad_normed_one, TENSOR)
    )
    attn_gain_full = jnp.sum(grad_normed_one * input_f * scale_one, axis=0)
    weighted_one = grad_normed_one * gain_one
    cube_one = scale_one * scale_one * scale_one
    input_grad = (
        grad_hidden
        + scale_one * weighted_one
        - input_f * cube_one * jnp.mean(input_f * weighted_one, axis=-1, keepdims=True)
    )
    room = total_experts + 2 + (-(total_experts + 2) % 64)
    logits_t = jnp.pad(grad_logits.T, ((0, room - total_experts), (0, 0)))
    extra = jnp.concatenate([
        jnp.zeros((total_experts, D), F32), attn_gain_full[None], ffn_gain_full[None],
        jnp.zeros((room - total_experts - 2, D), F32)])
    one_t, two_t = normed_one.T, normed_two.T
    lefts = (one_t, one_t, one_t, mixed_rows.T, two_t, two_t, shared_act_t, logits_t)
    rights = (grad_qpre, grad_kpre, value_grad_rows, grad_attn, grad_sgate, grad_sup, cotangent, normed_two)
    exp_left = (ggp_t, gup_t, act_t)
    dense = ((("rows", "z"),) * 3
             + (("cols", "z"), ("rows", "z"), ("rows", "p"), ("cols", "p"), ("cols", "z")))
    if kernels:
        sums = scatter(
            dense, lefts, rights, extra, exp_left, rows_all, owner_grads, owners, scatter_order, 1)
    else:
        sums = plain_scatter(dense, lefts, rights, extra, exp_left, rows_all, owner_grads)
    (query_grad, key_grad, value_grad, output_grad, shared_gate_grad, shared_up_grad,
     shared_down_grad, small_grad, expert_gate_grad, expert_up_grad, expert_down_grad) = sums
    return (
        block_output,
        input_grad,
        small_grad[total_experts],
        query_grad,
        key_grad,
        value_grad,
        output_grad,
        small_grad[total_experts + 1],
        small_grad[:total_experts].T,
        jnp.swapaxes(expert_gate_grad, 1, 2),
        jnp.swapaxes(expert_up_grad, 1, 2),
        expert_down_grad,
        shared_gate_grad,
        shared_up_grad,
        shared_down_grad,
    )


def solution(mesh):
    return jax.shard_map(
        body,
        mesh=mesh,
        in_specs=(
            P((DP, EXPERT), None),
            P((DP, EXPERT)),
            P((DP, EXPERT), TENSOR),
            P((DP, EXPERT), TENSOR),
            P((DP, EXPERT), TENSOR),
            P(TENSOR, (DP, EXPERT)),
            P((DP, EXPERT)),
            P((DP, EXPERT), None),
            P(EXPERT, DP, TENSOR),
            P(EXPERT, DP, TENSOR),
            P(EXPERT, TENSOR, DP),
            P((DP, EXPERT), TENSOR),
            P((DP, EXPERT), TENSOR),
            P(TENSOR, (DP, EXPERT)),
            P((DP, EXPERT), None),
            P((DP, EXPERT), None),
            P((DP, EXPERT), None),
        ),
        out_specs=(
            P((DP, EXPERT), None),
            P((DP, EXPERT), None),
            P((DP, EXPERT)),
            P((DP, EXPERT), TENSOR),
            P((DP, EXPERT), TENSOR),
            P((DP, EXPERT), TENSOR),
            P(TENSOR, (DP, EXPERT)),
            P((DP, EXPERT)),
            P((DP, EXPERT), None),
            P(EXPERT, DP, TENSOR),
            P(EXPERT, DP, TENSOR),
            P(EXPERT, TENSOR, DP),
            P((DP, EXPERT), TENSOR),
            P((DP, EXPERT), TENSOR),
            P(TENSOR, (DP, EXPERT)),
        ),
        check_vma=False,
    )
```

```python
import functools
import math

import jax
import jax.numpy as jnp
from jax import lax
from jax.experimental import pallas as pl
from jax.experimental.pallas import tpu as pltpu
from jax.sharding import PartitionSpec as P

MESH = pl.DeviceIdType.MESH
F32, BF = jnp.float32, jnp.bfloat16
DP, EXPERT, TENSOR = "dp", "expert", "tensor"
BOTH = (DP, EXPERT)
D = 2048
HD = 128


epsilon = 1e-06
rope_base = 10000.0
masked_score = -1e30
gather_starts = (1.91, 2.48, 3.88, 2.78, 2.0, 1.0)
scatter_order = (97, 98, 73, 45, 9, 55, 2, 65, 72, 19, 100, 82, 1, 64, 46, 99, 39, 83, 54, 36, 78, 18, 38, 92, 75, 74, 37, 11, 87, 56, 77, 93, 10, 12, 47, 0, 63, 85, 94, 57, 3, 66, 84, 80, 27, 20, 41, 14, 28, 79, 13, 21, 5, 68, 40, 101, 29, 16, 43, 15, 22, 4, 67, 42, 88, 30, 48, 86, 95, 61, 17, 81, 76, 6, 69, 44, 58, 23, 7, 70, 89, 49, 90, 60, 31, 50, 96, 25, 32, 24, 8, 71, 51, 59, 52, 91, 34, 33, 26, 53, 62, 35)
middle_order = (13, 8, 33, 113, 0, 9, 10, 14, 15, 57, 53, 91, 73, 37, 58, 59, 34, 35, 17, 18, 11, 12, 92, 19, 54, 55, 61, 77, 16, 3, 109, 99, 114, 81, 65, 66, 21, 25, 74, 67, 62, 36, 26, 27, 56, 69, 95, 100, 101, 82, 29, 30, 31, 93, 4, 115, 116, 110, 111, 20, 96, 97, 78, 28, 22, 23, 24, 94, 41, 63, 117, 5, 6, 7, 1, 68, 75, 76, 112, 98, 103, 32, 83, 84, 86, 60, 2, 70, 71, 72, 64, 102, 104, 127, 45, 42, 131, 38, 79, 80, 85, 87, 88, 89, 90, 105, 118, 135, 39, 40, 46, 49, 43, 128, 129, 106, 107, 108, 47, 121, 123, 44, 132, 119, 120, 122, 124, 125, 126, 136, 137, 50, 51, 52, 133, 134, 130, 139, 141, 48, 145, 138, 140, 142, 151, 143, 152, 144, 147, 146, 148, 149, 150, 153, 154)


class Leaf:
    def __init__(self, shape, dtype, form, first, n):
        self.shape, self.dtype, self.form, self.first, self.n = shape, dtype, form, first, n
        rows = shape[-2]
        if form == "rows":
            self.out = (4 * n * rows, shape[1])
        elif form == "cols":
            self.out = (shape[0], 4 * n * shape[1])
        elif form == "expert":
            self.out = (shape[0], shape[1], 4 * shape[2])
        elif form == "tokens":
            self.out = (n * rows, shape[1])

    def view(self, ref, d, e, half=None):
        if self.form == "rows":
            r = self.shape[0]
            s, k = (d * self.n + e) * r, r
            if half is not None:
                k = r // 2
                s = s + half * k
            return ref.at[pl.ds(pl.multiple_of(s, k), k), :]
        if self.form == "cols":
            c = self.shape[1]
            s = pl.multiple_of((d * self.n + e) * c, c)
            k = self.shape[0] // 2
            rows = slice(None) if half is None else pl.ds(half * k, k)
            return ref.at[rows, pl.ds(s, c)]
        if self.form == "tokens":
            r = self.shape[0]
            s = pl.multiple_of(e * r, r)
            if half is None:
                return ref.at[pl.ds(s, r), :]
            c = self.shape[1] // 2
            return ref.at[pl.ds(s, r), pl.ds(pl.multiple_of(half * c, c), c)]
        c = self.shape[2]
        k = self.shape[0] // 2
        heads = slice(None) if half is None else pl.ds(half * k, k)
        return ref.at[heads, :, pl.ds(pl.multiple_of(d * c, c), c)]

    def own(self, ref, half=None):
        if half is None:
            return ref
        if self.form == "tokens":
            c = self.shape[1] // 2
            return ref.at[:, pl.ds(pl.multiple_of(half * c, c), c)]
        k = self.shape[0] // 2
        return ref.at[pl.ds(half * k, k)]


def gather_kernel(leaves, n, starts, *refs):
    m = len(leaves)
    ins, plain, refs = refs[:m], refs[m : m + 2], refs[m + 2 :]
    outs, turned, refs = refs[:m], refs[m : m + 2], refs[m + 2 :]
    stages = refs[:m]
    in_sem, out_sem, send_sem, recv_sem = refs[m:]
    d, e, t = lax.axis_index(DP), lax.axis_index(EXPERT), lax.axis_index(TENSOR)
    dx = d + 1 - 2 * lax.rem(d, 2)
    dy = lax.rem(d + 2, 4)
    dd = lax.rem(dx + 2, 4)
    near = {"x": {DP: dx}, "y": {DP: dy}, "r": {EXPERT: e + 1}, "l": {EXPERT: e - 1},
            "c": {TENSOR: 1 - t}}
    has = {"r": e < n - 1, "l": e > 0}

    barrier = pltpu.get_barrier_semaphore()
    for side in ("x", "y", "c"):
        pl.semaphore_signal(barrier, inc=1, device_id=near[side], device_id_type=MESH)
    for side in ("r", "l"):
        @pl.when(has[side])
        def _():
            pl.semaphore_signal(barrier, inc=1, device_id=near[side], device_id_type=MESH)
    pl.semaphore_wait(barrier, 3 + has["r"].astype(jnp.int32) + has["l"].astype(jnp.int32))

    for i in range(m):
        pltpu.make_async_copy(ins[i], stages[i], in_sem.at[i]).start()

    count = [0]
    table = {}

    def slot(key):
        if key not in table:
            table[key] = len(table)
        return table[key]

    def copy(src, dst, side, key):
        k = slot(key)
        return pltpu.make_async_remote_copy(
            src_ref=src, dst_ref=dst, send_sem=send_sem.at[k], recv_sem=recv_sem.at[k],
            device_id=near[side], device_id_type=MESH)

    sends = []

    def send(i, dd_, ee_, half, side, key, own=False, cond=None):
        leaf = leaves[i]
        dst = leaf.view(outs[i], dd_, ee_, half)
        src = leaf.own(ins[i], half) if own else dst
        c = copy(src, dst, side, key)
        if cond is None:
            c.start()
        else:
            pl.when(cond)(c.start)
        sends.append((c, cond))

    def arrive(i, dd_, ee_, half, key, cond=None):
        leaf = leaves[i]
        dst = leaf.view(outs[i], dd_, ee_, half)
        c = copy(dst, dst, "x", key)
        if cond is None:
            c.wait_recv()
        else:
            pl.when(cond)(c.wait_recv)

    work = []

    def plane(i, ee_, at, tag, cond, own):
        def s0():
            for half, side in ((0, "x"), (1, "y"), (1, "x"), (0, "y")):
                send(i, d, ee_, half, side, (i, tag, half, side), own=own, cond=cond)
        def s1():
            arrive(i, dx, ee_, 0, (i, tag, 0, "x"), cond)
            send(i, dx, ee_, 0, "y", (i, tag, 0, "fy"), cond=cond)
            arrive(i, dy, ee_, 1, (i, tag, 1, "y"), cond)
            send(i, dy, ee_, 1, "x", (i, tag, 1, "fx"), cond=cond)
        def s2():
            arrive(i, dx, ee_, 1, (i, tag, 1, "x"), cond)
            arrive(i, dy, ee_, 0, (i, tag, 0, "y"), cond)
        def s3():
            arrive(i, dd, ee_, 0, (i, tag, 0, "fy"), cond)
            arrive(i, dd, ee_, 1, (i, tag, 1, "fx"), cond)
        for k, f in enumerate((s0, s1, s2, s3)):
            work.append((at + k, f))

    def line(i, dd_, at, tag, own, then=None):
        def s0():
            for side in ("r", "l"):
                send(i, dd_, e, None, side, (i, tag, side, 1), own=own, cond=has[side])
        work.append((at, s0))
        for k in range(1, n):
            def step(k=k):
                for side, o, there in (("r", e - k, e >= k), ("l", e + k, e + k < n)):
                    arrive(i, dd_, o, None, (i, tag, side, k), there)
                    if k < n - 1:
                        go = jnp.logical_and(there, has[side])
                        send(i, dd_, o, None, side, (i, tag, side, k + 1), cond=go)
            work.append((at + k, step))

    def tokens(i, at):
        def s0():
            for side in ("r", "l"):
                send(i, d, e, t, side, (i, side, 1), own=True, cond=has[side])
        work.append((at, s0))
        for k in range(1, n):
            def step(k=k):
                for side, o, there in (("r", e - k, e >= k), ("l", e + k, e + k < n)):
                    arrive(i, d, o, t, (i, side, k), there)
                    if k < n - 1:
                        go = jnp.logical_and(there, has[side])
                        send(i, d, o, t, side, (i, side, k + 1), cond=go)
                    send(i, d, o, t, "c", (i, "c", side, k), cond=there)
            def last(k=k):
                for side, o, there in (("r", e - k, e >= k), ("l", e + k, e + k < n)):
                    arrive(i, d, o, 1 - t, (i, "c", side, k), there)
            work.append((at + k, step))
            work.append((at + k + 1, last))

    for i, leaf in enumerate(leaves):
        at = starts[i]
        if leaf.form == "tokens":
            tokens(i, at)
            continue
        if leaf.form == "expert":
            plane(i, 0, at, "p", None, True)
        elif leaf.first == "xy":
            plane(i, e, at, "p", None, True)
            line(i, d, at, "z0", True)
            line(i, dx, at + 2.2, "zx", False)
            line(i, dy, at + 2.2, "zy", False)
            line(i, dd, at + 3.2, "zd", False)
        else:
            plane(i, e, at, "p", None, True)
            line(i, d, at, "z0", True)
            for k in range(1, n):
                plane(i, e - k, at + k + 0.5, ("pr", k), e >= k, False)
                plane(i, e + k, at + k + 0.5, ("pl", k), e + k < n, False)

    def settle():
        for a, b in zip(plain, turned):
            b[...] = a[...].astype(F32).T.astype(b.dtype)
        for i in range(m):
            pltpu.make_async_copy(ins[i], stages[i], in_sem.at[i]).wait()
            pltpu.make_async_copy(stages[i], leaves[i].view(outs[i], d, e), out_sem.at[i]).start()
    work.append((1.2, settle))
    for _, f in sorted(work, key=lambda w: w[0]):
        f()
    for c, cond in sends:
        if cond is None:
            c.wait_send()
        else:
            pl.when(cond)(c.wait_send)
    for i in range(m):
        pltpu.make_async_copy(stages[i], leaves[i].view(outs[i], d, e), out_sem.at[i]).wait()
    assert len(table) <= recv_sem.shape[0], len(table)


def gather(arrays, forms, firsts, n, starts, plain):
    leaves = [Leaf(a.shape, a.dtype, f, o, n) for a, f, o in zip(arrays, forms, firsts)]
    total = 0
    for leaf in leaves:
        plane, line = 6, 2 * (n - 1)
        if leaf.form == "tokens":
            total += 2 * line
            continue
        total += plane if leaf.form == "expert" else plane + 4 * line if leaf.first == "xy" else plane * (2 * n - 1) + line
    m = len(leaves)
    anyspace, vmem = pl.BlockSpec(memory_space=pl.ANY), pl.BlockSpec(memory_space=pltpu.VMEM)
    return pl.pallas_call(
        functools.partial(gather_kernel, leaves, n, starts),
        out_shape=[jax.ShapeDtypeStruct(leaf.out, leaf.dtype) for leaf in leaves] + [
            jax.ShapeDtypeStruct(v.shape[::-1], v.dtype) for v in plain],
        in_specs=[anyspace] * m + [vmem] * 2,
        out_specs=[anyspace] * m + [vmem] * 2,
        scratch_shapes=[pltpu.VMEM(leaf.shape, leaf.dtype) for leaf in leaves] + [
            pltpu.SemaphoreType.DMA((m,)), pltpu.SemaphoreType.DMA((m,)),
            pltpu.SemaphoreType.DMA((total,)), pltpu.SemaphoreType.DMA((total,))],
        compiler_params=pltpu.CompilerParams(
            collective_id=0, has_side_effects=True, vmem_limit_bytes=60 << 20),
    )(*arrays, *plain)


message_rows = 5632
ring_slots = {"x": 4, "y": 4, "z": 6}


def scatter_items(dense, units, n):
    ends = [k // 2 if k % 2 == 0 else n - 1 - k // 2 for k in range(n)]
    items = []
    for i, (_, first) in enumerate(dense):
        names = [("z", t) for t in ends] if first == "z" else []
        names += [("p", s) for s in ("y1", "x1", "x2", "y2")]
        names += [("z", t) for t in ends] if first != "z" else []
        items += [("d", i) + name for name in names] + [("d", i, "out", 0)]
    for u in range(units):
        items += [("e", u, "p", s) for s in ("y1", "x1", "x2", "y2")] + [("e", u, "out", 0)]
    return items


def scatter_kernel(dense, units, n, order, which, *refs):
    m = len(dense)
    u_ = max(which) + 1
    given, refs = refs[:u_], refs[u_:]
    held_in, refs = refs[-u_ - 1 : -1], refs[: -u_ - 1] + refs[-1:]
    in_sem, refs = refs[-1], refs[:-1]
    seat = [held_in[w] for w in which]
    lefts, rights = seat[:m], seat[m : 2 * m]
    exp_left = seat[2 * m : 2 * m + 3]
    rows_all, grads_in, extra = seat[2 * m + 3 : 2 * m + 6]
    here_yet = set()

    def need(*numbers):
        for k in numbers:
            w = which[k]
            if w not in here_yet:
                here_yet.add(w)
                pltpu.make_async_copy(given[w], held_in[w], in_sem.at[w]).wait()

    first_use = [k for it in ([scatter_items(dense, units, n)[o] for o in order] if order else scatter_items(dense, units, n))
                 for k in ((it[1], m + it[1]) + ((2 * m + 5,) if it[1] == m - 1 else ()) if it[0] == "d"
                           else (2 * m + it[1] // 2, 2 * m + 3 + (it[1] // 2 == 2)))]
    for w in dict.fromkeys(which[k] for k in first_use):
        pltpu.make_async_copy(given[w], held_in[w], in_sem.at[w]).start()
    outs, refs = refs[: m + 3], refs[m + 3 :]
    landed, refs = refs[: 3 * m + 2], refs[3 * m + 2 :]
    bufs = dict(zip("xyz", refs[:3]))
    held, tall, wide = refs[3:6]
    stage_sem, load_sem, recv_sem = refs[6:9]
    send_sems = dict(zip("xyz", refs[9:12]))
    d, e = lax.axis_index(DP), lax.axis_index(EXPERT)
    dx = d + 1 - 2 * lax.rem(d, 2)
    dy = lax.rem(d + 2, 4)
    dd = lax.rem(dx + 2, 4)
    after, before = e < n - 1, e > 0

    barrier = pltpu.get_barrier_semaphore()
    for dev in ({DP: dx}, {DP: dy}):
        pl.semaphore_signal(barrier, inc=1, device_id=dev, device_id_type=MESH)
    for cond, dev in ((after, {EXPERT: e + 1}), (before, {EXPERT: e - 1})):
        @pl.when(cond)
        def _():
            pl.semaphore_signal(barrier, inc=1, device_id=dev, device_id_type=MESH)
    pl.semaphore_wait(barrier, 2 + after.astype(jnp.int32) + before.astype(jnp.int32))
    held[...] = jnp.zeros_like(held)

    def when(cond, f):
        if cond is None:
            f()
        else:
            pl.when(cond)(f)

    sems = {}

    def sem_of(key, count=1):
        if key not in sems:
            sems[key] = sum(c for _, c in sems.values()), count
        return sems[key][0]

    turns = {"x": 0, "y": 0, "z": 0}
    pending = {}

    def slot(side):
        k = turns[side] % ring_slots[side]
        turns[side] += 1
        if (side, k) in pending:
            c, cond = pending.pop((side, k))
            when(cond, c.wait_send)
        return k

    def send(side, k, rows, dst, sem, dev, cond=None):
        c = pltpu.make_async_remote_copy(
            src_ref=bufs[side].at[k, pl.ds(0, rows)], dst_ref=dst,
            send_sem=send_sems[side].at[k], recv_sem=recv_sem.at[sem],
            device_id=dev, device_id_type=MESH)
        when(cond, c.start)
        pending[(side, k)] = (c, cond)

    seen = set()

    def arrived(key, view, sem, cond=None):
        if key in seen:
            return
        seen.add(key)
        c = pltpu.make_async_remote_copy(
            src_ref=view, dst_ref=view, send_sem=recv_sem.at[sem], recv_sem=recv_sem.at[sem],
            device_id={DP: dx}, device_id_type=MESH)
        when(cond, c.wait_recv)

    class Loads:
        def __init__(self):
            self.list = []

        def add(self, src, k, off, cond=None):
            rows = src.shape[0]
            c = pltpu.make_async_copy(src, held.at[k, pl.ds(off, rows)], load_sem.at[len(self.list)])
            when(cond, c.start)
            self.list.append((c, cond))

        def wait(self):
            for c, cond in self.list:
                when(cond, c.wait)

    def dense_piece(i, d_, e_, half, put):
        kind = dense[i][0]
        block = d_ * n + e_
        if kind == "rows":
            width = rights[i].shape[1]
            r = lefts[i].shape[0] // (4 * n)
            left = lefts[i][pl.ds(pl.multiple_of(block * r + half * (r // 2), r // 2), r // 2), :]
            for c in range(0, width, 256):
                w = min(256, width - c)
                res = jnp.dot(left, rights[i][:, c : c + w], preferred_element_type=F32)
                for k in range(0, w, 128):
                    put((c + k) // 128 * (r // 2), res[:, k : k + 128], c + k)
        else:
            half_rows = lefts[i].shape[0] // 2
            right = rights[i][:, pl.ds(pl.multiple_of(block * 128, 128), 128)]
            step = half_rows // 2
            for r in range(0, half_rows, step):
                left = lefts[i][pl.ds(pl.multiple_of(half * half_rows + r, 16), step), :]
                res = jnp.dot(left, right, preferred_element_type=F32)
                if i == m - 1:
                    at = pl.ds(pl.multiple_of(half * half_rows + r, 16), step)
                    res = res + extra[at, pl.ds(pl.multiple_of(block * 128, 128), 128)]
                put(r, res, 0)

    def half_rows_of(i):
        if dense[i][0] == "rows":
            return lefts[i].shape[0] // (8 * n) * rights[i].shape[1] // 128
        return lefts[i].shape[0] // 2

    def total(value, row, adds):
        rows = value.shape[0]
        for k, off, flag in adds:
            more = held[k, pl.ds(pl.multiple_of(off + row, 16), rows), :].astype(F32)
            value = value + (more if flag is None else jnp.where(flag, more, 0.0))
        return value

    def into(side, k, base, adds):
        def put(row, value, col):
            value = total(value, row, adds)
            start = pl.multiple_of(base + row, 16)
            bufs[side][k, pl.ds(start, value.shape[0]), :] = value.astype(jnp.bfloat16)
        return put

    out_busy = {}

    def out_wait(which):
        if which in out_busy:
            out_busy.pop(which).wait()

    def dense_step(i, stage, arg):
        need(i, m + i)
        if i == m - 1:
            need(2 * m + 5)
        z_land, first_land, second_land = landed[3 * i : 3 * i + 3]
        z_first = dense[i][1] == "z"
        hb = half_rows_of(i)
        z_rows = (8 if z_first else 2) * hb
        z_sem = sem_of(("z", i), 2 * n)
        groups = 1 if z_first else n
        p_sem = {s: sem_of((s, i)) for s in ("y1", "x1", "x2", "y2")}
        place = {"y1": (first_land, 0, 2), "x1": (first_land, 1, 2), "x2": (second_land, 0, 1), "y2": (second_land, 1, 1)}

        def view(s, g0, gs, sub):
            land, which, pieces = place[s]
            if sub is None:
                return land.at[which, pl.ds(0, groups * pieces * hb)]
            return land.at[which, pl.ds(pl.multiple_of((g0 * pieces + sub) * hb, hb), gs * hb)]

        def plane_arrived(s):
            arrived((s, i), view(s, 0, 0, None), p_sem[s])

        def own_line(ld, k, off, d_, half, rows):
            for side, there in ((0, after), (1, before)):
                arrived(("own", i, side), z_land.at[side, e], z_sem + side * n + e, there)
                src = z_land.at[side, e, pl.ds(pl.multiple_of((2 * d_ + half) * hb, hb), rows)]
                ld.add(src, k + side, off, there)

        def plane_out(ld, g):
            for s in ("y1", "x1", "x2", "y2"):
                plane_arrived(s)
            ld.add(view("y1", g, 1, 1), 2, 0)
            ld.add(view("x1", g, 1, 1), 2, hb)
            ld.add(view("x2", g, 1, 0), 3, 0)
            ld.add(view("y2", g, 1, 0), 3, hb)

        if stage == "z":
            t = arg
            side = 1 - (e + n - t) // n
            more = jnp.logical_or(jnp.logical_and(e > t, after), jnp.logical_and(e < t, before))
            cond = e != t
            k = slot("z")
            def go():
                ld = Loads()
                land = z_land.at[side, t]
                arrived(("pass", i, t), land, z_sem + side * n + t, more)
                ld.add(land, 0, 0, more)
                if not z_first:
                    plane_out(ld, t)
                ld.wait()
                if z_first:
                    def one(h, _):
                        dense_piece(i, h // 2, t, h % 2, into("z", k, h * hb, [(0, h * hb, more)]))
                        return 0
                    lax.fori_loop(0, 8, one, 0)
                else:
                    def one(h, _):
                        dense_piece(i, d, t, h, into("z", k, h * hb, [(0, h * hb, more), (2, h * hb, None), (3, h * hb, None)]))
                        return 0
                    lax.fori_loop(0, 2, one, 0)
            if not z_first:
                for s in ("y1", "x1", "x2", "y2"):
                    plane_arrived(s)
            pl.when(cond)(go)
            send("z", k, z_rows, z_land.at[side, t], z_sem + side * n + t, {EXPERT: e - 1 + 2 * side}, cond)
        elif stage == "p":
            s = arg
            link = s[0]
            dev = {DP: dy if link == "y" else dx}
            half = 0 if s in ("y1", "x2") else 1
            k = slot(link)
            ld = Loads()
            if s in ("y1", "x1"):
                owners = (dd, dy if link == "y" else dx)
                if z_first:
                    for q, o in enumerate(owners):
                        own_line(ld, 0, q * hb, o, half, hb)
                    ld.wait()
                    for q, o in enumerate(owners):
                        dense_piece(i, o, e, half, into(link, k, q * hb, [(0, q * hb, after), (1, q * hb, before)]))
                else:
                    def one(g, _):
                        for q, o in enumerate(owners):
                            dense_piece(i, o, g, half, into(link, k, (2 * g + q) * hb, []))
                        return 0
                    lax.fori_loop(0, n, one, 0)
                send(link, k, groups * 2 * hb, view(s, 0, 0, None), p_sem[s], dev)
            else:
                o = dx if link == "x" else dy
                prior = "y1" if s == "x2" else "x1"
                plane_arrived(prior)
                if z_first:
                    own_line(ld, 0, 0, o, half, hb)
                    ld.add(view(prior, 0, 1, 0), 2, 0)
                    ld.wait()
                    dense_piece(i, o, e, half, into(link, k, 0, [(0, 0, after), (1, 0, before), (2, 0, None)]))
                else:
                    ld.add(view(prior, 0, 0, None), 2, 0)
                    ld.wait()
                    def one(g, _):
                        dense_piece(i, o, g, half, into(link, k, g * hb, [(2, 2 * g * hb, None)]))
                        return 0
                    lax.fori_loop(0, n, one, 0)
                send(link, k, groups * hb, view(s, 0, 0, None), p_sem[s], dev)
        else:
            ld = Loads()
            if z_first:
                own_line(ld, 0, 0, d, 0, 2 * hb)
                plane_out(ld, 0)
            else:
                for side, there in ((0, after), (1, before)):
                    arrived(("own", i, side), z_land.at[side, e], z_sem + side * n + e, there)
                    ld.add(z_land.at[side, e], side, 0, there)
                plane_out(ld, e)
            rows = dense[i][0] == "rows"
            which = "wide" if rows else "tall"
            out_wait(which)
            ld.wait()
            def one(h, _):
                adds = [(0, h * hb, after), (1, h * hb, before), (2, h * hb, None), (3, h * hb, None)]
                def put(row, value, col):
                    value = total(value, row, adds)
                    if rows:
                        r = value.shape[0]
                        wide[pl.ds(pl.multiple_of(h * r, r), r), col : col + 128] = value
                    else:
                        tall[0, pl.ds(pl.multiple_of(h * hb + row, 16), value.shape[0]), 0:128] = value
                dense_piece(i, d, e, h, put)
                return 0
            lax.fori_loop(0, 2, one, 0)
            if rows:
                src = wide.at[:, pl.ds(0, outs[i].shape[1])]
            else:
                src = tall.at[0, pl.ds(0, outs[i].shape[0]), pl.ds(0, 128)]
            c = pltpu.make_async_copy(src, outs[i], stage_sem.at[0 if rows else 1])
            c.start()
            out_busy[which] = c

    first_exp, second_exp = landed[3 * m], landed[3 * m + 1]

    def expert_step(u, stage, s):
        a, q = u // 2, u % 2
        need(2 * m + a, 2 * m + 3 + (a == 2))
        rows, width = exp_left[a].shape[1], outs[m + a].shape[2]
        tiles = width // 128
        piece = rows * tiles
        step = rows // 4
        sem = {s_: sem_of((s_, "e", u)) for s_ in ("y1", "x1", "x2", "y2")}
        place = {"y1": (first_exp, 0, 2), "x1": (first_exp, 1, 2), "x2": (second_exp, 0, 1), "y2": (second_exp, 1, 1)}

        def view(s_, sub=None):
            land, which, pieces = place[s_]
            if sub is None:
                return land.at[u, which]
            return land.at[u, which, pl.ds(sub * piece, piece)]

        def one_piece(j, d_, put):
            def body(r, _):
                left = exp_left[a][j, pl.ds(pl.multiple_of(r * step, 16), step), :]
                cols = pl.ds(pl.multiple_of(d_ * width, 128), width)
                right = grads_in[j, :, cols] if a == 2 else rows_all[:, cols]
                res = jnp.dot(left, right, preferred_element_type=F32)
                for c in range(tiles):
                    put(c * rows + r * step, res[:, c * 128 : (c + 1) * 128], (r * step, c * 128))
                return 0
            lax.fori_loop(0, 4, body, 0)

        def get(s_):
            arrived((s_, "e", u), view(s_), sem[s_])

        ld = Loads()
        if stage == "p":
            link = s[0]
            dev = {DP: dy if link == "y" else dx}
            j = q if s in ("y1", "x2") else q + 2
            k = slot(link)
            if s in ("y1", "x1"):
                for b, o in enumerate((dd, dy if link == "y" else dx)):
                    one_piece(j, o, into(link, k, b * piece, []))
                send(link, k, 2 * piece, view(s), sem[s], dev)
            else:
                prior = "y1" if s == "x2" else "x1"
                get(prior)
                ld.add(view(prior, 0), 0, 0)
                ld.wait()
                one_piece(j, dx if link == "x" else dy, into(link, k, 0, [(0, 0, None)]))
                send(link, k, piece, view(s), sem[s], dev)
        else:
            for b, (j, one, two) in enumerate(((q, "y1", "x2"), (q + 2, "x1", "y2"))):
                get(one)
                get(two)
                ld.add(view(one, 1), 2 * b, 0)
                ld.add(view(two, 0), 2 * b + 1, 0)
            out_wait("tall")
            ld.wait()
            for b, j in enumerate((q, q + 2)):
                adds = [(2 * b, 0, None), (2 * b + 1, 0, None)]
                def put(row, value, at):
                    value = total(value, row, adds)
                    r, c = at
                    tall[b, pl.ds(pl.multiple_of(r, 16), value.shape[0]), c : c + 128] = value
                one_piece(j, d, put)
            cs = [pltpu.make_async_copy(tall.at[b, pl.ds(0, rows), pl.ds(0, width)], outs[m + a].at[q + 2 * b], stage_sem.at[1 + b]) for b in range(2)]
            for c in cs:
                c.start()
            class Both:
                def wait(self):
                    for c in cs:
                        c.wait()
            out_busy["tall"] = Both()

    items = scatter_items(dense, units, n)
    for kind, i, stage, arg in [items[k] for k in order] if order else items:
        (dense_step if kind == "d" else expert_step)(i, stage, arg)
    for c, cond in pending.values():
        when(cond, c.wait_send)
    for which in list(out_busy):
        out_wait(which)
    assert sum(c for _, c in sems.values()) <= recv_sem.shape[0]


def scatter(dense, lefts, rights, extra, exp_left, rows_all, grads_in, n, order, cid):
    m, units = len(dense), 6
    bf = jnp.bfloat16
    outs, landed = [], []
    for (kind, first), a, b in zip(dense, lefts, rights):
        if kind == "rows":
            r = a.shape[0] // (4 * n)
            shape, hb = (r, b.shape[1]), r // 2 * b.shape[1] // 128
        else:
            shape, hb = (a.shape[0], 128), a.shape[0] // 2
        outs.append(jax.ShapeDtypeStruct(shape, F32))
        g, z = (1, 8) if first == "z" else (n, 2)
        landed += [jax.ShapeDtypeStruct((2, n, z * hb, 128), bf),
                   jax.ShapeDtypeStruct((2, g * 2 * hb, 128), bf),
                   jax.ShapeDtypeStruct((2, g * hb, 128), bf)]
    here, rows = exp_left[0].shape[:2]
    width = rows_all.shape[1] // 4
    outs += [jax.ShapeDtypeStruct((here, rows, width), F32)] * 3
    piece = rows * width // 128
    landed += [jax.ShapeDtypeStruct((units, 2, 2 * piece, 128), bf),
               jax.ShapeDtypeStruct((units, 2, piece, 128), bf)]
    anyspace = pl.BlockSpec(memory_space=pl.ANY)
    count = m * (2 * n + 4) + 4 * units
    taken = [*lefts, *rights, *exp_left, rows_all, grads_in, extra]
    single = list({id(v): v for v in taken}.values())
    which = tuple([id(v) for v in single].index(id(v)) for v in taken)
    res = pl.pallas_call(
        functools.partial(scatter_kernel, dense, units, n, order, which),
        out_shape=outs + landed,
        in_specs=[anyspace] * len(single),
        out_specs=[anyspace] * (len(outs) + len(landed)),
        scratch_shapes=[pltpu.VMEM((ring_slots[s], message_rows, 128), bf) for s in "xyz"] + [
            pltpu.VMEM((4, message_rows, 128), bf),
            pltpu.VMEM((2, max(rows, max(o.shape[0] for o in outs[:m])), width), F32),
            pltpu.VMEM((128, max(o.shape[1] for o in outs[:m])), F32),
            pltpu.SemaphoreType.DMA((3,)), pltpu.SemaphoreType.DMA((8,)),
            pltpu.SemaphoreType.DMA((count,)),
        ] + [pltpu.SemaphoreType.DMA((ring_slots[s],)) for s in "xyz"] + [
            pltpu.VMEM(v.shape, v.dtype) for v in single] + [pltpu.SemaphoreType.DMA((len(single),))],
        compiler_params=pltpu.CompilerParams(
            collective_id=cid, has_side_effects=True, vmem_limit_bytes=67043328),
    )(*single)
    return res[: m + 3]


def pair_kernel(part, total, other, send_sem, recv_sem):
    t = lax.axis_index(TENSOR)
    partner = {TENSOR: 1 - t}
    barrier = pltpu.get_barrier_semaphore()
    pl.semaphore_signal(barrier, inc=1, device_id=partner, device_id_type=MESH)
    pl.semaphore_wait(barrier, 1)
    rows = part.shape[0] // 4
    copies = []
    for k in range(4):
        piece = pl.ds(k * rows, rows)
        c = pltpu.make_async_remote_copy(
            src_ref=part.at[piece], dst_ref=other.at[piece], send_sem=send_sem.at[k],
            recv_sem=recv_sem.at[k], device_id=partner, device_id_type=MESH)
        c.start()
        copies.append(c)
    for k, c in enumerate(copies):
        c.wait_recv()
        piece = pl.ds(k * rows, rows)
        total[piece, :] = part[piece, :].astype(F32) + other[piece, :].astype(F32)
    for c in copies:
        c.wait_send()


def pair_sum(part, cid):
    vmem = pl.BlockSpec(memory_space=pltpu.VMEM)
    return pl.pallas_call(
        pair_kernel,
        out_shape=jax.ShapeDtypeStruct(part.shape, F32),
        in_specs=[vmem],
        out_specs=vmem,
        scratch_shapes=[pltpu.VMEM(part.shape, part.dtype),
                        pltpu.SemaphoreType.DMA((4,)), pltpu.SemaphoreType.DMA((4,))],
        compiler_params=pltpu.CompilerParams(collective_id=cid, has_side_effects=True),
    )(part)


def across(a, b):
    return lax.dot_general(a, b, (((1,), (1,)), ((), ())), preferred_element_type=F32)


def times(a, b):
    return jnp.dot(a, b, preferred_element_type=F32)


def middle_items(n, here):
    items = [("join",), ("gates",), ("settle",)]
    for q in range(2):
        items += [("tok", q, k) for k in range(n)] + [("tokend", q)]
    for i in range(3):
        items += [("plane", 12 + i, s) for s in range(4)]
        items += [("line", i, b, k) for b in range(4) for k in range(n)]
    for j in range(here):
        for a in range(3):
            items += [("plane", 3 * j + a, s) for s in range(4)]
        items += [(name, j) for name in ("load", "load_down", "pre", "front", "back", "rows")]
    for v in range(2):
        items += [("shared_load", v), ("shared", v), ("fold_start", v), ("fold_lines", v)]
    return items + [("fold_shared",), ("fold_end",)]


def middle_kernel(n, order, *refs):
    (part, inp, gain, router, named, cot_own, one, mixed, gate_in, up_in, down_in, sg_in, su_in, sd_in) = refs[:14]
    refs = refs[14:]
    (hidden, normed, rows_all, probs, few, gn2, ffn, act_t, ggp_t, gup_t, copies_out,
     gsg, gsu, sact_t, one_t, two_t, mixed_t) = refs[:17]
    exp_land, sh_land = refs[17:20], refs[20:23]
    refs = refs[23:]
    (other, weights, gates, back, routed, gpre, upre, act, grad, copy_buf, turned, eye,
     sh_stage, dot_sums, fold_other, fold_own, fold_out, fold_in, few_other, few_out, few_in,
     ffn_own, gn_own, cot) = refs[:24]
    (pair_send, pair_recv, row_send, row_recv, plane_send, plane_recv, line_send, line_recv,
     load_sem, out_sem, stage_sem, zsend, zrecv) = refs[24:]
    ins = (gate_in, up_in, down_in)
    sh_ins = (sg_in, su_in, sd_in)
    here, hid, width = gate_in.shape
    toks = inp.shape[0]
    alltoks = n * toks
    D_ = inp.shape[1]
    half = D_ // 2
    d, e, t = lax.axis_index(DP), lax.axis_index(EXPERT), lax.axis_index(TENSOR)
    dx = d + 1 - 2 * lax.rem(d, 2)
    dy = lax.rem(d + 2, 4)
    dd = lax.rem(dx + 2, 4)
    after, before = e < n - 1, e > 0
    near = {"x": {DP: dx}, "y": {DP: dy}, "r": {EXPERT: e + 1}, "l": {EXPERT: e - 1},
            "c": {TENSOR: 1 - t}}
    peers = [lax.rem(e + k, n) for k in range(1, n)]
    mine = pl.ds(pl.multiple_of(t * half, half), half)
    theirs = pl.ds(pl.multiple_of((1 - t) * half, half), half)

    barrier = pltpu.get_barrier_semaphore()
    for dev in [near["x"], near["y"], near["c"]] + [{EXPERT: p} for p in peers]:
        pl.semaphore_signal(barrier, inc=1, device_id=dev, device_id_type=MESH)
    pl.semaphore_wait(barrier, 3 + n - 1)

    def when(cond, f):
        if cond is None:
            f()
        else:
            pl.when(cond)(f)

    sends = []

    def remote(src, dst, ssem, rsem, dev, cond=None, start=True):
        c = pltpu.make_async_remote_copy(
            src_ref=src, dst_ref=dst, send_sem=ssem, recv_sem=rsem, device_id=dev,
            device_id_type=MESH)
        if start:
            when(cond, c.start)
            sends.append((c, cond))
        return c

    def block(p):
        return pl.ds(pl.multiple_of(p * toks, toks), toks)

    first = [remote(part.at[pl.ds(k * (toks // 2), toks // 2)], other.at[pl.ds(k * (toks // 2), toks // 2)],
                    pair_send.at[k], pair_recv.at[k], near["c"]) for k in range(2)]
    for i in range(3):
        pltpu.make_async_copy(sh_ins[i], sh_stage.at[i], stage_sem.at[i]).start()

    def join():
        for k, c in enumerate(first):
            c.wait_recv()
            p = pl.ds(k * (toks // 2), toks // 2)
            h = inp[p, :].astype(F32) + (part[p, :] + other[p, :])
            scale = lax.rsqrt(jnp.mean(h * h, axis=-1, keepdims=True) + epsilon)
            hidden[p, :] = h
            rows = (h * scale * gain[...]).astype(jnp.bfloat16)
            normed[p, :] = rows
            rows_all[pl.ds(pl.multiple_of(e * toks + k * (toks // 2), toks // 2), toks // 2), :] = rows
        two_t[...] = normed[...].astype(F32).T.astype(jnp.bfloat16)

    def along(k):
        return (("r", e - k, e >= k, after, 0), ("l", e + k, e + k < n, before, 1))

    def tok_step(q, k):
        every = (rows_all, cot)[q]
        base = 4 * (n - 1) * q
        if k == 0:
            src = (normed, cot_own)[q]
            for side, has, w in (("r", after, 0), ("l", before, 1)):
                s = base + (n - 1) * w
                remote(src.at[:, mine], every.at[block(e), mine], row_send.at[s], row_recv.at[s], near[side], has)
            return
        for side, o, there, has, w in along(k):
            view = every.at[block(o), mine]
            s = base + (n - 1) * w + k - 1
            when(there, remote(view, view, row_send.at[s], row_recv.at[s], near[side], start=False).wait_recv)
            if k < n - 1:
                remote(view, view, row_send.at[s + 1], row_recv.at[s + 1], near[side], jnp.logical_and(there, has))
            s += 2 * (n - 1)
            remote(view, view, row_send.at[s], row_recv.at[s], near["c"], there)

    def tok_end(q):
        every = (rows_all, cot)[q]
        for k in range(1, n):
            for side, o, there, has, w in along(k):
                view = every.at[block(o), theirs]
                s = 4 * (n - 1) * q + (n - 1) * (2 + w) + k - 1
                when(there, remote(view, view, row_send.at[s], row_recv.at[s], near["c"], start=False).wait_recv)

    def gates_step():
        cot[block(e), :] = cot_own[...]
        one_t[...] = one[...].astype(F32).T.astype(jnp.bfloat16)
        mixed_t[...] = mixed[...].astype(F32).T.astype(jnp.bfloat16)
        logits = across(rows_all[...], router[...])
        lane = lax.broadcasted_iota(jnp.int32, logits.shape, 1)
        logits = jnp.where(lane < 4 * n, logits, -1e30)
        top = jnp.max(logits, axis=-1, keepdims=True)
        ex = jnp.exp(logits - top)
        pr = ex / jnp.sum(ex, axis=-1, keepdims=True)
        gates[...] = pr * named[...].astype(F32)
        back[...] = jnp.zeros_like(back)
        routed[...] = jnp.zeros_like(routed)
        dot_sums[...] = jnp.zeros_like(dot_sums)
        ffn_own[...] = jnp.zeros_like(ffn_own)
        gn_own[...] = jnp.zeros_like(gn_own)
        r = lax.broadcasted_iota(jnp.int32, eye.shape, 0)
        c = lax.broadcasted_iota(jnp.int32, eye.shape, 1)
        eye[...] = jnp.where(r == c, 1.0, 0.0).astype(jnp.bfloat16)
        own = block(e)
        probs[...] = (across(rows_all[own, :], router[...]))

    def plane_view(i, o, h):
        if i < 12:
            k = hid // 2
            return exp_land[i % 3].at[i // 3, pl.ds(h * k, k), pl.ds(pl.multiple_of(o * width, width), width)]
        k = sh_land[i - 12].shape[0] // 2
        return sh_land[i - 12].at[pl.ds(h * k, k), pl.ds(pl.multiple_of((o * n + e) * 128, 128), 128)]

    def plane_own(i, h):
        if i < 12:
            k = hid // 2
            return ins[i % 3].at[i // 3, pl.ds(h * k, k)]
        k = sh_land[i - 12].shape[0] // 2
        return sh_ins[i - 12].at[pl.ds(h * k, k)]

    kinds = ("x0", "y1", "x1", "y0", "f0", "f1")

    def plane_copy(i, o, h, side, kind, own=False, start=True):
        s = 6 * i + kinds.index(kind)
        dst = plane_view(i, o, h)
        return remote(plane_own(i, h) if own else dst, dst, plane_send.at[s], plane_recv.at[s], near[side], start=start)

    def plane_step(i, s):
        if s == 0:
            plane_copy(i, d, 0, "x", "x0", own=True)
            plane_copy(i, d, 1, "y", "y1", own=True)
            plane_copy(i, d, 1, "x", "x1", own=True)
            plane_copy(i, d, 0, "y", "y0", own=True)
        elif s == 1:
            plane_copy(i, dx, 0, "x", "x0", start=False).wait_recv()
            plane_copy(i, dx, 0, "y", "f0")
            plane_copy(i, dy, 1, "x", "y1", start=False).wait_recv()
            plane_copy(i, dy, 1, "x", "f1")
        elif s == 2:
            plane_copy(i, dx, 1, "x", "x1", start=False).wait_recv()
            plane_copy(i, dy, 0, "x", "y0", start=False).wait_recv()
        else:
            plane_copy(i, dd, 0, "x", "f0", start=False).wait_recv()
            plane_copy(i, dd, 1, "x", "f1", start=False).wait_recv()

    def line_view(i, o, eo):
        return sh_land[i].at[:, pl.ds(pl.multiple_of((o * n + eo) * 128, 128), 128)]

    def line_step(i, b, k):
        o = (d, dx, dy, dd)[b]
        base = (i * 4 + b) * 2 * (n - 1)

        def copy(eo, side, hop, own=False, cond=None, start=True):
            s = base + (0 if side == "r" else n - 1) + hop - 1
            dst = line_view(i, o, eo)
            return remote(sh_ins[i] if own else dst, dst, line_send.at[s], line_recv.at[s], near[side], cond, start)

        if k == 0:
            copy(e, "r", 1, b == 0, after)
            copy(e, "l", 1, b == 0, before)
            return
        for side, eo, there, has in (("r", e - k, e >= k, after), ("l", e + k, e + k < n, before)):
            when(there, copy(eo, side, k, start=False).wait_recv)
            if k < n - 1:
                copy(eo, side, k + 1, cond=jnp.logical_and(there, has))

    loads = {}

    def load(j, arrays=(0, 1)):
        cs = []
        for a in arrays:
            for q, o in enumerate((d, dx, dy, dd)):
                cols = pl.ds(pl.multiple_of(o * width, width), width)
                src = ins[a].at[j] if q == 0 else exp_land[a].at[j, :, cols]
                c = pltpu.make_async_copy(src, weights.at[j % 2, a, :, cols], load_sem.at[j % 2, 4 * a + q])
                c.start()
                cs.append(c)
        loads[j, arrays] = cs

    def load_down(j):
        load(j, (2,))

    writes = []
    waiting = {}

    def write(src, dst, k):
        c = pltpu.make_async_copy(src, dst, out_sem.at[k])
        c.start()
        waiting[k] = c

    def free(k):
        if k in waiting:
            waiting.pop(k).wait()

    def ffn_front(rows, count, w):
        step = min(256, count)
        def pre(m, _):
            r = pl.ds(pl.multiple_of(m * step, step), step)
            x = rows[r, :]
            g = across(x, w(0))
            u = across(x, w(1))
            gpre[r, :] = g
            upre[r, :] = u
            act[r, :] = (g * jax.nn.sigmoid(g) * u).astype(jnp.bfloat16)
            return 0
        lax.fori_loop(0, count // step, pre, 0)

    def pre_step(j):
        for c in loads.pop((j, (0, 1))):
            c.wait()
        ffn_front(rows_all, alltoks, lambda a: weights[j % 2, a])

    def front(j):
        for c in loads.pop((j, (2,))):
            c.wait()
        free(3)
        lane = lax.broadcasted_iota(jnp.int32, (256, 128), 1)
        def out(k, _):
            m, c = k // 4, k % 4
            r = pl.ds(pl.multiple_of(m * 256, 256), 256)
            cols = pl.ds(pl.multiple_of(c * 512, 512), 512)
            piece = times(act[r, :], weights[j % 2, 2, :, cols]).astype(jnp.bfloat16).astype(F32)
            gt = gates[r, :][:, j : j + 1]
            ct = cot[r, cols].astype(F32)
            routed[r, cols] += gt * piece
            dot = jnp.sum(piece * ct, axis=-1, keepdims=True)
            dot_sums[r, :] += jnp.where(lane == e * here + j, dot, 0.0)
            copy_buf[r, cols] = (gt * ct).astype(jnp.bfloat16)
            return 0
        lax.fori_loop(0, alltoks // 256 * 4, out, 0)
        write(copy_buf, copies_out.at[j], 3)
        free(0)
        turned[0] = across(eye[...], act[...]).astype(jnp.bfloat16)
        write(turned.at[0], act_t.at[j], 0)

    def ffn_back(rows, count, w):
        step = min(256, count)
        def pre(m, _):
            r = pl.ds(pl.multiple_of(m * step, step), step)
            ga = across(rows[r, :], w(2))
            g, u = gpre[r, :], upre[r, :]
            s = jax.nn.sigmoid(g)
            grad[0, r, :] = (ga * u * (s * (1.0 + g * (1.0 - s)))).astype(jnp.bfloat16)
            grad[1, r, :] = (ga * (g * s)).astype(jnp.bfloat16)
            return 0
        lax.fori_loop(0, count // step, pre, 0)

    def back_step(j):
        ffn_back(copy_buf, alltoks, lambda a: weights[j % 2, a])

    def rows_step(j):
        def out(k, _):
            m, c = k // 4, k % 4
            r = pl.ds(pl.multiple_of(m * 256, 256), 256)
            cols = pl.ds(pl.multiple_of(c * 512, 512), 512)
            back[r, cols] += (times(grad[0, r, :], weights[j % 2, 0, :, cols])
                              + times(grad[1, r, :], weights[j % 2, 1, :, cols]))
            return 0
        lax.fori_loop(0, alltoks // 256 * 4, out, 0)
        for q, dst in ((0, ggp_t), (1, gup_t)):
            free(1 + q)
            turned[1 + q] = across(eye[...], grad[q]).astype(jnp.bfloat16)
            write(turned.at[1 + q], dst.at[j], 1 + q)

    def shared_load(v):
        cs = []
        for a in range(3):
            c = pltpu.make_async_copy(sh_land[a].at[pl.ds(v * hid, hid)], weights.at[v, a], load_sem.at[v, a])
            c.start()
            cs.append(c)
        loads["s", v] = cs

    def shared(v):
        for c in loads.pop(("s", v)):
            c.wait()
        free(3)
        w = lambda a: weights[v, a]
        own = block(e)
        ffn_front(normed, toks, w)
        for c in range(4):
            ffn_own[:, c * 512 : (c + 1) * 512] += times(act[0:toks, :], weights[v, 2, :, c * 512 : (c + 1) * 512])
        sact_t[pl.ds(v * hid, hid), :] = across(eye[...], act[0:toks, :]).astype(jnp.bfloat16)
        copy_buf[0:toks, :] = cot[own, :]
        ffn_back(copy_buf, toks, w)
        for c in range(4):
            gn_own[:, c * 512 : (c + 1) * 512] += (
                times(grad[0, 0:toks, :], weights[v, 0, :, c * 512 : (c + 1) * 512])
                + times(grad[1, 0:toks, :], weights[v, 1, :, c * 512 : (c + 1) * 512]))
        gsg[v] = grad[0, 0:toks, :]
        gsu[v] = grad[1, 0:toks, :]

    def settle():
        for i in range(3):
            pltpu.make_async_copy(sh_ins[i], sh_stage.at[i], stage_sem.at[i]).wait()
            pltpu.make_async_copy(sh_stage.at[i], line_view(i, d, e), stage_sem.at[i]).start()
        for i in range(3):
            pltpu.make_async_copy(sh_stage.at[i], line_view(i, d, e), stage_sem.at[i]).wait()

    def fold_start(q):
        src, base = ((back, 2), (routed, 2 + 2 * n))[q]
        for k, p in enumerate(peers + [e]):
            remote(src.at[block(p), theirs], fold_other.at[q, block(p)], pair_send.at[base + k], pair_recv.at[base + k], near["c"])
            if q == 1:
                s = 2 + n + k
                remote(dot_sums.at[block(p)], few_other.at[block(p)], pair_send.at[s], pair_recv.at[s], near["c"])

    def got(view, k):
        remote(view, view, pair_send.at[k], pair_recv.at[k], near["c"], start=False).wait_recv()

    def fold_shared():
        base = 2 + 3 * n
        for q, src in enumerate((gn_own, ffn_own)):
            remote(src.at[:, theirs], fold_own.at[q], pair_send.at[base + q], pair_recv.at[base + q], near["c"])

    def fold_lines(q):
        src, base = ((back, 2), (routed, 2 + 2 * n))[q]
        for k, p in enumerate(peers):
            got(fold_other.at[q, block(p)], base + k)
            fold_out[q, k] = (src[block(p), mine] + fold_other[q, block(p), :]).astype(jnp.bfloat16)
            s = 2 * (n - 1) * q + k
            remote(fold_out.at[q, k], fold_in.at[q, k], zsend.at[s], zrecv.at[s], {EXPERT: p})
            if q == 1:
                got(few_other.at[block(p)], 2 + n + k)
                few_out[k] = (dot_sums[block(p), :] + few_other[block(p), :]).astype(jnp.bfloat16)
                s = n - 1 + k
                remote(few_out.at[k], few_in.at[k], zsend.at[s], zrecv.at[s], {EXPERT: p})

    def fold_end():
        for src, q, base in ((back, 0, 2), (routed, 1, 2 + 2 * n)):
            got(fold_other.at[q, block(e)], base + n - 1)
            got(fold_own.at[q], 2 + 3 * n + q)
            dst, own = ((gn2, gn_own), (ffn, ffn_own))[q]
            dst[:, mine] = (src[block(e), mine] + fold_other[q, block(e), :]) + (own[:, mine] + fold_own[q])
        got(few_other.at[block(e)], 2 + n + n - 1)
        few[...] = dot_sums[block(e), :] + few_other[block(e), :]
        for k in range(n - 1):
            s = n - 1 + k
            remote(few_in.at[k], few_in.at[k], zsend.at[s], zrecv.at[s], near["c"], start=False).wait_recv()
            few[...] += few_in[k].astype(F32)
        for q, dst in ((0, gn2), (1, ffn)):
            for k in range(n - 1):
                s = 2 * (n - 1) * q + k
                remote(fold_in.at[q, k], fold_in.at[q, k], zsend.at[s], zrecv.at[s], near["c"], start=False).wait_recv()
                dst[:, mine] += fold_in[q, k].astype(F32)
            s = 2 + 3 * n + 2 + q
            remote(dst.at[:, mine], dst.at[:, mine], pair_send.at[s], pair_recv.at[s], near["c"])
        for q, dst in ((0, gn2), (1, ffn)):
            got(dst.at[:, theirs], 2 + 3 * n + 2 + q)

    steps = {"join": join, "tok": tok_step, "tokend": tok_end, "gates": gates_step, "plane": plane_step, "line": line_step,
             "load": load, "load_down": load_down, "pre": pre_step, "front": front, "back": back_step, "rows": rows_step, "shared_load": shared_load, "shared": shared,
             "settle": settle, "fold_start": fold_start, "fold_shared": fold_shared, "fold_lines": fold_lines,
             "fold_end": fold_end}
    items = middle_items(n, here)
    for name, *args in [items[k] for k in order]:
        steps[name](*args)
    for k in list(waiting):
        free(k)
    for c, cond in sends:
        when(cond, c.wait_send)


def middle(part, inp, gain, router, named, cot, one, mixed, experts, shared_t, n, order, cid):
    bf, dma, vm = jnp.bfloat16, pltpu.SemaphoreType.DMA, pltpu.VMEM
    toks, width = inp.shape
    here, hid, cut = experts[0].shape
    al = n * toks
    sh = shared_t[0].shape[0]
    S = jax.ShapeDtypeStruct
    vmem, anyspace = pl.BlockSpec(memory_space=pltpu.VMEM), pl.BlockSpec(memory_space=pl.ANY)
    outs = [
        (S((toks, width), F32), vmem), (S((toks, width), bf), vmem), (S((al, width), bf), vmem),
        (S((toks, 128), F32), vmem), (S((toks, 128), F32), vmem), (S((toks, width), F32), vmem),
        (S((toks, width), F32), vmem), (S((here, hid, al), bf), anyspace), (S((here, hid, al), bf), anyspace),
        (S((here, hid, al), bf), anyspace), (S((here, al, width), bf), anyspace),
        (S((2, toks, hid), bf), vmem), (S((2, toks, hid), bf), vmem), (S((2 * hid, toks), bf), vmem),
        (S((width, toks), bf), vmem), (S((width, toks), bf), vmem), (S((mixed.shape[1], toks), bf), vmem),
    ] + [(S((here, hid, width), bf), anyspace)] * 3 + [(S((sh, width), bf), anyspace)] * 3
    scratch = [
        vm((toks, width), F32), vm((2, 3, hid, width), bf), vm((al, 128), F32), vm((al, width), F32),
        vm((al, width), F32), vm((al, hid), F32), vm((al, hid), F32), vm((al, hid), bf), vm((2, al, hid), bf),
        vm((al, width), bf), vm((3, hid, al), bf), vm((hid, hid), bf), vm((3, sh, 128), bf), vm((al, 128), F32),
        vm((2, al, width // 2), F32), vm((2, toks, width // 2), F32), vm((2, n - 1, toks, width // 2), bf),
        vm((2, n - 1, toks, width // 2), bf), vm((al, 128), F32), vm((n - 1, toks, 128), bf),
        vm((n - 1, toks, 128), bf), vm((toks, width), F32), vm((toks, width), F32), vm((al, width), bf),
        dma((6 + 3 * n,)), dma((6 + 3 * n,)), dma((8 * (n - 1),)), dma((8 * (n - 1),)), dma((90,)), dma((90,)),
        dma((24 * (n - 1),)), dma((24 * (n - 1),)), dma((2, 12)), dma((4,)), dma((3,)),
        dma((3 * (n - 1),)), dma((3 * (n - 1),)),
    ]
    res = pl.pallas_call(
        functools.partial(middle_kernel, n, order),
        out_shape=[s for s, _ in outs], out_specs=[b for _, b in outs],
        in_specs=[vmem] * 8 + [anyspace] * 6,
        scratch_shapes=scratch,
        compiler_params=pltpu.CompilerParams(
            collective_id=cid, has_side_effects=True, vmem_limit_bytes=67043328),
    )(part, inp, gain, router, named, cot, one, mixed, *experts, *shared_t)
    return res[:17]


def rms_scale(vector):
    return lax.rsqrt(jnp.mean(vector * vector, axis=-1, keepdims=True) + epsilon)


def rope_tables(count, width):
    half_width = width // 2
    frequency = rope_base ** (-jnp.arange(half_width, dtype=jnp.float32) / half_width)
    angles = jnp.arange(count, dtype=jnp.float32)[:, None] * frequency[None, :]
    return (jnp.cos(angles)[:, None, :], jnp.sin(angles)[:, None, :])


def rotate(vector, cosine, sine_table):
    half_width = vector.shape[-1] // 2
    first_half = vector[..., :half_width]
    second_half = vector[..., half_width:]
    return jnp.concatenate(
        [
            first_half * cosine - second_half * sine_table,
            first_half * sine_table + second_half * cosine,
        ],
        axis=-1,
    )


def unrotate(vector, cosine, sine_table):
    half_width = vector.shape[-1] // 2
    first_half = vector[..., :half_width]
    second_half = vector[..., half_width:]
    return jnp.concatenate(
        [
            first_half * cosine + second_half * sine_table,
            second_half * cosine - first_half * sine_table,
        ],
        axis=-1,
    )


def dots(left, right, *dims):
    return lax.dot_general(left, right, dims, preferred_element_type=F32)


def silu_parts(before):
    sigmoid_val = jax.nn.sigmoid(before)
    return (before * sigmoid_val, sigmoid_val * (1.0 + before * (1.0 - sigmoid_val)))


def masked_scores(query_rot, key_rot, allowed):
    scores = dots(query_rot, key_rot, ((2,), (2,)), ((1,), (1,))) / math.sqrt(query_rot.shape[-1])
    return jnp.where(allowed[None], scores, masked_score)


def turn(array, by, axis):
    return lax.dynamic_slice_in_dim(
        jnp.concatenate([array, array], axis=axis), by, array.shape[axis], axis=axis)


def plain_middle(attn_part, input_f, gain_two, router_rows, named_all, grads_all, cotangent,
                 expert_weights, full_sgate, full_sup, full_sdown):
    here = lax.axis_index(EXPERT)
    local_gate, local_up, local_down = expert_weights
    experts_here = local_gate.shape[0]
    hidden_one = input_f + lax.psum(attn_part, TENSOR)
    normed_two = (hidden_one * rms_scale(hidden_one) * gain_two).astype(BF)
    rows_all = lax.all_gather(normed_two, EXPERT, axis=0, tiled=True)
    probs_all = jax.nn.softmax(dots(rows_all, router_rows, ((1,), (1,)), ((), ())), axis=-1)
    gates_here = lax.dynamic_slice_in_dim(
        probs_all * named_all, here * experts_here, experts_here, axis=1)
    gate_pre = dots(local_gate, rows_all, ((2,), (1,)), ((), ()))
    up_pre = dots(local_up, rows_all, ((2,), (1,)), ((), ()))
    silu_gate, slope_gate = silu_parts(gate_pre)
    act_t = (silu_gate * up_pre).astype(BF)
    part_rows = dots(act_t, local_down, ((1,), (1,)), ((0,), (0,))).astype(BF).astype(F32)
    routed = sum(gates_here[:, j : j + 1] * part_rows[j] for j in range(experts_here))
    grads_wide = grads_all.astype(F32)
    owner_grads = (jnp.transpose(gates_here)[:, :, None] * grads_wide[None]).astype(BF)
    gate_dots = jnp.sum(part_rows * grads_wide[None], axis=-1)
    dots_wide = lax.dynamic_update_slice(
        jnp.zeros_like(probs_all), jnp.transpose(gate_dots), (0, here * experts_here))
    grad_act = dots(local_down, owner_grads, ((2,), (2,)), ((0,), (0,)))
    ggp_t = (grad_act * up_pre * slope_gate).astype(BF)
    gup_t = (grad_act * silu_gate).astype(BF)
    grad_rows = dots(ggp_t, local_gate, ((0, 1), (0, 1)), ((), ()))
    grad_rows = grad_rows + dots(gup_t, local_up, ((0, 1), (0, 1)), ((), ()))
    shared_gpre = jnp.dot(normed_two, full_sgate, preferred_element_type=F32)
    shared_upre = jnp.dot(normed_two, full_sup, preferred_element_type=F32)
    silu_shared, slope_shared = silu_parts(shared_gpre)
    shared_act = (silu_shared * shared_upre).astype(BF)
    shared_part = jnp.dot(shared_act, full_sdown, preferred_element_type=F32)
    grad_sact = dots(cotangent, full_sdown, ((1,), (1,)), ((), ()))
    grad_sgate = (grad_sact * shared_upre * slope_shared).astype(BF)
    grad_sup = (grad_sact * silu_shared).astype(BF)
    own_rows = dots(grad_sgate, full_sgate, ((1,), (1,)), ((), ()))
    own_rows = own_rows + dots(grad_sup, full_sup, ((1,), (1,)), ((), ()))
    back = [lax.psum_scatter(v, EXPERT, scatter_dimension=0, tiled=True)
            for v in (grad_rows, routed, dots_wide)]
    grad_normed_two = lax.psum(back[0] + own_rows, TENSOR)
    ffn_total = lax.psum(back[1] + shared_part, TENSOR)
    dots_sum = lax.psum(back[2], TENSOR)
    router_probs = lax.dynamic_slice_in_dim(
        probs_all, here * normed_two.shape[0], normed_two.shape[0], axis=0)
    return (hidden_one, normed_two, rows_all, router_probs, dots_sum, grad_normed_two, ffn_total,
            act_t, ggp_t, gup_t, owner_grads, grad_sgate, grad_sup, shared_act.T)


def plain_scatter(dense, lefts, rights, extra, exp_left, rows_all, owner_grads):
    sums = []
    for k, ((kind, _), left, right) in enumerate(zip(dense, lefts, rights)):
        part = jnp.dot(left, right, preferred_element_type=F32)
        if k == len(dense) - 1:
            part = part + extra
        dim = 0 if kind == "rows" else 1
        sums.append(lax.psum_scatter(part, BOTH, scatter_dimension=dim, tiled=True))
    for left, right in zip(exp_left, (rows_all, rows_all, owner_grads)):
        dims = (((2,), (0,)), ((), ())) if right.ndim == 2 else (((2,), (1,)), ((0,), (0,)))
        part = dots(left, right, *dims).astype(BF)
        sums.append(lax.psum_scatter(part, DP, scatter_dimension=2, tiled=True).astype(F32))
    return sums


def body(
    block_input,
    attn_gain,
    query_weight,
    key_weight,
    value_weight,
    output_weight,
    ffn_gain,
    router_weight,
    expert_gate,
    expert_up,
    expert_down,
    shared_gate,
    shared_up,
    shared_down,
    segments,
    routes,
    cotangent,
):
    seq_len = block_input.shape[0]
    total_experts = router_weight.shape[1]
    owners, here = lax.axis_size(EXPERT), lax.axis_index(EXPERT)
    kernels = (output_weight.shape[1] % 128 == 0 and lax.axis_size(DP) == 4
               and total_experts <= 128 and seq_len == 128)
    expert_ids = jnp.arange(total_experts, dtype=jnp.int32)
    named = jnp.any(routes[:, :, None] == expert_ids[None, None, :], axis=1)
    small = jnp.concatenate([router_weight, attn_gain[:, None], ffn_gain[:, None]], axis=1).T
    flip_gate, flip_up = jnp.swapaxes(expert_gate, 1, 2), jnp.swapaxes(expert_up, 1, 2)
    named_low = named.astype(BF)
    if kernels:
        small = jnp.pad(small, ((0, -small.shape[0] % 32), (0, 0)))
        named_low = jnp.pad(named_low, ((0, 0), (0, 256 - total_experts)))
        arrays = (query_weight, key_weight, value_weight, output_weight, small, named_low)
        forms = ("rows",) * 3 + ("cols", "cols", "tokens")
        firsts = ("z",) * 3 + ("xy", "z", "xy")
        (full_query, full_key, full_value, full_output, full_small, named_all, sgate_t, sup_t) = gather(
            arrays, forms, firsts, owners, gather_starts, (shared_gate, shared_up))
    else:
        full_small = lax.all_gather(small, BOTH, axis=1, tiled=True)
        full_query = lax.all_gather(query_weight, BOTH, axis=0, tiled=True)
        full_key = lax.all_gather(key_weight, BOTH, axis=0, tiled=True)
        full_value = lax.all_gather(value_weight, BOTH, axis=0, tiled=True)
        full_output = lax.all_gather(output_weight, BOTH, axis=1, tiled=True)
        named_all = lax.all_gather(named_low, EXPERT, axis=0, tiled=True)
    named_all = named_all[:, :total_experts]
    router_rows = full_small[:total_experts]
    gain_one = full_small[total_experts].astype(F32)
    gain_two = full_small[total_experts + 1].astype(F32)
    heads_here = full_query.shape[1] // HD
    input_f = block_input.astype(F32)
    scale_one = rms_scale(input_f)
    normed_one = (input_f * scale_one * gain_one).astype(BF)
    cosine, sine_table = rope_tables(seq_len, HD)
    query_pre = jnp.dot(normed_one, full_query, preferred_element_type=F32).reshape(
        seq_len, heads_here, HD
    )
    key_pre = jnp.dot(normed_one, full_key, preferred_element_type=F32).reshape(
        seq_len, heads_here, HD
    )
    query_rot = rotate(query_pre, cosine, sine_table).astype(BF)
    key_rot = rotate(key_pre, cosine, sine_table).astype(BF)
    value_rows = (
        jnp.dot(normed_one, full_value, preferred_element_type=F32)
        .astype(BF)
        .reshape(seq_len, heads_here, HD)
    )
    position = jnp.arange(seq_len)
    segment_row = segments[0]
    allowed = (position[:, None] >= position[None, :]) & (
        segment_row[:, None] == segment_row[None, :]
    )
    scores = masked_scores(query_rot, key_rot, allowed)
    top_score = jnp.max(scores, axis=-1, keepdims=True)
    shifted = jnp.exp(scores - top_score)
    row_total = jnp.sum(shifted, axis=-1, keepdims=True)
    log_total = top_score + jnp.log(row_total)
    prob_low = (shifted / row_total).astype(BF)
    mixed_rows = (
        jnp.transpose(dots(prob_low, value_rows, ((2,), (0,)), ((0,), (1,))), (1, 0, 2))
        .astype(BF)
        .reshape(seq_len, heads_here * HD)
    )
    attn_part = jnp.dot(mixed_rows, full_output, preferred_element_type=F32)
    experts = (flip_gate, flip_up, expert_down)
    if kernels:
        first = here * expert_gate.shape[0]
        router_pad = jnp.pad(turn(router_rows, first, 0), ((0, 128 - total_experts), (0, 0)))
        named_pad = jnp.pad(turn(named_all, first, 1), ((0, 0), (0, 128 - total_experts)))
        (hidden_one, normed_two, rows_all, logits, dots_sum, grad_normed_two, ffn_total, act_t, ggp_t, gup_t,
         owner_grads, grad_sgate, grad_sup, shared_act_t, one_t, two_t, mixed_t) = middle(
            attn_part, block_input, gain_two[None], router_pad, named_pad, cotangent, normed_one,
            mixed_rows, experts, (sgate_t, sup_t, shared_down), owners, middle_order, 2)
        grad_sgate = jnp.concatenate([grad_sgate[0], grad_sgate[1]], axis=1)
        grad_sup = jnp.concatenate([grad_sup[0], grad_sup[1]], axis=1)
        router_probs = jax.nn.softmax(
            turn(logits[:, :total_experts], total_experts - first, 1), axis=-1)
        dots_sum = dots_sum[:, :total_experts]
    else:
        (hidden_one, normed_two, rows_all, router_probs, dots_sum, grad_normed_two, ffn_total, act_t, ggp_t, gup_t,
         owner_grads, grad_sgate, grad_sup, shared_act_t) = plain_middle(
            attn_part, input_f, gain_two, router_rows, named_all.astype(F32),
            lax.all_gather(cotangent, EXPERT, axis=0, tiled=True), cotangent,
            tuple(lax.all_gather(w, DP, axis=2, tiled=True) for w in experts),
            lax.all_gather(shared_gate, BOTH, axis=0, tiled=True),
            lax.all_gather(shared_up, BOTH, axis=0, tiled=True),
            lax.all_gather(shared_down, BOTH, axis=1, tiled=True))
        one_t, two_t, mixed_t = normed_one.T, normed_two.T, mixed_rows.T
    scale_two = rms_scale(hidden_one)
    block_output = (hidden_one + ffn_total).astype(BF)
    grad_out = cotangent.astype(F32)
    grad_rprobs = jnp.where(named, dots_sum, 0.0)
    grad_logits = (
        router_probs * (grad_rprobs - jnp.sum(grad_rprobs * router_probs, axis=-1, keepdims=True))
    ).astype(BF)
    grad_normed_two = grad_normed_two + dots(grad_logits, router_rows, ((1,), (0,)), ((), ()))
    ffn_gain_full = jnp.sum(grad_normed_two * hidden_one * scale_two, axis=0)
    weighted_two = grad_normed_two * gain_two
    cube_two = scale_two * scale_two * scale_two
    grad_hidden = (
        grad_out
        + scale_two * weighted_two
        - hidden_one * cube_two * jnp.mean(hidden_one * weighted_two, axis=-1, keepdims=True)
    )
    grad_attn = grad_hidden.astype(BF)
    grad_mixed = (
        dots(grad_attn, full_output, ((1,), (1,)), ((), ()))
        .astype(BF)
        .reshape(seq_len, heads_here, HD)
    )
    prob_again = jnp.exp(masked_scores(query_rot, key_rot, allowed) - log_total)
    grad_probs = dots(grad_mixed, value_rows, ((2,), (2,)), ((1,), (1,)))
    grad_scores = (
        prob_again * (grad_probs - jnp.sum(prob_again * grad_probs, axis=-1, keepdims=True))
    ).astype(BF)
    value_grad_rows = (
        jnp.transpose(dots(prob_again.astype(BF), grad_mixed, ((1,), (0,)), ((0,), (1,))), (1, 0, 2))
        .astype(BF)
        .reshape(seq_len, heads_here * HD)
    )
    inverse_root = 1.0 / math.sqrt(HD)
    grad_qrot = (
        jnp.transpose(dots(grad_scores, key_rot, ((2,), (0,)), ((0,), (1,))), (1, 0, 2))
        * inverse_root
    )
    grad_krot = (
        jnp.transpose(dots(grad_scores, query_rot, ((1,), (0,)), ((0,), (1,))), (1, 0, 2))
        * inverse_root
    )
    grad_qpre = (
        unrotate(grad_qrot, cosine, sine_table).astype(BF).reshape(seq_len, heads_here * HD)
    )
    grad_kpre = (
        unrotate(grad_krot, cosine, sine_table).astype(BF).reshape(seq_len, heads_here * HD)
    )
    grad_normed_one = dots(grad_qpre, full_query, ((1,), (1,)), ((), ()))
    grad_normed_one = grad_normed_one + dots(grad_kpre, full_key, ((1,), (1,)), ((), ()))
    grad_normed_one = grad_normed_one + dots(value_grad_rows, full_value, ((1,), (1,)), ((), ()))
    grad_normed_one = (
        pair_sum(grad_normed_one, 3) if kernels else lax.psum(grad_normed_one, TENSOR)
    )
    attn_gain_full = jnp.sum(grad_normed_one * input_f * scale_one, axis=0)
    weighted_one = grad_normed_one * gain_one
    cube_one = scale_one * scale_one * scale_one
    input_grad = (
        grad_hidden
        + scale_one * weighted_one
        - input_f * cube_one * jnp.mean(input_f * weighted_one, axis=-1, keepdims=True)
    )
    room = total_experts + 2 + (-(total_experts + 2) % 64)
    logits_t = jnp.pad(grad_logits.T, ((0, room - total_experts), (0, 0)))
    extra = jnp.concatenate([
        jnp.zeros((total_experts, D), F32), attn_gain_full[None], ffn_gain_full[None],
        jnp.zeros((room - total_experts - 2, D), F32)])
    lefts = (one_t, one_t, one_t, mixed_t, two_t, two_t, shared_act_t, logits_t)
    rights = (grad_qpre, grad_kpre, value_grad_rows, grad_attn, grad_sgate, grad_sup, cotangent, normed_two)
    exp_left = (ggp_t, gup_t, act_t)
    dense = ((("rows", "z"),) * 3
             + (("cols", "z"), ("rows", "z"), ("rows", "p"), ("cols", "p"), ("cols", "z")))
    if kernels:
        sums = scatter(
            dense, lefts, rights, extra, exp_left, rows_all, owner_grads, owners, scatter_order, 1)
    else:
        sums = plain_scatter(dense, lefts, rights, extra, exp_left, rows_all, owner_grads)
    (query_grad, key_grad, value_grad, output_grad, shared_gate_grad, shared_up_grad,
     shared_down_grad, small_grad, expert_gate_grad, expert_up_grad, expert_down_grad) = sums
    return (
        block_output,
        input_grad,
        small_grad[total_experts],
        query_grad,
        key_grad,
        value_grad,
        output_grad,
        small_grad[total_experts + 1],
        small_grad[:total_experts].T,
        jnp.swapaxes(expert_gate_grad, 1, 2),
        jnp.swapaxes(expert_up_grad, 1, 2),
        expert_down_grad,
        shared_gate_grad,
        shared_up_grad,
        shared_down_grad,
    )


def solution(mesh):
    return jax.shard_map(
        body,
        mesh=mesh,
        in_specs=(
            P((DP, EXPERT), None),
            P((DP, EXPERT)),
            P((DP, EXPERT), TENSOR),
            P((DP, EXPERT), TENSOR),
            P((DP, EXPERT), TENSOR),
            P(TENSOR, (DP, EXPERT)),
            P((DP, EXPERT)),
            P((DP, EXPERT), None),
            P(EXPERT, DP, TENSOR),
            P(EXPERT, DP, TENSOR),
            P(EXPERT, TENSOR, DP),
            P((DP, EXPERT), TENSOR),
            P((DP, EXPERT), TENSOR),
            P(TENSOR, (DP, EXPERT)),
            P((DP, EXPERT), None),
            P((DP, EXPERT), None),
            P((DP, EXPERT), None),
        ),
        out_specs=(
            P((DP, EXPERT), None),
            P((DP, EXPERT), None),
            P((DP, EXPERT)),
            P((DP, EXPERT), TENSOR),
            P((DP, EXPERT), TENSOR),
            P((DP, EXPERT), TENSOR),
            P(TENSOR, (DP, EXPERT)),
            P((DP, EXPERT)),
            P((DP, EXPERT), None),
            P(EXPERT, DP, TENSOR),
            P(EXPERT, DP, TENSOR),
            P(EXPERT, TENSOR, DP),
            P((DP, EXPERT), TENSOR),
            P((DP, EXPERT), TENSOR),
            P(TENSOR, (DP, EXPERT)),
        ),
        check_vma=False,
    )
```

```python
import functools
import math
import types

import jax
import jax.numpy as jnp
from jax import lax
from jax.experimental import pallas as pl
from jax.experimental.pallas import tpu as pltpu
from jax.sharding import PartitionSpec as P

MESH = pl.DeviceIdType.MESH
F32, BF = jnp.float32, jnp.bfloat16
DP, EXPERT, TENSOR = "dp", "expert", "tensor"
BOTH = (DP, EXPERT)
D = 2048
HD = 128


epsilon = 1e-06
rope_base = 10000.0
masked_score = -1e30
gather_starts = (1.91, 2.48, 3.88, 2.78, 2.0, 1.0)
scatter_order = (102, 91, 81, 101, 87, 49, 76, 82, 92, 50, 51, 0, 1, 31, 32, 22, 97, 41, 7, 58, 104, 42, 77, 96, 83, 59, 61, 86, 24, 13, 14, 40, 103, 52, 78, 89, 99, 2, 3, 67, 70, 98, 4, 79, 69, 68, 23, 5, 53, 43, 60, 72, 54, 16, 105, 15, 55, 71, 25, 74, 100, 34, 56, 33, 73, 6, 93, 94, 45, 80, 62, 18, 44, 27, 75, 63, 36, 38, 17, 29, 28, 88, 84, 95, 9, 35, 8, 64, 47, 26, 20, 46, 37, 65, 19, 90, 57, 85, 21, 30, 11, 10, 39, 66, 48, 12)
middle_order = (13, 8, 33, 113, 0, 9, 10, 14, 15, 57, 53, 91, 73, 37, 58, 59, 34, 35, 17, 18, 11, 12, 92, 19, 54, 55, 61, 77, 16, 3, 109, 99, 114, 81, 65, 66, 21, 25, 74, 67, 62, 36, 26, 27, 56, 69, 95, 100, 101, 82, 29, 30, 31, 93, 4, 115, 116, 110, 111, 20, 96, 97, 78, 28, 22, 23, 24, 94, 41, 63, 117, 5, 6, 7, 1, 68, 75, 76, 112, 98, 103, 32, 83, 84, 86, 60, 2, 70, 71, 72, 64, 102, 104, 127, 45, 42, 131, 38, 79, 80, 85, 87, 88, 89, 90, 105, 118, 135, 39, 40, 46, 49, 43, 128, 129, 106, 107, 108, 47, 121, 123, 44, 132, 119, 120, 122, 124, 125, 126, 136, 137, 50, 51, 52, 133, 134, 130, 139, 141, 48, 145, 138, 140, 142, 151, 143, 152, 144, 147, 146, 148, 149, 150, 153, 154)


class Leaf:
    def __init__(self, shape, dtype, form, first, n):
        self.shape, self.dtype, self.form, self.first, self.n = shape, dtype, form, first, n
        rows = shape[-2]
        if form == "rows":
            self.out = (4 * n * rows, shape[1])
        elif form == "cols":
            self.out = (shape[0], 4 * n * shape[1])
        elif form == "expert":
            self.out = (shape[0], shape[1], 4 * shape[2])
        elif form == "tokens":
            self.out = (n * rows, shape[1])

    def view(self, ref, d, e, half=None):
        if self.form == "rows":
            r = self.shape[0]
            s, k = (d * self.n + e) * r, r
            if half is not None:
                k = r // 2
                s = s + half * k
            return ref.at[pl.ds(pl.multiple_of(s, k), k), :]
        if self.form == "cols":
            c = self.shape[1]
            s = pl.multiple_of((d * self.n + e) * c, c)
            k = self.shape[0] // 2
            rows = slice(None) if half is None else pl.ds(half * k, k)
            return ref.at[rows, pl.ds(s, c)]
        if self.form == "tokens":
            r = self.shape[0]
            s = pl.multiple_of(e * r, r)
            if half is None:
                return ref.at[pl.ds(s, r), :]
            c = self.shape[1] // 2
            return ref.at[pl.ds(s, r), pl.ds(pl.multiple_of(half * c, c), c)]
        c = self.shape[2]
        k = self.shape[0] // 2
        heads = slice(None) if half is None else pl.ds(half * k, k)
        return ref.at[heads, :, pl.ds(pl.multiple_of(d * c, c), c)]

    def own(self, ref, half=None):
        if half is None:
            return ref
        if self.form == "tokens":
            c = self.shape[1] // 2
            return ref.at[:, pl.ds(pl.multiple_of(half * c, c), c)]
        k = self.shape[0] // 2
        return ref.at[pl.ds(half * k, k)]


def gather_kernel(leaves, n, starts, *refs):
    m = len(leaves)
    ins, plain, refs = refs[:m], refs[m : m + 2], refs[m + 2 :]
    outs, turned, refs = refs[:m], refs[m : m + 2], refs[m + 2 :]
    stages = refs[:m]
    in_sem, out_sem, send_sem, recv_sem = refs[m:]
    d, e, t = lax.axis_index(DP), lax.axis_index(EXPERT), lax.axis_index(TENSOR)
    dx = d + 1 - 2 * lax.rem(d, 2)
    dy = lax.rem(d + 2, 4)
    dd = lax.rem(dx + 2, 4)
    near = {"x": {DP: dx}, "y": {DP: dy}, "r": {EXPERT: e + 1}, "l": {EXPERT: e - 1},
            "c": {TENSOR: 1 - t}}
    has = {"r": e < n - 1, "l": e > 0}

    barrier = pltpu.get_barrier_semaphore()
    for side in ("x", "y", "c"):
        pl.semaphore_signal(barrier, inc=1, device_id=near[side], device_id_type=MESH)
    for side in ("r", "l"):
        @pl.when(has[side])
        def _():
            pl.semaphore_signal(barrier, inc=1, device_id=near[side], device_id_type=MESH)
    pl.semaphore_wait(barrier, 3 + has["r"].astype(jnp.int32) + has["l"].astype(jnp.int32))

    for i in range(m):
        pltpu.make_async_copy(ins[i], stages[i], in_sem.at[i]).start()

    count = [0]
    table = {}

    def slot(key):
        if key not in table:
            table[key] = len(table)
        return table[key]

    def copy(src, dst, side, key):
        k = slot(key)
        return pltpu.make_async_remote_copy(
            src_ref=src, dst_ref=dst, send_sem=send_sem.at[k], recv_sem=recv_sem.at[k],
            device_id=near[side], device_id_type=MESH)

    sends = []

    def send(i, dd_, ee_, half, side, key, own=False, cond=None):
        leaf = leaves[i]
        dst = leaf.view(outs[i], dd_, ee_, half)
        src = leaf.own(ins[i], half) if own else dst
        c = copy(src, dst, side, key)
        if cond is None:
            c.start()
        else:
            pl.when(cond)(c.start)
        sends.append((c, cond))

    def arrive(i, dd_, ee_, half, key, cond=None):
        leaf = leaves[i]
        dst = leaf.view(outs[i], dd_, ee_, half)
        c = copy(dst, dst, "x", key)
        if cond is None:
            c.wait_recv()
        else:
            pl.when(cond)(c.wait_recv)

    work = []

    def plane(i, ee_, at, tag, cond, own):
        def s0():
            for half, side in ((0, "x"), (1, "y"), (1, "x"), (0, "y")):
                send(i, d, ee_, half, side, (i, tag, half, side), own=own, cond=cond)
        def s1():
            arrive(i, dx, ee_, 0, (i, tag, 0, "x"), cond)
            send(i, dx, ee_, 0, "y", (i, tag, 0, "fy"), cond=cond)
            arrive(i, dy, ee_, 1, (i, tag, 1, "y"), cond)
            send(i, dy, ee_, 1, "x", (i, tag, 1, "fx"), cond=cond)
        def s2():
            arrive(i, dx, ee_, 1, (i, tag, 1, "x"), cond)
            arrive(i, dy, ee_, 0, (i, tag, 0, "y"), cond)
        def s3():
            arrive(i, dd, ee_, 0, (i, tag, 0, "fy"), cond)
            arrive(i, dd, ee_, 1, (i, tag, 1, "fx"), cond)
        for k, f in enumerate((s0, s1, s2, s3)):
            work.append((at + k, f))

    def line(i, dd_, at, tag, own, then=None):
        def s0():
            for side in ("r", "l"):
                send(i, dd_, e, None, side, (i, tag, side, 1), own=own, cond=has[side])
        work.append((at, s0))
        for k in range(1, n):
            def step(k=k):
                for side, o, there in (("r", e - k, e >= k), ("l", e + k, e + k < n)):
                    arrive(i, dd_, o, None, (i, tag, side, k), there)
                    if k < n - 1:
                        go = jnp.logical_and(there, has[side])
                        send(i, dd_, o, None, side, (i, tag, side, k + 1), cond=go)
            work.append((at + k, step))

    def tokens(i, at):
        def s0():
            for side in ("r", "l"):
                send(i, d, e, t, side, (i, side, 1), own=True, cond=has[side])
        work.append((at, s0))
        for k in range(1, n):
            def step(k=k):
                for side, o, there in (("r", e - k, e >= k), ("l", e + k, e + k < n)):
                    arrive(i, d, o, t, (i, side, k), there)
                    if k < n - 1:
                        go = jnp.logical_and(there, has[side])
                        send(i, d, o, t, side, (i, side, k + 1), cond=go)
                    send(i, d, o, t, "c", (i, "c", side, k), cond=there)
            def last(k=k):
                for side, o, there in (("r", e - k, e >= k), ("l", e + k, e + k < n)):
                    arrive(i, d, o, 1 - t, (i, "c", side, k), there)
            work.append((at + k, step))
            work.append((at + k + 1, last))

    for i, leaf in enumerate(leaves):
        at = starts[i]
        if leaf.form == "tokens":
            tokens(i, at)
            continue
        if leaf.form == "expert":
            plane(i, 0, at, "p", None, True)
        elif leaf.first == "xy":
            plane(i, e, at, "p", None, True)
            line(i, d, at, "z0", True)
            line(i, dx, at + 2.2, "zx", False)
            line(i, dy, at + 2.2, "zy", False)
            line(i, dd, at + 3.2, "zd", False)
        else:
            plane(i, e, at, "p", None, True)
            line(i, d, at, "z0", True)
            for k in range(1, n):
                plane(i, e - k, at + k + 0.5, ("pr", k), e >= k, False)
                plane(i, e + k, at + k + 0.5, ("pl", k), e + k < n, False)

    def settle():
        for a, b in zip(plain, turned):
            b[...] = a[...].astype(F32).T.astype(b.dtype)
        for i in range(m):
            pltpu.make_async_copy(ins[i], stages[i], in_sem.at[i]).wait()
            pltpu.make_async_copy(stages[i], leaves[i].view(outs[i], d, e), out_sem.at[i]).start()
    work.append((1.2, settle))
    for _, f in sorted(work, key=lambda w: w[0]):
        f()
    for c, cond in sends:
        if cond is None:
            c.wait_send()
        else:
            pl.when(cond)(c.wait_send)
    for i in range(m):
        pltpu.make_async_copy(stages[i], leaves[i].view(outs[i], d, e), out_sem.at[i]).wait()
    assert len(table) <= recv_sem.shape[0], len(table)


def gather(arrays, forms, firsts, n, starts, plain):
    leaves = [Leaf(a.shape, a.dtype, f, o, n) for a, f, o in zip(arrays, forms, firsts)]
    total = 0
    for leaf in leaves:
        plane, line = 6, 2 * (n - 1)
        if leaf.form == "tokens":
            total += 2 * line
            continue
        total += plane if leaf.form == "expert" else plane + 4 * line if leaf.first == "xy" else plane * (2 * n - 1) + line
    m = len(leaves)
    anyspace, vmem = pl.BlockSpec(memory_space=pl.ANY), pl.BlockSpec(memory_space=pltpu.VMEM)
    return pl.pallas_call(
        functools.partial(gather_kernel, leaves, n, starts),
        out_shape=[jax.ShapeDtypeStruct(leaf.out, leaf.dtype) for leaf in leaves] + [
            jax.ShapeDtypeStruct(v.shape[::-1], v.dtype) for v in plain],
        in_specs=[anyspace] * m + [vmem] * 2,
        out_specs=[anyspace] * m + [vmem] * 2,
        scratch_shapes=[pltpu.VMEM(leaf.shape, leaf.dtype) for leaf in leaves] + [
            pltpu.SemaphoreType.DMA((m,)), pltpu.SemaphoreType.DMA((m,)),
            pltpu.SemaphoreType.DMA((total,)), pltpu.SemaphoreType.DMA((total,))],
        compiler_params=pltpu.CompilerParams(
            collective_id=0, has_side_effects=True, vmem_limit_bytes=60 << 20),
    )(*arrays, *plain)


message_rows = 5632
ring_slots = {"x": 4, "y": 4, "z": 6}


def scatter_items(dense, units, n):
    ends = [k // 2 if k % 2 == 0 else n - 1 - k // 2 for k in range(n)]
    items = [("a", k, "", 0) for k in range(4)]
    for i, (_, first) in enumerate(dense):
        names = [("z", t) for t in ends] if first == "z" else []
        names += [("p", s) for s in ("y1", "x1", "x2", "y2")]
        names += [("z", t) for t in ends] if first != "z" else []
        items += [("d", i) + name for name in names] + [("d", i, "out", 0)]
    for u in range(units):
        items += [("e", u, "p", s) for s in ("y1", "x1", "x2", "y2")] + [("e", u, "out", 0)]
    return items


def scatter_uses(item, m):
    kind, i = item[:2]
    if kind == "a":
        return (("hidden", "back", "few", "named", "gain_two", "router", "cot", "normed"),
                ("q", "k", "v", "cos", "sin", "mask"), (), ("inp", "gain_one"))[i]
    if kind == "e":
        return (("ggp", "rows_all"), ("gup", "rows_all"), ("act", "cot_all", "gates"))[i // 2]
    return (("one_t",), ("one_t",), ("one_t",), ("mixed_t",), ("two_t", "gsg"), ("two_t", "gsu"),
            ("sact_t", "cot"), ("normed",))[i]


def scatter_kernel(dense, units, n, order, names, experts, *refs):
    m = len(dense)
    c_ = len(names)
    given = dict(zip(names, refs[:c_]))
    w_out, w_qkv = refs[c_], refs[c_ + 1 : c_ + 4]
    refs = refs[c_ + 4 :]
    box, refs = types.SimpleNamespace(**dict(zip(names, refs[-c_:]))), refs[:-c_]
    (in_sem, logits_t, gq, gk, gv, gattn, extra, gm, wbuf, gh, part, other, rhs, w_sem, pair_send, pair_recv,
     small_out) = refs[-17:]
    refs = refs[:-17]
    own_grads = (gq, gk, gv)
    lefts = (box.one_t,) * 3 + (box.mixed_t, box.two_t, box.two_t, box.sact_t, logits_t)
    rights = own_grads + (gattn, box.gsg, box.gsu, box.cot, box.normed)
    exp_left = (box.ggp, box.gup, box.act)
    rows_all = box.rows_all
    here_yet = set()

    def fetch(name):
        k = names.index(name)
        return pltpu.make_async_copy(given[name], getattr(box, name), in_sem.at[k])

    def need(item):
        for name in scatter_uses(item, m):
            if name not in here_yet:
                here_yet.add(name)
                fetch(name).wait()

    steps = scatter_items(dense, units, n)
    steps = [steps[k] for k in order] if order else steps
    for name in dict.fromkeys(v for it in steps for v in scatter_uses(it, m)):
        fetch(name).start()
    input_out, refs = refs[m + 3], refs[: m + 3] + refs[m + 4 :]
    outs, refs = refs[: m + 3], refs[m + 3 :]
    landed, refs = refs[: 3 * m + 2], refs[3 * m + 2 :]
    bufs = dict(zip("xyz", refs[:3]))
    held, tall, wide = refs[3:6]
    stage_sem, load_sem, recv_sem = refs[6:9]
    send_sems = dict(zip("xyz", refs[9:12]))
    d, e = lax.axis_index("dp"), lax.axis_index("expert")
    dx = d + 1 - 2 * lax.rem(d, 2)
    dy = lax.rem(d + 2, 4)
    dd = lax.rem(dx + 2, 4)
    after, before = e < n - 1, e > 0

    barrier = pltpu.get_barrier_semaphore()
    partner = {"tensor": 1 - lax.axis_index("tensor")}
    for dev in ({"dp": dx}, {"dp": dy}, partner):
        pl.semaphore_signal(barrier, inc=1, device_id=dev, device_id_type=MESH)
    for cond, dev in ((after, {"expert": e + 1}), (before, {"expert": e - 1})):
        @pl.when(cond)
        def _():
            pl.semaphore_signal(barrier, inc=1, device_id=dev, device_id_type=MESH)
    pl.semaphore_wait(barrier, 3 + after.astype(jnp.int32) + before.astype(jnp.int32))
    held[...] = jnp.zeros_like(held)

    def when(cond, f):
        if cond is None:
            f()
        else:
            pl.when(cond)(f)

    sems = {}

    def sem_of(key, count=1):
        if key not in sems:
            sems[key] = sum(c for _, c in sems.values()), count
        return sems[key][0]

    turns = {"x": 0, "y": 0, "z": 0}
    pending = {}

    def slot(side):
        k = turns[side] % ring_slots[side]
        turns[side] += 1
        if (side, k) in pending:
            c, cond = pending.pop((side, k))
            when(cond, c.wait_send)
        return k

    def send(side, k, rows, dst, sem, dev, cond=None):
        c = pltpu.make_async_remote_copy(
            src_ref=bufs[side].at[k, pl.ds(0, rows)], dst_ref=dst,
            send_sem=send_sems[side].at[k], recv_sem=recv_sem.at[sem],
            device_id=dev, device_id_type=MESH)
        when(cond, c.start)
        pending[(side, k)] = (c, cond)

    seen = set()

    def arrived(key, view, sem, cond=None):
        if key in seen:
            return
        seen.add(key)
        c = pltpu.make_async_remote_copy(
            src_ref=view, dst_ref=view, send_sem=recv_sem.at[sem], recv_sem=recv_sem.at[sem],
            device_id={"dp": dx}, device_id_type=MESH)
        when(cond, c.wait_recv)

    class Loads:
        def __init__(self):
            self.list = []

        def add(self, src, k, off, cond=None):
            rows = src.shape[0]
            c = pltpu.make_async_copy(src, held.at[k, pl.ds(off, rows)], load_sem.at[len(self.list)])
            when(cond, c.start)
            self.list.append((c, cond))

        def wait(self):
            for c, cond in self.list:
                when(cond, c.wait)

    def dense_piece(i, d_, e_, half, put):
        kind = dense[i][0]
        block = d_ * n + e_
        if kind == "rows":
            width = rights[i].shape[1]
            r = lefts[i].shape[0] // (4 * n)
            left = lefts[i][pl.ds(pl.multiple_of(block * r + half * (r // 2), r // 2), r // 2), :]
            for c in range(0, width, 256):
                w = min(256, width - c)
                res = jnp.dot(left, rights[i][:, c : c + w], preferred_element_type=F32)
                for k in range(0, w, 128):
                    put((c + k) // 128 * (r // 2), res[:, k : k + 128], c + k)
        else:
            half_rows = lefts[i].shape[0] // 2
            right = rights[i][:, pl.ds(pl.multiple_of(block * 128, 128), 128)]
            step = half_rows // 2
            for r in range(0, half_rows, step):
                left = lefts[i][pl.ds(pl.multiple_of(half * half_rows + r, 16), step), :]
                res = jnp.dot(left, right, preferred_element_type=F32)
                if i == m - 1:
                    at = pl.ds(pl.multiple_of(half * half_rows + r, 16), step)
                    res = res + extra[at, pl.ds(pl.multiple_of(block * 128, 128), 128)]
                put(r, res, 0)

    def half_rows_of(i):
        if dense[i][0] == "rows":
            return lefts[i].shape[0] // (8 * n) * rights[i].shape[1] // 128
        return lefts[i].shape[0] // 2

    def total(value, row, adds):
        rows = value.shape[0]
        for k, off, flag in adds:
            more = held[k, pl.ds(pl.multiple_of(off + row, 16), rows), :].astype(F32)
            value = value + (more if flag is None else jnp.where(flag, more, 0.0))
        return value

    def into(side, k, base, adds):
        def put(row, value, col):
            value = total(value, row, adds)
            start = pl.multiple_of(base + row, 16)
            bufs[side][k, pl.ds(start, value.shape[0]), :] = value.astype(jnp.bfloat16)
        return put

    out_busy = {}

    def out_wait(which):
        if which in out_busy:
            out_busy.pop(which).wait()

    def dense_step(i, stage, arg):
        z_land, first_land, second_land = landed[3 * i : 3 * i + 3]
        z_first = dense[i][1] == "z"
        hb = half_rows_of(i)
        z_rows = (8 if z_first else 2) * hb
        z_sem = sem_of(("z", i), 2 * n)
        groups = 1 if z_first else n
        p_sem = {s: sem_of((s, i)) for s in ("y1", "x1", "x2", "y2")}
        place = {"y1": (first_land, 0, 2), "x1": (first_land, 1, 2), "x2": (second_land, 0, 1), "y2": (second_land, 1, 1)}

        def view(s, g0, gs, sub):
            land, which, pieces = place[s]
            if sub is None:
                return land.at[which, pl.ds(0, groups * pieces * hb)]
            return land.at[which, pl.ds(pl.multiple_of((g0 * pieces + sub) * hb, hb), gs * hb)]

        def plane_arrived(s):
            arrived((s, i), view(s, 0, 0, None), p_sem[s])

        def own_line(ld, k, off, d_, half, rows):
            for side, there in ((0, after), (1, before)):
                arrived(("own", i, side), z_land.at[side, e], z_sem + side * n + e, there)
                src = z_land.at[side, e, pl.ds(pl.multiple_of((2 * d_ + half) * hb, hb), rows)]
                ld.add(src, k + side, off, there)

        def plane_out(ld, g):
            for s in ("y1", "x1", "x2", "y2"):
                plane_arrived(s)
            ld.add(view("y1", g, 1, 1), 2, 0)
            ld.add(view("x1", g, 1, 1), 2, hb)
            ld.add(view("x2", g, 1, 0), 3, 0)
            ld.add(view("y2", g, 1, 0), 3, hb)

        if stage == "z":
            t = arg
            side = 1 - (e + n - t) // n
            more = jnp.logical_or(jnp.logical_and(e > t, after), jnp.logical_and(e < t, before))
            cond = e != t
            k = slot("z")
            def go():
                ld = Loads()
                land = z_land.at[side, t]
                arrived(("pass", i, t), land, z_sem + side * n + t, more)
                ld.add(land, 0, 0, more)
                if not z_first:
                    plane_out(ld, t)
                ld.wait()
                if z_first:
                    def one(h, _):
                        dense_piece(i, h // 2, t, h % 2, into("z", k, h * hb, [(0, h * hb, more)]))
                        return 0
                    lax.fori_loop(0, 8, one, 0)
                else:
                    def one(h, _):
                        dense_piece(i, d, t, h, into("z", k, h * hb, [(0, h * hb, more), (2, h * hb, None), (3, h * hb, None)]))
                        return 0
                    lax.fori_loop(0, 2, one, 0)
            if not z_first:
                for s in ("y1", "x1", "x2", "y2"):
                    plane_arrived(s)
            pl.when(cond)(go)
            send("z", k, z_rows, z_land.at[side, t], z_sem + side * n + t, {"expert": e - 1 + 2 * side}, cond)
        elif stage == "p":
            s = arg
            link = s[0]
            dev = {"dp": dy if link == "y" else dx}
            half = 0 if s in ("y1", "x2") else 1
            k = slot(link)
            ld = Loads()
            if s in ("y1", "x1"):
                owners = (dd, dy if link == "y" else dx)
                if z_first:
                    for q, o in enumerate(owners):
                        own_line(ld, 0, q * hb, o, half, hb)
                    ld.wait()
                    for q, o in enumerate(owners):
                        dense_piece(i, o, e, half, into(link, k, q * hb, [(0, q * hb, after), (1, q * hb, before)]))
                else:
                    def one(g, _):
                        for q, o in enumerate(owners):
                            dense_piece(i, o, g, half, into(link, k, (2 * g + q) * hb, []))
                        return 0
                    lax.fori_loop(0, n, one, 0)
                send(link, k, groups * 2 * hb, view(s, 0, 0, None), p_sem[s], dev)
            else:
                o = dx if link == "x" else dy
                prior = "y1" if s == "x2" else "x1"
                plane_arrived(prior)
                if z_first:
                    own_line(ld, 0, 0, o, half, hb)
                    ld.add(view(prior, 0, 1, 0), 2, 0)
                    ld.wait()
                    dense_piece(i, o, e, half, into(link, k, 0, [(0, 0, after), (1, 0, before), (2, 0, None)]))
                else:
                    ld.add(view(prior, 0, 0, None), 2, 0)
                    ld.wait()
                    def one(g, _):
                        dense_piece(i, o, g, half, into(link, k, g * hb, [(2, 2 * g * hb, None)]))
                        return 0
                    lax.fori_loop(0, n, one, 0)
                send(link, k, groups * hb, view(s, 0, 0, None), p_sem[s], dev)
        else:
            ld = Loads()
            if z_first:
                own_line(ld, 0, 0, d, 0, 2 * hb)
                plane_out(ld, 0)
            else:
                for side, there in ((0, after), (1, before)):
                    arrived(("own", i, side), z_land.at[side, e], z_sem + side * n + e, there)
                    ld.add(z_land.at[side, e], side, 0, there)
                plane_out(ld, e)
            rows = dense[i][0] == "rows"
            which = "wide" if rows else "slim"
            out_wait(which)
            ld.wait()
            def one(h, _):
                adds = [(0, h * hb, after), (1, h * hb, before), (2, h * hb, None), (3, h * hb, None)]
                def put(row, value, col):
                    value = total(value, row, adds)
                    if rows:
                        r = value.shape[0]
                        wide[pl.ds(pl.multiple_of(h * r, r), r), col : col + 128] = value
                    else:
                        small_out[pl.ds(pl.multiple_of(h * hb + row, 16), value.shape[0]), :] = value
                dense_piece(i, d, e, h, put)
                return 0
            lax.fori_loop(0, 2, one, 0)
            if rows:
                src = wide.at[:, pl.ds(0, outs[i].shape[1])]
            else:
                src = small_out.at[pl.ds(0, outs[i].shape[0])]
            c = pltpu.make_async_copy(src, outs[i], stage_sem.at[0 if rows else 3])
            c.start()
            out_busy[which] = c

    first_exp, second_exp = landed[3 * m], landed[3 * m + 1]

    def expert_step(u, stage, s):
        a, q = u // 2, u % 2
        rows, width = exp_left[a].shape[1], outs[m + a].shape[2]
        tiles = width // 128
        piece = rows * tiles
        step = rows // 4
        sem = {s_: sem_of((s_, "e", u)) for s_ in ("y1", "x1", "x2", "y2")}
        place = {"y1": (first_exp, 0, 2), "x1": (first_exp, 1, 2), "x2": (second_exp, 0, 1), "y2": (second_exp, 1, 1)}

        def view(s_, sub=None):
            land, which, pieces = place[s_]
            if sub is None:
                return land.at[u, which]
            return land.at[u, which, pl.ds(sub * piece, piece)]

        def one_piece(j, d_, put):
            if a == 2:
                for r in range(0, rhs.shape[0], 128):
                    gate = box.gates[r : r + 128, :][:, j : j + 1]
                    ct = box.cot_all[r : r + 128, pl.ds(pl.multiple_of(d_ * width, 128), width)]
                    rhs[r : r + 128, :] = (gate * ct.astype(F32)).astype(jnp.bfloat16)
            def body(r, _):
                left = exp_left[a][j, pl.ds(pl.multiple_of(r * step, 16), step), :]
                cols = pl.ds(pl.multiple_of(d_ * width, 128), width)
                right = rhs[...] if a == 2 else rows_all[:, cols]
                res = jnp.dot(left, right, preferred_element_type=F32)
                for c in range(tiles):
                    put(c * rows + r * step, res[:, c * 128 : (c + 1) * 128], (r * step, c * 128))
                return 0
            lax.fori_loop(0, 4, body, 0)

        def get(s_):
            arrived((s_, "e", u), view(s_), sem[s_])

        ld = Loads()
        if stage == "p":
            link = s[0]
            dev = {"dp": dy if link == "y" else dx}
            j = q if s in ("y1", "x2") else q + 2
            k = slot(link)
            if s in ("y1", "x1"):
                for b, o in enumerate((dd, dy if link == "y" else dx)):
                    one_piece(j, o, into(link, k, b * piece, []))
                send(link, k, 2 * piece, view(s), sem[s], dev)
            else:
                prior = "y1" if s == "x2" else "x1"
                get(prior)
                ld.add(view(prior, 0), 0, 0)
                ld.wait()
                one_piece(j, dx if link == "x" else dy, into(link, k, 0, [(0, 0, None)]))
                send(link, k, piece, view(s), sem[s], dev)
        else:
            for b, (j, one, two) in enumerate(((q, "y1", "x2"), (q + 2, "x1", "y2"))):
                get(one)
                get(two)
                ld.add(view(one, 1), 2 * b, 0)
                ld.add(view(two, 0), 2 * b + 1, 0)
            out_wait("tall")
            ld.wait()
            for b, j in enumerate((q, q + 2)):
                adds = [(2 * b, 0, None), (2 * b + 1, 0, None)]
                def put(row, value, at):
                    value = total(value, row, adds)
                    r, c = at
                    tall[b, pl.ds(pl.multiple_of(r, 16), value.shape[0]), c : c + 128] = value
                one_piece(j, d, put)
            cs = [pltpu.make_async_copy(tall.at[b, pl.ds(0, rows), pl.ds(0, width)], outs[m + a].at[q + 2 * b], stage_sem.at[1 + b]) for b in range(2)]
            for c in cs:
                c.start()
            class Both:
                def wait(self):
                    for c in cs:
                        c.wait()
            out_busy["tall"] = Both()

    width_all = gh.shape[1]
    chunk = wbuf.shape[1]
    plan = [w_out.at[:, pl.ds(c * chunk, chunk)] for c in range(width_all // chunk)]
    plan += [w.at[pl.ds(c * chunk, chunk)] for c in range(width_all // chunk) for w in w_qkv]

    def weight(k):
        return pltpu.make_async_copy(plan[k], wbuf.at[k % 2], w_sem.at[k % 2])

    def a_t_b(a, b):
        return lax.dot_general(a, b, (((1,), (1,)), ((), ())), preferred_element_type=F32)

    def attn_step(k):
        if k == 0:
            weight(0).start()
            weight(1).start()
            logits = a_t_b(box.normed[...], box.router[...])
            lane = lax.broadcasted_iota(jnp.int32, logits.shape, 1)
            logits = jnp.where(lane < experts, logits, -1e30)
            ex = jnp.exp(logits - jnp.max(logits, axis=-1, keepdims=True))
            probs = ex / jnp.sum(ex, axis=-1, keepdims=True)
            grads = jnp.where(box.named[...] > 0.0, box.few[...], 0.0)
            grads = probs * (grads - jnp.sum(grads * probs, axis=-1, keepdims=True))
            logits_t[...] = grads.T[: logits_t.shape[0], :].astype(jnp.bfloat16)
            extra[...] = jnp.zeros_like(extra)
            gains = jnp.zeros((1, width_all), F32)
            for r in range(0, gh.shape[0], 32):
                p = slice(r, r + 32)
                low = grads[p].astype(jnp.bfloat16)
                gn = box.back[p, :] + jnp.dot(low, box.router[...], preferred_element_type=F32)
                h = box.hidden[p, :]
                scale = lax.rsqrt(jnp.mean(h * h, axis=-1, keepdims=True) + epsilon)
                gains = gains + jnp.sum(gn * h * scale, axis=0, keepdims=True)
                w = gn * box.gain_two[...]
                g = (box.cot[p, :].astype(F32) + scale * w
                     - h * (scale * scale * scale) * jnp.mean(h * w, axis=-1, keepdims=True))
                gh[p, :] = g
                gattn[p, :] = g.astype(jnp.bfloat16)
            extra[experts + 1 : experts + 2, :] = gains
        elif k == 1:
            count = width_all // chunk
            for c in range(count):
                weight(c).wait()
                piece = a_t_b(gattn[:, c * chunk : (c + 1) * chunk], wbuf[c % 2])
                weight(c + 2).start()
                part[:, : piece.shape[1]] = piece if c == 0 else part[:, : piece.shape[1]] + piece
            gm[...] = part[:, : gm.shape[1]].astype(jnp.bfloat16)
            root = 1.0 / math.sqrt(HD)
            for h in range(gm.shape[1] // HD):
                cols = slice(h * HD, (h + 1) * HD)
                q, kk, v, g = box.q[:, cols], box.k[:, cols], box.v[:, cols], gm[:, cols]
                scores = a_t_b(q, kk) / math.sqrt(HD)
                scores = jnp.where(box.mask[...] > 0.0, scores, masked_score)
                ex = jnp.exp(scores - jnp.max(scores, axis=-1, keepdims=True))
                prob = ex / jnp.sum(ex, axis=-1, keepdims=True)
                gp = a_t_b(g, v)
                gs = prob * (gp - jnp.sum(prob * gp, axis=-1, keepdims=True))
                gv[:, cols] = jnp.dot(prob.T.astype(jnp.bfloat16), g, preferred_element_type=F32).astype(jnp.bfloat16)
                for dst, left, right in ((gq, gs, kk), (gk, gs.T, q)):
                    u = jnp.dot(left.astype(jnp.bfloat16), right, preferred_element_type=F32) * root
                    u = u * box.cos[...] + pltpu.roll(u, HD // 2, 1) * box.sin[...]
                    dst[:, cols] = u.astype(jnp.bfloat16)
        elif k == 2:
            base = width_all // chunk
            for c in range(width_all // chunk):
                cols = slice(c * chunk, (c + 1) * chunk)
                for j in range(3):
                    i = base + 3 * c + j
                    weight(i).wait()
                    piece = a_t_b(own_grads[j][...], wbuf[i % 2])
                    if i + 2 < len(plan):
                        weight(i + 2).start()
                    part[:, cols] = piece if j == 0 else part[:, cols] + piece
            pair_copy().start()
        else:
            pair_copy().wait_recv()
            gains = jnp.zeros((1, width_all), F32)
            for r in range(0, gh.shape[0], 32):
                p = slice(r, r + 32)
                gn = part[p, :] + other[p, :]
                x = box.inp[p, :].astype(F32)
                scale = lax.rsqrt(jnp.mean(x * x, axis=-1, keepdims=True) + epsilon)
                gains = gains + jnp.sum(gn * x * scale, axis=0, keepdims=True)
                w = gn * box.gain_one[...]
                gh[p, :] = (gh[p, :] + scale * w
                            - x * (scale * scale * scale) * jnp.mean(x * w, axis=-1, keepdims=True))
            extra[experts : experts + 1, :] = gains
            c = pltpu.make_async_copy(gh, input_out, stage_sem.at[4])
            c.start()
            out_busy["input"] = c

    def pair_copy():
        return pltpu.make_async_remote_copy(
            src_ref=part, dst_ref=other, send_sem=pair_send, recv_sem=pair_recv,
            device_id=partner, device_id_type=MESH)

    for item in steps:
        kind, i, stage, arg = item
        need(item)
        if kind == "a":
            attn_step(i)
        else:
            (dense_step if kind == "d" else expert_step)(i, stage, arg)
    pair_copy().wait_send()
    for c, cond in pending.values():
        when(cond, c.wait_send)
    for which in list(out_busy):
        out_wait(which)
    assert sum(c for _, c in sems.values()) <= recv_sem.shape[0]


def scatter(dense, given, weights, experts, n, order, cid):
    m, units = len(dense), 6
    bf, dma, vm = jnp.bfloat16, pltpu.SemaphoreType.DMA, pltpu.VMEM
    toks, width = given["hidden"].shape
    heads = given["q"].shape[1]
    room = experts + 2 + (-(experts + 2) % 64)
    left = dict(zip(range(m), ("one_t", "one_t", "one_t", "mixed_t", "two_t", "two_t", "sact_t")))
    outs, landed = [], []
    for i, (kind, first) in enumerate(dense):
        rows = given[left[i]].shape[0] if i in left else room
        if kind == "rows":
            r = rows // (4 * n)
            cols = heads if i < 3 else given["gsg"].shape[1]
            shape, hb = (r, cols), r // 2 * cols // 128
        else:
            shape, hb = (rows, 128), rows // 2
        outs.append(jax.ShapeDtypeStruct(shape, F32))
        g, z = (1, 8) if first == "z" else (n, 2)
        landed += [jax.ShapeDtypeStruct((2, n, z * hb, 128), bf),
                   jax.ShapeDtypeStruct((2, g * 2 * hb, 128), bf),
                   jax.ShapeDtypeStruct((2, g * hb, 128), bf)]
    here, rows = given["act"].shape[:2]
    cut = width // 4
    tall_rows = max(o.shape[0] for o in outs)
    wide_cols = max(o.shape[1] for o in outs)
    outs += [jax.ShapeDtypeStruct((here, rows, cut), F32)] * 3
    outs.append(jax.ShapeDtypeStruct((toks, width), F32))
    piece = rows * cut // 128
    landed += [jax.ShapeDtypeStruct((units, 2, 2 * piece, 128), bf),
               jax.ShapeDtypeStruct((units, 2, piece, 128), bf)]
    anyspace = pl.BlockSpec(memory_space=pl.ANY)
    count = m * (2 * n + 4) + 4 * units
    names = tuple(given)
    res = pl.pallas_call(
        functools.partial(scatter_kernel, dense, units, n, order, names, experts),
        out_shape=outs + landed,
        in_specs=[anyspace] * (len(names) + 4),
        out_specs=[anyspace] * (len(outs) + len(landed)),
        scratch_shapes=[vm((ring_slots[s], message_rows, 128), bf) for s in "xyz"] + [
            vm((4, message_rows, 128), bf), vm((2, rows, cut), F32), vm((128, wide_cols), F32),
            dma((5,)), dma((8,)), dma((count,))] + [dma((ring_slots[s],)) for s in "xyz"] + [
            dma((len(names),)), vm((room, toks), bf)] + [vm((toks, heads), bf)] * 3 + [
            vm((toks, width), bf), vm((room, width), F32), vm((toks, heads), bf),
            vm((2, width // 2, heads), bf), vm((toks, width), F32), vm((toks, width), F32),
            vm((toks, width), F32), vm((n * toks, cut), bf), dma((2,)), dma, dma, vm((tall_rows, 128), F32),
        ] + [vm(v.shape, v.dtype) for v in given.values()],
        compiler_params=pltpu.CompilerParams(
            collective_id=cid, has_side_effects=True, vmem_limit_bytes=67043328),
    )(*given.values(), *weights)
    return res[: m + 4]


def across(a, b):
    return lax.dot_general(a, b, (((1,), (1,)), ((), ())), preferred_element_type=F32)


def times(a, b):
    return jnp.dot(a, b, preferred_element_type=F32)


def middle_items(n, here):
    items = [("join",), ("gates",), ("settle",)]
    for q in range(2):
        items += [("tok", q, k) for k in range(n)] + [("tokend", q)]
    for i in range(3):
        items += [("plane", 12 + i, s) for s in range(4)]
        items += [("line", i, b, k) for b in range(4) for k in range(n)]
    for j in range(here):
        for a in range(3):
            items += [("plane", 3 * j + a, s) for s in range(4)]
        items += [(name, j) for name in ("load", "load_down", "pre", "front", "back", "rows")]
    for v in range(2):
        items += [("shared_load", v), ("shared", v), ("fold_start", v), ("fold_lines", v)]
    return items + [("fold_shared",), ("fold_end",)]


def middle_kernel(n, order, *refs):
    (part, inp, gain, router, named, cot_own, one, mixed, gate_in, up_in, down_in, sg_in, su_in, sd_in) = refs[:14]
    refs = refs[14:]
    (hidden, normed, rows_all, few, gn2, ffn, act_t, ggp_t, gup_t, gates, cot,
     gsg, gsu, sact_t, one_t, two_t, mixed_t) = refs[:17]
    exp_land, sh_land = refs[17:20], refs[20:23]
    refs = refs[23:]
    (other, weights, back, routed, gpre, upre, act, grad, copy_buf, turned, eye,
     sh_stage, dot_sums, fold_other, fold_own, fold_out, fold_in, few_other, few_out, few_in,
     ffn_own, gn_own) = refs[:22]
    (pair_send, pair_recv, row_send, row_recv, plane_send, plane_recv, line_send, line_recv,
     load_sem, out_sem, stage_sem, zsend, zrecv) = refs[22:]
    ins = (gate_in, up_in, down_in)
    sh_ins = (sg_in, su_in, sd_in)
    here, hid, width = gate_in.shape
    toks = inp.shape[0]
    alltoks = n * toks
    D_ = inp.shape[1]
    half = D_ // 2
    d, e, t = lax.axis_index(DP), lax.axis_index(EXPERT), lax.axis_index(TENSOR)
    dx = d + 1 - 2 * lax.rem(d, 2)
    dy = lax.rem(d + 2, 4)
    dd = lax.rem(dx + 2, 4)
    after, before = e < n - 1, e > 0
    near = {"x": {DP: dx}, "y": {DP: dy}, "r": {EXPERT: e + 1}, "l": {EXPERT: e - 1},
            "c": {TENSOR: 1 - t}}
    peers = [lax.rem(e + k, n) for k in range(1, n)]
    mine = pl.ds(pl.multiple_of(t * half, half), half)
    theirs = pl.ds(pl.multiple_of((1 - t) * half, half), half)

    barrier = pltpu.get_barrier_semaphore()
    for dev in [near["x"], near["y"], near["c"]] + [{EXPERT: p} for p in peers]:
        pl.semaphore_signal(barrier, inc=1, device_id=dev, device_id_type=MESH)
    pl.semaphore_wait(barrier, 3 + n - 1)

    def when(cond, f):
        if cond is None:
            f()
        else:
            pl.when(cond)(f)

    sends = []

    def remote(src, dst, ssem, rsem, dev, cond=None, start=True):
        c = pltpu.make_async_remote_copy(
            src_ref=src, dst_ref=dst, send_sem=ssem, recv_sem=rsem, device_id=dev,
            device_id_type=MESH)
        if start:
            when(cond, c.start)
            sends.append((c, cond))
        return c

    def block(p):
        return pl.ds(pl.multiple_of(p * toks, toks), toks)

    first = [remote(part.at[pl.ds(k * (toks // 2), toks // 2)], other.at[pl.ds(k * (toks // 2), toks // 2)],
                    pair_send.at[k], pair_recv.at[k], near["c"]) for k in range(2)]
    for i in range(3):
        pltpu.make_async_copy(sh_ins[i], sh_stage.at[i], stage_sem.at[i]).start()

    def join():
        for k, c in enumerate(first):
            c.wait_recv()
            p = pl.ds(k * (toks // 2), toks // 2)
            h = inp[p, :].astype(F32) + (part[p, :] + other[p, :])
            scale = lax.rsqrt(jnp.mean(h * h, axis=-1, keepdims=True) + epsilon)
            hidden[p, :] = h
            rows = (h * scale * gain[...]).astype(jnp.bfloat16)
            normed[p, :] = rows
            rows_all[pl.ds(pl.multiple_of(e * toks + k * (toks // 2), toks // 2), toks // 2), :] = rows
        two_t[...] = normed[...].astype(F32).T.astype(jnp.bfloat16)

    def along(k):
        return (("r", e - k, e >= k, after, 0), ("l", e + k, e + k < n, before, 1))

    def tok_step(q, k):
        every = (rows_all, cot)[q]
        base = 4 * (n - 1) * q
        if k == 0:
            src = (normed, cot_own)[q]
            for side, has, w in (("r", after, 0), ("l", before, 1)):
                s = base + (n - 1) * w
                remote(src.at[:, mine], every.at[block(e), mine], row_send.at[s], row_recv.at[s], near[side], has)
            return
        for side, o, there, has, w in along(k):
            view = every.at[block(o), mine]
            s = base + (n - 1) * w + k - 1
            when(there, remote(view, view, row_send.at[s], row_recv.at[s], near[side], start=False).wait_recv)
            if k < n - 1:
                remote(view, view, row_send.at[s + 1], row_recv.at[s + 1], near[side], jnp.logical_and(there, has))
            s += 2 * (n - 1)
            remote(view, view, row_send.at[s], row_recv.at[s], near["c"], there)

    def tok_end(q):
        every = (rows_all, cot)[q]
        for k in range(1, n):
            for side, o, there, has, w in along(k):
                view = every.at[block(o), theirs]
                s = 4 * (n - 1) * q + (n - 1) * (2 + w) + k - 1
                when(there, remote(view, view, row_send.at[s], row_recv.at[s], near["c"], start=False).wait_recv)

    def gates_step():
        cot[block(e), :] = cot_own[...]
        one_t[...] = one[...].astype(F32).T.astype(jnp.bfloat16)
        mixed_t[...] = mixed[...].astype(F32).T.astype(jnp.bfloat16)
        logits = across(rows_all[...], router[...])
        lane = lax.broadcasted_iota(jnp.int32, logits.shape, 1)
        logits = jnp.where(lane < 4 * n, logits, -1e30)
        top = jnp.max(logits, axis=-1, keepdims=True)
        ex = jnp.exp(logits - top)
        pr = ex / jnp.sum(ex, axis=-1, keepdims=True)
        gates[...] = pr * named[...].astype(F32)
        back[...] = jnp.zeros_like(back)
        routed[...] = jnp.zeros_like(routed)
        dot_sums[...] = jnp.zeros_like(dot_sums)
        ffn_own[...] = jnp.zeros_like(ffn_own)
        gn_own[...] = jnp.zeros_like(gn_own)
        r = lax.broadcasted_iota(jnp.int32, eye.shape, 0)
        c = lax.broadcasted_iota(jnp.int32, eye.shape, 1)
        eye[...] = jnp.where(r == c, 1.0, 0.0).astype(jnp.bfloat16)

    def plane_view(i, o, h):
        if i < 12:
            k = hid // 2
            return exp_land[i % 3].at[i // 3, pl.ds(h * k, k), pl.ds(pl.multiple_of(o * width, width), width)]
        k = sh_land[i - 12].shape[0] // 2
        return sh_land[i - 12].at[pl.ds(h * k, k), pl.ds(pl.multiple_of((o * n + e) * 128, 128), 128)]

    def plane_own(i, h):
        if i < 12:
            k = hid // 2
            return ins[i % 3].at[i // 3, pl.ds(h * k, k)]
        k = sh_land[i - 12].shape[0] // 2
        return sh_ins[i - 12].at[pl.ds(h * k, k)]

    kinds = ("x0", "y1", "x1", "y0", "f0", "f1")

    def plane_copy(i, o, h, side, kind, own=False, start=True):
        s = 6 * i + kinds.index(kind)
        dst = plane_view(i, o, h)
        return remote(plane_own(i, h) if own else dst, dst, plane_send.at[s], plane_recv.at[s], near[side], start=start)

    def plane_step(i, s):
        if s == 0:
            plane_copy(i, d, 0, "x", "x0", own=True)
            plane_copy(i, d, 1, "y", "y1", own=True)
            plane_copy(i, d, 1, "x", "x1", own=True)
            plane_copy(i, d, 0, "y", "y0", own=True)
        elif s == 1:
            plane_copy(i, dx, 0, "x", "x0", start=False).wait_recv()
            plane_copy(i, dx, 0, "y", "f0")
            plane_copy(i, dy, 1, "x", "y1", start=False).wait_recv()
            plane_copy(i, dy, 1, "x", "f1")
        elif s == 2:
            plane_copy(i, dx, 1, "x", "x1", start=False).wait_recv()
            plane_copy(i, dy, 0, "x", "y0", start=False).wait_recv()
        else:
            plane_copy(i, dd, 0, "x", "f0", start=False).wait_recv()
            plane_copy(i, dd, 1, "x", "f1", start=False).wait_recv()

    def line_view(i, o, eo):
        return sh_land[i].at[:, pl.ds(pl.multiple_of((o * n + eo) * 128, 128), 128)]

    def line_step(i, b, k):
        o = (d, dx, dy, dd)[b]
        base = (i * 4 + b) * 2 * (n - 1)

        def copy(eo, side, hop, own=False, cond=None, start=True):
            s = base + (0 if side == "r" else n - 1) + hop - 1
            dst = line_view(i, o, eo)
            return remote(sh_ins[i] if own else dst, dst, line_send.at[s], line_recv.at[s], near[side], cond, start)

        if k == 0:
            copy(e, "r", 1, b == 0, after)
            copy(e, "l", 1, b == 0, before)
            return
        for side, eo, there, has in (("r", e - k, e >= k, after), ("l", e + k, e + k < n, before)):
            when(there, copy(eo, side, k, start=False).wait_recv)
            if k < n - 1:
                copy(eo, side, k + 1, cond=jnp.logical_and(there, has))

    loads = {}

    def load(j, arrays=(0, 1)):
        cs = []
        for a in arrays:
            for q, o in enumerate((d, dx, dy, dd)):
                cols = pl.ds(pl.multiple_of(o * width, width), width)
                src = ins[a].at[j] if q == 0 else exp_land[a].at[j, :, cols]
                c = pltpu.make_async_copy(src, weights.at[j % 2, a, :, cols], load_sem.at[j % 2, 4 * a + q])
                c.start()
                cs.append(c)
        loads[j, arrays] = cs

    def load_down(j):
        load(j, (2,))

    writes = []
    waiting = {}

    def write(src, dst, k):
        c = pltpu.make_async_copy(src, dst, out_sem.at[k])
        c.start()
        waiting[k] = c

    def free(k):
        if k in waiting:
            waiting.pop(k).wait()

    def ffn_front(rows, count, w):
        step = min(256, count)
        def pre(m, _):
            r = pl.ds(pl.multiple_of(m * step, step), step)
            x = rows[r, :]
            g = across(x, w(0))
            u = across(x, w(1))
            gpre[r, :] = g
            upre[r, :] = u
            act[r, :] = (g * jax.nn.sigmoid(g) * u).astype(jnp.bfloat16)
            return 0
        lax.fori_loop(0, count // step, pre, 0)

    def pre_step(j):
        for c in loads.pop((j, (0, 1))):
            c.wait()
        ffn_front(rows_all, alltoks, lambda a: weights[j % 2, a])

    def front(j):
        for c in loads.pop((j, (2,))):
            c.wait()
        lane = lax.broadcasted_iota(jnp.int32, (256, 128), 1)
        def out(k, _):
            m, c = k // 4, k % 4
            r = pl.ds(pl.multiple_of(m * 256, 256), 256)
            cols = pl.ds(pl.multiple_of(c * 512, 512), 512)
            piece = times(act[r, :], weights[j % 2, 2, :, cols]).astype(jnp.bfloat16).astype(F32)
            gt = gates[r, :][:, j : j + 1]
            ct = cot[r, cols].astype(F32)
            routed[r, cols] += gt * piece
            dot = jnp.sum(piece * ct, axis=-1, keepdims=True)
            dot_sums[r, :] += jnp.where(lane == e * here + j, dot, 0.0)
            copy_buf[r, cols] = (gt * ct).astype(jnp.bfloat16)
            return 0
        lax.fori_loop(0, alltoks // 256 * 4, out, 0)
        free(0)
        turned[0] = across(eye[...], act[...]).astype(jnp.bfloat16)
        write(turned.at[0], act_t.at[j], 0)

    def ffn_back(rows, count, w):
        step = min(256, count)
        def pre(m, _):
            r = pl.ds(pl.multiple_of(m * step, step), step)
            ga = across(rows[r, :], w(2))
            g, u = gpre[r, :], upre[r, :]
            s = jax.nn.sigmoid(g)
            grad[0, r, :] = (ga * u * (s * (1.0 + g * (1.0 - s)))).astype(jnp.bfloat16)
            grad[1, r, :] = (ga * (g * s)).astype(jnp.bfloat16)
            return 0
        lax.fori_loop(0, count // step, pre, 0)

    def back_step(j):
        ffn_back(copy_buf, alltoks, lambda a: weights[j % 2, a])

    def rows_step(j):
        def out(k, _):
            m, c = k // 4, k % 4
            r = pl.ds(pl.multiple_of(m * 256, 256), 256)
            cols = pl.ds(pl.multiple_of(c * 512, 512), 512)
            back[r, cols] += (times(grad[0, r, :], weights[j % 2, 0, :, cols])
                              + times(grad[1, r, :], weights[j % 2, 1, :, cols]))
            return 0
        lax.fori_loop(0, alltoks // 256 * 4, out, 0)
        for q, dst in ((0, ggp_t), (1, gup_t)):
            free(1 + q)
            turned[1 + q] = across(eye[...], grad[q]).astype(jnp.bfloat16)
            write(turned.at[1 + q], dst.at[j], 1 + q)

    def shared_load(v):
        cs = []
        for a in range(3):
            c = pltpu.make_async_copy(sh_land[a].at[pl.ds(v * hid, hid)], weights.at[v, a], load_sem.at[v, a])
            c.start()
            cs.append(c)
        loads["s", v] = cs

    def shared(v):
        for c in loads.pop(("s", v)):
            c.wait()
        w = lambda a: weights[v, a]
        own = block(e)
        ffn_front(normed, toks, w)
        for c in range(4):
            ffn_own[:, c * 512 : (c + 1) * 512] += times(act[0:toks, :], weights[v, 2, :, c * 512 : (c + 1) * 512])
        sact_t[pl.ds(v * hid, hid), :] = across(eye[...], act[0:toks, :]).astype(jnp.bfloat16)
        copy_buf[0:toks, :] = cot[own, :]
        ffn_back(copy_buf, toks, w)
        for c in range(4):
            gn_own[:, c * 512 : (c + 1) * 512] += (
                times(grad[0, 0:toks, :], weights[v, 0, :, c * 512 : (c + 1) * 512])
                + times(grad[1, 0:toks, :], weights[v, 1, :, c * 512 : (c + 1) * 512]))
        gsg[:, v * hid : (v + 1) * hid] = grad[0, 0:toks, :]
        gsu[:, v * hid : (v + 1) * hid] = grad[1, 0:toks, :]

    def settle():
        for i in range(3):
            pltpu.make_async_copy(sh_ins[i], sh_stage.at[i], stage_sem.at[i]).wait()
            pltpu.make_async_copy(sh_stage.at[i], line_view(i, d, e), stage_sem.at[i]).start()
        for i in range(3):
            pltpu.make_async_copy(sh_stage.at[i], line_view(i, d, e), stage_sem.at[i]).wait()

    def fold_start(q):
        src, base = ((back, 2), (routed, 2 + 2 * n))[q]
        for k, p in enumerate(peers + [e]):
            remote(src.at[block(p), theirs], fold_other.at[q, block(p)], pair_send.at[base + k], pair_recv.at[base + k], near["c"])
            if q == 1:
                s = 2 + n + k
                remote(dot_sums.at[block(p)], few_other.at[block(p)], pair_send.at[s], pair_recv.at[s], near["c"])

    def got(view, k):
        remote(view, view, pair_send.at[k], pair_recv.at[k], near["c"], start=False).wait_recv()

    def fold_shared():
        base = 2 + 3 * n
        for q, src in enumerate((gn_own, ffn_own)):
            remote(src.at[:, theirs], fold_own.at[q], pair_send.at[base + q], pair_recv.at[base + q], near["c"])

    def fold_lines(q):
        src, base = ((back, 2), (routed, 2 + 2 * n))[q]
        for k, p in enumerate(peers):
            got(fold_other.at[q, block(p)], base + k)
            fold_out[q, k] = (src[block(p), mine] + fold_other[q, block(p), :]).astype(jnp.bfloat16)
            s = 2 * (n - 1) * q + k
            remote(fold_out.at[q, k], fold_in.at[q, k], zsend.at[s], zrecv.at[s], {EXPERT: p})
            if q == 1:
                got(few_other.at[block(p)], 2 + n + k)
                few_out[k] = (dot_sums[block(p), :] + few_other[block(p), :]).astype(jnp.bfloat16)
                s = n - 1 + k
                remote(few_out.at[k], few_in.at[k], zsend.at[s], zrecv.at[s], {EXPERT: p})

    def fold_end():
        for src, q, base in ((back, 0, 2), (routed, 1, 2 + 2 * n)):
            got(fold_other.at[q, block(e)], base + n - 1)
            got(fold_own.at[q], 2 + 3 * n + q)
            dst, own = ((gn2, gn_own), (ffn, ffn_own))[q]
            dst[:, mine] = (src[block(e), mine] + fold_other[q, block(e), :]) + (own[:, mine] + fold_own[q])
        got(few_other.at[block(e)], 2 + n + n - 1)
        few[...] = dot_sums[block(e), :] + few_other[block(e), :]
        for k in range(n - 1):
            s = n - 1 + k
            remote(few_in.at[k], few_in.at[k], zsend.at[s], zrecv.at[s], near["c"], start=False).wait_recv()
            few[...] += few_in[k].astype(F32)
        for q, dst in ((0, gn2), (1, ffn)):
            for k in range(n - 1):
                s = 2 * (n - 1) * q + k
                remote(fold_in.at[q, k], fold_in.at[q, k], zsend.at[s], zrecv.at[s], near["c"], start=False).wait_recv()
                dst[:, mine] += fold_in[q, k].astype(F32)
            s = 2 + 3 * n + 2 + q
            remote(dst.at[:, mine], dst.at[:, mine], pair_send.at[s], pair_recv.at[s], near["c"])
        for q, dst in ((0, gn2), (1, ffn)):
            got(dst.at[:, theirs], 2 + 3 * n + 2 + q)

    steps = {"join": join, "tok": tok_step, "tokend": tok_end, "gates": gates_step, "plane": plane_step, "line": line_step,
             "load": load, "load_down": load_down, "pre": pre_step, "front": front, "back": back_step, "rows": rows_step, "shared_load": shared_load, "shared": shared,
             "settle": settle, "fold_start": fold_start, "fold_shared": fold_shared, "fold_lines": fold_lines,
             "fold_end": fold_end}
    items = middle_items(n, here)
    for name, *args in [items[k] for k in order]:
        steps[name](*args)
    for k in list(waiting):
        free(k)
    for c, cond in sends:
        when(cond, c.wait_send)


def middle(part, inp, gain, router, named, cot, one, mixed, experts, shared_t, n, order, cid):
    bf, dma, vm = jnp.bfloat16, pltpu.SemaphoreType.DMA, pltpu.VMEM
    toks, width = inp.shape
    here, hid, cut = experts[0].shape
    al = n * toks
    sh = shared_t[0].shape[0]
    S = jax.ShapeDtypeStruct
    vmem, anyspace = pl.BlockSpec(memory_space=pltpu.VMEM), pl.BlockSpec(memory_space=pl.ANY)
    outs = [
        (S((toks, width), F32), vmem), (S((toks, width), bf), vmem), (S((al, width), bf), vmem),
        (S((toks, 128), F32), vmem), (S((toks, width), F32), vmem),
        (S((toks, width), F32), vmem), (S((here, hid, al), bf), anyspace), (S((here, hid, al), bf), anyspace),
        (S((here, hid, al), bf), anyspace), (S((al, 128), F32), vmem), (S((al, width), bf), vmem),
        (S((toks, 2 * hid), bf), vmem), (S((toks, 2 * hid), bf), vmem), (S((2 * hid, toks), bf), vmem),
        (S((width, toks), bf), vmem), (S((width, toks), bf), vmem), (S((mixed.shape[1], toks), bf), vmem),
    ] + [(S((here, hid, width), bf), anyspace)] * 3 + [(S((sh, width), bf), anyspace)] * 3
    scratch = [
        vm((toks, width), F32), vm((2, 3, hid, width), bf), vm((al, width), F32),
        vm((al, width), F32), vm((al, hid), F32), vm((al, hid), F32), vm((al, hid), bf), vm((2, al, hid), bf),
        vm((al, width), bf), vm((3, hid, al), bf), vm((hid, hid), bf), vm((3, sh, 128), bf), vm((al, 128), F32),
        vm((2, al, width // 2), F32), vm((2, toks, width // 2), F32), vm((2, n - 1, toks, width // 2), bf),
        vm((2, n - 1, toks, width // 2), bf), vm((al, 128), F32), vm((n - 1, toks, 128), bf),
        vm((n - 1, toks, 128), bf), vm((toks, width), F32), vm((toks, width), F32),
        dma((6 + 3 * n,)), dma((6 + 3 * n,)), dma((8 * (n - 1),)), dma((8 * (n - 1),)), dma((90,)), dma((90,)),
        dma((24 * (n - 1),)), dma((24 * (n - 1),)), dma((2, 12)), dma((4,)), dma((3,)),
        dma((3 * (n - 1),)), dma((3 * (n - 1),)),
    ]
    res = pl.pallas_call(
        functools.partial(middle_kernel, n, order),
        out_shape=[s for s, _ in outs], out_specs=[b for _, b in outs],
        in_specs=[vmem] * 8 + [anyspace] * 6,
        scratch_shapes=scratch,
        compiler_params=pltpu.CompilerParams(
            collective_id=cid, has_side_effects=True, vmem_limit_bytes=67043328),
    )(part, inp, gain, router, named, cot, one, mixed, *experts, *shared_t)
    return res[:17]


def rms_scale(vector):
    return lax.rsqrt(jnp.mean(vector * vector, axis=-1, keepdims=True) + epsilon)


def rope_tables(count, width):
    half_width = width // 2
    frequency = rope_base ** (-jnp.arange(half_width, dtype=jnp.float32) / half_width)
    angles = jnp.arange(count, dtype=jnp.float32)[:, None] * frequency[None, :]
    return (jnp.cos(angles)[:, None, :], jnp.sin(angles)[:, None, :])


def rotate(vector, cosine, sine_table):
    half_width = vector.shape[-1] // 2
    first_half = vector[..., :half_width]
    second_half = vector[..., half_width:]
    return jnp.concatenate(
        [
            first_half * cosine - second_half * sine_table,
            first_half * sine_table + second_half * cosine,
        ],
        axis=-1,
    )


def unrotate(vector, cosine, sine_table):
    half_width = vector.shape[-1] // 2
    first_half = vector[..., :half_width]
    second_half = vector[..., half_width:]
    return jnp.concatenate(
        [
            first_half * cosine + second_half * sine_table,
            second_half * cosine - first_half * sine_table,
        ],
        axis=-1,
    )


def dots(left, right, *dims):
    return lax.dot_general(left, right, dims, preferred_element_type=F32)


def silu_parts(before):
    sigmoid_val = jax.nn.sigmoid(before)
    return (before * sigmoid_val, sigmoid_val * (1.0 + before * (1.0 - sigmoid_val)))


def masked_scores(query_rot, key_rot, allowed):
    scores = dots(query_rot, key_rot, ((2,), (2,)), ((1,), (1,))) / math.sqrt(query_rot.shape[-1])
    return jnp.where(allowed[None], scores, masked_score)


def turn(array, by, axis):
    return lax.dynamic_slice_in_dim(
        jnp.concatenate([array, array], axis=axis), by, array.shape[axis], axis=axis)


def plain_middle(attn_part, input_f, gain_two, router_rows, named_all, grads_all, cotangent,
                 expert_weights, full_sgate, full_sup, full_sdown):
    here = lax.axis_index(EXPERT)
    local_gate, local_up, local_down = expert_weights
    experts_here = local_gate.shape[0]
    hidden_one = input_f + lax.psum(attn_part, TENSOR)
    normed_two = (hidden_one * rms_scale(hidden_one) * gain_two).astype(BF)
    rows_all = lax.all_gather(normed_two, EXPERT, axis=0, tiled=True)
    probs_all = jax.nn.softmax(dots(rows_all, router_rows, ((1,), (1,)), ((), ())), axis=-1)
    gates_here = lax.dynamic_slice_in_dim(
        probs_all * named_all, here * experts_here, experts_here, axis=1)
    gate_pre = dots(local_gate, rows_all, ((2,), (1,)), ((), ()))
    up_pre = dots(local_up, rows_all, ((2,), (1,)), ((), ()))
    silu_gate, slope_gate = silu_parts(gate_pre)
    act_t = (silu_gate * up_pre).astype(BF)
    part_rows = dots(act_t, local_down, ((1,), (1,)), ((0,), (0,))).astype(BF).astype(F32)
    routed = sum(gates_here[:, j : j + 1] * part_rows[j] for j in range(experts_here))
    grads_wide = grads_all.astype(F32)
    owner_grads = (jnp.transpose(gates_here)[:, :, None] * grads_wide[None]).astype(BF)
    gate_dots = jnp.sum(part_rows * grads_wide[None], axis=-1)
    dots_wide = lax.dynamic_update_slice(
        jnp.zeros_like(probs_all), jnp.transpose(gate_dots), (0, here * experts_here))
    grad_act = dots(local_down, owner_grads, ((2,), (2,)), ((0,), (0,)))
    ggp_t = (grad_act * up_pre * slope_gate).astype(BF)
    gup_t = (grad_act * silu_gate).astype(BF)
    grad_rows = dots(ggp_t, local_gate, ((0, 1), (0, 1)), ((), ()))
    grad_rows = grad_rows + dots(gup_t, local_up, ((0, 1), (0, 1)), ((), ()))
    shared_gpre = jnp.dot(normed_two, full_sgate, preferred_element_type=F32)
    shared_upre = jnp.dot(normed_two, full_sup, preferred_element_type=F32)
    silu_shared, slope_shared = silu_parts(shared_gpre)
    shared_act = (silu_shared * shared_upre).astype(BF)
    shared_part = jnp.dot(shared_act, full_sdown, preferred_element_type=F32)
    grad_sact = dots(cotangent, full_sdown, ((1,), (1,)), ((), ()))
    grad_sgate = (grad_sact * shared_upre * slope_shared).astype(BF)
    grad_sup = (grad_sact * silu_shared).astype(BF)
    own_rows = dots(grad_sgate, full_sgate, ((1,), (1,)), ((), ()))
    own_rows = own_rows + dots(grad_sup, full_sup, ((1,), (1,)), ((), ()))
    back = [lax.psum_scatter(v, EXPERT, scatter_dimension=0, tiled=True)
            for v in (grad_rows, routed, dots_wide)]
    grad_normed_two = lax.psum(back[0] + own_rows, TENSOR)
    ffn_total = lax.psum(back[1] + shared_part, TENSOR)
    dots_sum = lax.psum(back[2], TENSOR)
    router_probs = lax.dynamic_slice_in_dim(
        probs_all, here * normed_two.shape[0], normed_two.shape[0], axis=0)
    return (hidden_one, normed_two, rows_all, router_probs, dots_sum, grad_normed_two, ffn_total,
            act_t, ggp_t, gup_t, owner_grads, grad_sgate, grad_sup, shared_act.T)


def plain_scatter(dense, lefts, rights, extra, exp_left, rows_all, owner_grads):
    sums = []
    for k, ((kind, _), left, right) in enumerate(zip(dense, lefts, rights)):
        part = jnp.dot(left, right, preferred_element_type=F32)
        if k == len(dense) - 1:
            part = part + extra
        dim = 0 if kind == "rows" else 1
        sums.append(lax.psum_scatter(part, BOTH, scatter_dimension=dim, tiled=True))
    for left, right in zip(exp_left, (rows_all, rows_all, owner_grads)):
        dims = (((2,), (0,)), ((), ())) if right.ndim == 2 else (((2,), (1,)), ((0,), (0,)))
        part = dots(left, right, *dims).astype(BF)
        sums.append(lax.psum_scatter(part, DP, scatter_dimension=2, tiled=True).astype(F32))
    return sums


def plain_backward(
    dense, cotangent, block_input, named, router_probs, dots_sum, grad_normed_two, router_rows,
    hidden_one, gain_two, gain_one, full_query, full_key, full_value, full_output, query_rot, key_rot,
    value_rows, allowed, log_total, cosine, sine_table, one_t, two_t, mixed_t, shared_act_t,
    grad_sgate, grad_sup, normed_two, ggp_t, gup_t, act_t, rows_all, owner_grads,
):
    total_experts = router_rows.shape[0]
    seq_len, heads_here = query_rot.shape[:2]
    input_f = block_input.astype(F32)
    scale_one = rms_scale(input_f)
    scale_two = rms_scale(hidden_one)
    grad_out = cotangent.astype(F32)
    grad_rprobs = jnp.where(named, dots_sum, 0.0)
    grad_logits = (
        router_probs * (grad_rprobs - jnp.sum(grad_rprobs * router_probs, axis=-1, keepdims=True))
    ).astype(BF)
    grad_normed_two = grad_normed_two + dots(grad_logits, router_rows, ((1,), (0,)), ((), ()))
    ffn_gain_full = jnp.sum(grad_normed_two * hidden_one * scale_two, axis=0)
    weighted_two = grad_normed_two * gain_two
    cube_two = scale_two * scale_two * scale_two
    grad_hidden = (
        grad_out
        + scale_two * weighted_two
        - hidden_one * cube_two * jnp.mean(hidden_one * weighted_two, axis=-1, keepdims=True)
    )
    grad_attn = grad_hidden.astype(BF)
    grad_mixed = (
        dots(grad_attn, full_output, ((1,), (1,)), ((), ()))
        .astype(BF)
        .reshape(seq_len, heads_here, HD)
    )
    prob_again = jnp.exp(masked_scores(query_rot, key_rot, allowed) - log_total)
    grad_probs = dots(grad_mixed, value_rows, ((2,), (2,)), ((1,), (1,)))
    grad_scores = (
        prob_again * (grad_probs - jnp.sum(prob_again * grad_probs, axis=-1, keepdims=True))
    ).astype(BF)
    value_grad_rows = (
        jnp.transpose(dots(prob_again.astype(BF), grad_mixed, ((1,), (0,)), ((0,), (1,))), (1, 0, 2))
        .astype(BF)
        .reshape(seq_len, heads_here * HD)
    )
    inverse_root = 1.0 / math.sqrt(HD)
    grad_qrot = (
        jnp.transpose(dots(grad_scores, key_rot, ((2,), (0,)), ((0,), (1,))), (1, 0, 2))
        * inverse_root
    )
    grad_krot = (
        jnp.transpose(dots(grad_scores, query_rot, ((1,), (0,)), ((0,), (1,))), (1, 0, 2))
        * inverse_root
    )
    grad_qpre = (
        unrotate(grad_qrot, cosine, sine_table).astype(BF).reshape(seq_len, heads_here * HD)
    )
    grad_kpre = (
        unrotate(grad_krot, cosine, sine_table).astype(BF).reshape(seq_len, heads_here * HD)
    )
    grad_normed_one = dots(grad_qpre, full_query, ((1,), (1,)), ((), ()))
    grad_normed_one = grad_normed_one + dots(grad_kpre, full_key, ((1,), (1,)), ((), ()))
    grad_normed_one = grad_normed_one + dots(value_grad_rows, full_value, ((1,), (1,)), ((), ()))
    grad_normed_one = lax.psum(grad_normed_one, TENSOR)
    attn_gain_full = jnp.sum(grad_normed_one * input_f * scale_one, axis=0)
    weighted_one = grad_normed_one * gain_one
    cube_one = scale_one * scale_one * scale_one
    input_grad = (
        grad_hidden
        + scale_one * weighted_one
        - input_f * cube_one * jnp.mean(input_f * weighted_one, axis=-1, keepdims=True)
    )
    room = total_experts + 2 + (-(total_experts + 2) % 64)
    logits_t = jnp.pad(grad_logits.T, ((0, room - total_experts), (0, 0)))
    extra = jnp.concatenate([
        jnp.zeros((total_experts, D), F32), attn_gain_full[None], ffn_gain_full[None],
        jnp.zeros((room - total_experts - 2, D), F32)])
    lefts = (one_t, one_t, one_t, mixed_t, two_t, two_t, shared_act_t, logits_t)
    rights = (grad_qpre, grad_kpre, value_grad_rows, grad_attn, grad_sgate, grad_sup, cotangent, normed_two)
    exp_left = (ggp_t, gup_t, act_t)
    sums = plain_scatter(dense, lefts, rights, extra, exp_left, rows_all, owner_grads)
    return sums, input_grad


def body(
    block_input,
    attn_gain,
    query_weight,
    key_weight,
    value_weight,
    output_weight,
    ffn_gain,
    router_weight,
    expert_gate,
    expert_up,
    expert_down,
    shared_gate,
    shared_up,
    shared_down,
    segments,
    routes,
    cotangent,
):
    seq_len = block_input.shape[0]
    total_experts = router_weight.shape[1]
    owners, here = lax.axis_size(EXPERT), lax.axis_index(EXPERT)
    kernels = (output_weight.shape[1] % 128 == 0 and lax.axis_size(DP) == 4
               and total_experts <= 128 and seq_len == 128)
    expert_ids = jnp.arange(total_experts, dtype=jnp.int32)
    named = jnp.any(routes[:, :, None] == expert_ids[None, None, :], axis=1)
    small = jnp.concatenate([router_weight, attn_gain[:, None], ffn_gain[:, None]], axis=1).T
    flip_gate, flip_up = jnp.swapaxes(expert_gate, 1, 2), jnp.swapaxes(expert_up, 1, 2)
    named_low = named.astype(BF)
    if kernels:
        small = jnp.pad(small, ((0, -small.shape[0] % 32), (0, 0)))
        named_low = jnp.pad(named_low, ((0, 0), (0, 256 - total_experts)))
        arrays = (query_weight, key_weight, value_weight, output_weight, small, named_low)
        forms = ("rows",) * 3 + ("cols", "cols", "tokens")
        firsts = ("z",) * 3 + ("xy", "z", "xy")
        (full_query, full_key, full_value, full_output, full_small, named_all, sgate_t, sup_t) = gather(
            arrays, forms, firsts, owners, gather_starts, (shared_gate, shared_up))
    else:
        full_small = lax.all_gather(small, BOTH, axis=1, tiled=True)
        full_query = lax.all_gather(query_weight, BOTH, axis=0, tiled=True)
        full_key = lax.all_gather(key_weight, BOTH, axis=0, tiled=True)
        full_value = lax.all_gather(value_weight, BOTH, axis=0, tiled=True)
        full_output = lax.all_gather(output_weight, BOTH, axis=1, tiled=True)
        named_all = lax.all_gather(named_low, EXPERT, axis=0, tiled=True)
    named_all = named_all[:, :total_experts]
    router_rows = full_small[:total_experts]
    gain_one = full_small[total_experts].astype(F32)
    gain_two = full_small[total_experts + 1].astype(F32)
    heads_here = full_query.shape[1] // HD
    input_f = block_input.astype(F32)
    scale_one = rms_scale(input_f)
    normed_one = (input_f * scale_one * gain_one).astype(BF)
    cosine, sine_table = rope_tables(seq_len, HD)
    query_pre = jnp.dot(normed_one, full_query, preferred_element_type=F32).reshape(
        seq_len, heads_here, HD
    )
    key_pre = jnp.dot(normed_one, full_key, preferred_element_type=F32).reshape(
        seq_len, heads_here, HD
    )
    query_rot = rotate(query_pre, cosine, sine_table).astype(BF)
    key_rot = rotate(key_pre, cosine, sine_table).astype(BF)
    value_rows = (
        jnp.dot(normed_one, full_value, preferred_element_type=F32)
        .astype(BF)
        .reshape(seq_len, heads_here, HD)
    )
    position = jnp.arange(seq_len)
    segment_row = segments[0]
    allowed = (position[:, None] >= position[None, :]) & (
        segment_row[:, None] == segment_row[None, :]
    )
    scores = masked_scores(query_rot, key_rot, allowed)
    top_score = jnp.max(scores, axis=-1, keepdims=True)
    shifted = jnp.exp(scores - top_score)
    row_total = jnp.sum(shifted, axis=-1, keepdims=True)
    log_total = top_score + jnp.log(row_total)
    prob_low = (shifted / row_total).astype(BF)
    mixed_rows = (
        jnp.transpose(dots(prob_low, value_rows, ((2,), (0,)), ((0,), (1,))), (1, 0, 2))
        .astype(BF)
        .reshape(seq_len, heads_here * HD)
    )
    attn_part = jnp.dot(mixed_rows, full_output, preferred_element_type=F32)
    experts = (flip_gate, flip_up, expert_down)
    if kernels:
        first = here * expert_gate.shape[0]
        router_pad = jnp.pad(turn(router_rows, first, 0), ((0, 128 - total_experts), (0, 0)))
        named_pad = jnp.pad(turn(named_all, first, 1), ((0, 0), (0, 128 - total_experts)))
        (hidden_one, normed_two, rows_all, dots_sum, back, ffn_total, act_t, ggp_t, gup_t, gates, cot_all,
         grad_sgate, grad_sup, shared_act_t, one_t, two_t, mixed_t) = middle(
            attn_part, block_input, gain_two[None], router_pad, named_pad, cotangent, normed_one,
            mixed_rows, experts, (sgate_t, sup_t, shared_down), owners, middle_order, 2)
    else:
        (hidden_one, normed_two, rows_all, router_probs, dots_sum, grad_normed_two, ffn_total, act_t, ggp_t, gup_t,
         owner_grads, grad_sgate, grad_sup, shared_act_t) = plain_middle(
            attn_part, input_f, gain_two, router_rows, named_all.astype(F32),
            lax.all_gather(cotangent, EXPERT, axis=0, tiled=True), cotangent,
            tuple(lax.all_gather(w, DP, axis=2, tiled=True) for w in experts),
            lax.all_gather(shared_gate, BOTH, axis=0, tiled=True),
            lax.all_gather(shared_up, BOTH, axis=0, tiled=True),
            lax.all_gather(shared_down, BOTH, axis=1, tiled=True))
        one_t, two_t, mixed_t = normed_one.T, normed_two.T, mixed_rows.T
    block_output = (hidden_one + ffn_total).astype(BF)
    dense = ((("rows", "z"),) + (("rows", "p"),) * 2
             + (("cols", "p"),) + (("rows", "z"),) * 2 + (("cols", "z"),) * 2)
    if kernels:
        pair = lambda first, last: jnp.concatenate([first, last], axis=-1)[:, 0]
        flat = lambda v: v.reshape(seq_len, heads_here * HD)
        given = dict(
            one_t=one_t, mixed_t=mixed_t, two_t=two_t, sact_t=shared_act_t, gsg=grad_sgate, gsu=grad_sup,
            cot=cotangent, normed=normed_two, ggp=ggp_t, gup=gup_t, act=act_t, rows_all=rows_all,
            cot_all=cot_all, gates=gates, hidden=hidden_one, back=back, few=dots_sum,
            named=jnp.pad(named.astype(F32), ((0, 0), (0, 128 - total_experts))),
            gain_two=gain_two[None], gain_one=gain_one[None], inp=block_input,
            q=flat(query_rot), k=flat(key_rot), v=flat(value_rows), cos=pair(cosine, cosine),
            sin=pair(sine_table, -sine_table), mask=allowed.astype(F32),
            router=jnp.pad(router_rows, ((0, 128 - total_experts), (0, 0))))
        *sums, input_grad = scatter(
            dense, given, (full_output, full_query, full_key, full_value), total_experts, owners,
            scatter_order, 1)
    else:
        sums, input_grad = plain_backward(
            dense, cotangent, block_input, named, router_probs, dots_sum, grad_normed_two, router_rows,
            hidden_one, gain_two, gain_one, full_query, full_key, full_value, full_output, query_rot, key_rot,
            value_rows, allowed, log_total, cosine, sine_table, one_t, two_t, mixed_t, shared_act_t,
            grad_sgate, grad_sup, normed_two, ggp_t, gup_t, act_t, rows_all, owner_grads)
    (query_grad, key_grad, value_grad, output_grad, shared_gate_grad, shared_up_grad,
     shared_down_grad, small_grad, expert_gate_grad, expert_up_grad, expert_down_grad) = sums
    return (
        block_output,
        input_grad,
        small_grad[total_experts],
        query_grad,
        key_grad,
        value_grad,
        output_grad,
        small_grad[total_experts + 1],
        small_grad[:total_experts].T,
        jnp.swapaxes(expert_gate_grad, 1, 2),
        jnp.swapaxes(expert_up_grad, 1, 2),
        expert_down_grad,
        shared_gate_grad,
        shared_up_grad,
        shared_down_grad,
    )


def solution(mesh):
    return jax.shard_map(
        body,
        mesh=mesh,
        in_specs=(
            P((DP, EXPERT), None),
            P((DP, EXPERT)),
            P((DP, EXPERT), TENSOR),
            P((DP, EXPERT), TENSOR),
            P((DP, EXPERT), TENSOR),
            P(TENSOR, (DP, EXPERT)),
            P((DP, EXPERT)),
            P((DP, EXPERT), None),
            P(EXPERT, DP, TENSOR),
            P(EXPERT, DP, TENSOR),
            P(EXPERT, TENSOR, DP),
            P((DP, EXPERT), TENSOR),
            P((DP, EXPERT), TENSOR),
            P(TENSOR, (DP, EXPERT)),
            P((DP, EXPERT), None),
            P((DP, EXPERT), None),
            P((DP, EXPERT), None),
        ),
        out_specs=(
            P((DP, EXPERT), None),
            P((DP, EXPERT), None),
            P((DP, EXPERT)),
            P((DP, EXPERT), TENSOR),
            P((DP, EXPERT), TENSOR),
            P((DP, EXPERT), TENSOR),
            P(TENSOR, (DP, EXPERT)),
            P((DP, EXPERT)),
            P((DP, EXPERT), None),
            P(EXPERT, DP, TENSOR),
            P(EXPERT, DP, TENSOR),
            P(EXPERT, TENSOR, DP),
            P((DP, EXPERT), TENSOR),
            P((DP, EXPERT), TENSOR),
            P(TENSOR, (DP, EXPERT)),
        ),
        check_vma=False,
    )
```

```python
import functools
import math
import types

import jax
import jax.numpy as jnp
from jax import lax
from jax.experimental import pallas as pl
from jax.experimental.pallas import tpu as pltpu
from jax.sharding import PartitionSpec as P

MESH = pl.DeviceIdType.MESH
F32, BF = jnp.float32, jnp.bfloat16
DP, EXPERT, TENSOR = "dp", "expert", "tensor"
BOTH = (DP, EXPERT)
D = 2048
HD = 128


epsilon = 1e-06
rope_base = 10000.0
masked_score = -1e30
gather_starts = (1.91, 2.48, 3.88, 2.78, 2.0, 1.0)
scatter_order = (91, 92, 86, 87, 49, 60, 102, 0, 96, 31, 93, 59, 1, 13, 14, 22, 23, 50, 43, 94, 32, 58, 52, 101, 82, 4, 88, 76, 33, 40, 51, 97, 25, 6, 15, 81, 41, 24, 16, 42, 34, 103, 53, 95, 5, 54, 99, 27, 83, 61, 26, 84, 45, 17, 98, 56, 35, 28, 2, 19, 55, 47, 77, 7, 104, 89, 62, 85, 44, 3, 67, 68, 69, 70, 9, 18, 57, 37, 20, 63, 78, 8, 21, 36, 72, 29, 100, 71, 38, 79, 105, 65, 90, 46, 30, 11, 73, 64, 39, 10, 74, 48, 80, 66, 75, 12)
middle_order = (13, 8, 33, 113, 0, 9, 10, 14, 15, 57, 53, 91, 73, 37, 58, 59, 34, 35, 17, 18, 11, 12, 92, 19, 54, 55, 61, 77, 16, 3, 109, 99, 114, 81, 65, 66, 21, 25, 74, 67, 62, 36, 26, 27, 56, 69, 95, 100, 101, 82, 29, 30, 31, 93, 4, 115, 116, 110, 111, 20, 96, 97, 78, 28, 22, 23, 24, 94, 41, 63, 117, 5, 6, 7, 1, 68, 75, 76, 112, 98, 103, 32, 83, 84, 86, 60, 2, 70, 71, 72, 64, 102, 104, 127, 45, 42, 131, 38, 79, 80, 85, 87, 88, 89, 90, 105, 118, 135, 39, 40, 46, 49, 43, 128, 129, 106, 107, 108, 47, 121, 123, 44, 132, 119, 120, 122, 124, 125, 126, 136, 137, 50, 51, 52, 133, 134, 130, 139, 141, 48, 145, 138, 140, 142, 151, 143, 152, 144, 147, 146, 148, 149, 150, 153, 154)


class Leaf:
    def __init__(self, shape, dtype, form, first, n):
        self.shape, self.dtype, self.form, self.first, self.n = shape, dtype, form, first, n
        rows = shape[-2]
        if form == "rows":
            self.out = (4 * n * rows, shape[1])
        elif form == "cols":
            self.out = (shape[0], 4 * n * shape[1])
        elif form == "expert":
            self.out = (shape[0], shape[1], 4 * shape[2])
        elif form == "tokens":
            self.out = (n * rows, shape[1])

    def view(self, ref, d, e, half=None):
        if self.form == "rows":
            r = self.shape[0]
            s, k = (d * self.n + e) * r, r
            if half is not None:
                k = r // 2
                s = s + half * k
            return ref.at[pl.ds(pl.multiple_of(s, k), k), :]
        if self.form == "cols":
            c = self.shape[1]
            s = pl.multiple_of((d * self.n + e) * c, c)
            k = self.shape[0] // 2
            rows = slice(None) if half is None else pl.ds(half * k, k)
            return ref.at[rows, pl.ds(s, c)]
        if self.form == "tokens":
            r = self.shape[0]
            s = pl.multiple_of(e * r, r)
            if half is None:
                return ref.at[pl.ds(s, r), :]
            c = self.shape[1] // 2
            return ref.at[pl.ds(s, r), pl.ds(pl.multiple_of(half * c, c), c)]
        c = self.shape[2]
        k = self.shape[0] // 2
        heads = slice(None) if half is None else pl.ds(half * k, k)
        return ref.at[heads, :, pl.ds(pl.multiple_of(d * c, c), c)]

    def own(self, ref, half=None):
        if half is None:
            return ref
        if self.form == "tokens":
            c = self.shape[1] // 2
            return ref.at[:, pl.ds(pl.multiple_of(half * c, c), c)]
        k = self.shape[0] // 2
        return ref.at[pl.ds(half * k, k)]


def gather_kernel(leaves, n, starts, *refs):
    m = len(leaves)
    ins, plain, refs = refs[:m], refs[m : m + 2], refs[m + 2 :]
    outs, turned, refs = refs[:m], refs[m : m + 2], refs[m + 2 :]
    stages = refs[:m]
    in_sem, out_sem, send_sem, recv_sem = refs[m:]
    d, e, t = lax.axis_index(DP), lax.axis_index(EXPERT), lax.axis_index(TENSOR)
    dx = d + 1 - 2 * lax.rem(d, 2)
    dy = lax.rem(d + 2, 4)
    dd = lax.rem(dx + 2, 4)
    near = {"x": {DP: dx}, "y": {DP: dy}, "r": {EXPERT: e + 1}, "l": {EXPERT: e - 1},
            "c": {TENSOR: 1 - t}}
    has = {"r": e < n - 1, "l": e > 0}

    barrier = pltpu.get_barrier_semaphore()
    for side in ("x", "y", "c"):
        pl.semaphore_signal(barrier, inc=1, device_id=near[side], device_id_type=MESH)
    for side in ("r", "l"):
        @pl.when(has[side])
        def _():
            pl.semaphore_signal(barrier, inc=1, device_id=near[side], device_id_type=MESH)
    pl.semaphore_wait(barrier, 3 + has["r"].astype(jnp.int32) + has["l"].astype(jnp.int32))

    for i in range(m):
        pltpu.make_async_copy(ins[i], stages[i], in_sem.at[i]).start()

    count = [0]
    table = {}

    def slot(key):
        if key not in table:
            table[key] = len(table)
        return table[key]

    def copy(src, dst, side, key):
        k = slot(key)
        return pltpu.make_async_remote_copy(
            src_ref=src, dst_ref=dst, send_sem=send_sem.at[k], recv_sem=recv_sem.at[k],
            device_id=near[side], device_id_type=MESH)

    sends = []

    def send(i, dd_, ee_, half, side, key, own=False, cond=None):
        leaf = leaves[i]
        dst = leaf.view(outs[i], dd_, ee_, half)
        src = leaf.own(ins[i], half) if own else dst
        c = copy(src, dst, side, key)
        if cond is None:
            c.start()
        else:
            pl.when(cond)(c.start)
        sends.append((c, cond))

    def arrive(i, dd_, ee_, half, key, cond=None):
        leaf = leaves[i]
        dst = leaf.view(outs[i], dd_, ee_, half)
        c = copy(dst, dst, "x", key)
        if cond is None:
            c.wait_recv()
        else:
            pl.when(cond)(c.wait_recv)

    work = []

    def plane(i, ee_, at, tag, cond, own):
        def s0():
            for half, side in ((0, "x"), (1, "y"), (1, "x"), (0, "y")):
                send(i, d, ee_, half, side, (i, tag, half, side), own=own, cond=cond)
        def s1():
            arrive(i, dx, ee_, 0, (i, tag, 0, "x"), cond)
            send(i, dx, ee_, 0, "y", (i, tag, 0, "fy"), cond=cond)
            arrive(i, dy, ee_, 1, (i, tag, 1, "y"), cond)
            send(i, dy, ee_, 1, "x", (i, tag, 1, "fx"), cond=cond)
        def s2():
            arrive(i, dx, ee_, 1, (i, tag, 1, "x"), cond)
            arrive(i, dy, ee_, 0, (i, tag, 0, "y"), cond)
        def s3():
            arrive(i, dd, ee_, 0, (i, tag, 0, "fy"), cond)
            arrive(i, dd, ee_, 1, (i, tag, 1, "fx"), cond)
        for k, f in enumerate((s0, s1, s2, s3)):
            work.append((at + k, f))

    def line(i, dd_, at, tag, own, then=None):
        def s0():
            for side in ("r", "l"):
                send(i, dd_, e, None, side, (i, tag, side, 1), own=own, cond=has[side])
        work.append((at, s0))
        for k in range(1, n):
            def step(k=k):
                for side, o, there in (("r", e - k, e >= k), ("l", e + k, e + k < n)):
                    arrive(i, dd_, o, None, (i, tag, side, k), there)
                    if k < n - 1:
                        go = jnp.logical_and(there, has[side])
                        send(i, dd_, o, None, side, (i, tag, side, k + 1), cond=go)
            work.append((at + k, step))

    def tokens(i, at):
        def s0():
            for side in ("r", "l"):
                send(i, d, e, t, side, (i, side, 1), own=True, cond=has[side])
        work.append((at, s0))
        for k in range(1, n):
            def step(k=k):
                for side, o, there in (("r", e - k, e >= k), ("l", e + k, e + k < n)):
                    arrive(i, d, o, t, (i, side, k), there)
                    if k < n - 1:
                        go = jnp.logical_and(there, has[side])
                        send(i, d, o, t, side, (i, side, k + 1), cond=go)
                    send(i, d, o, t, "c", (i, "c", side, k), cond=there)
            def last(k=k):
                for side, o, there in (("r", e - k, e >= k), ("l", e + k, e + k < n)):
                    arrive(i, d, o, 1 - t, (i, "c", side, k), there)
            work.append((at + k, step))
            work.append((at + k + 1, last))

    for i, leaf in enumerate(leaves):
        at = starts[i]
        if leaf.form == "tokens":
            tokens(i, at)
            continue
        if leaf.form == "expert":
            plane(i, 0, at, "p", None, True)
        elif leaf.first == "xy":
            plane(i, e, at, "p", None, True)
            line(i, d, at, "z0", True)
            line(i, dx, at + 2.2, "zx", False)
            line(i, dy, at + 2.2, "zy", False)
            line(i, dd, at + 3.2, "zd", False)
        else:
            plane(i, e, at, "p", None, True)
            line(i, d, at, "z0", True)
            for k in range(1, n):
                plane(i, e - k, at + k + 0.5, ("pr", k), e >= k, False)
                plane(i, e + k, at + k + 0.5, ("pl", k), e + k < n, False)

    def settle():
        for a, b in zip(plain, turned):
            b[...] = a[...].astype(F32).T.astype(b.dtype)
        for i in range(m):
            pltpu.make_async_copy(ins[i], stages[i], in_sem.at[i]).wait()
            pltpu.make_async_copy(stages[i], leaves[i].view(outs[i], d, e), out_sem.at[i]).start()
    work.append((1.2, settle))
    for _, f in sorted(work, key=lambda w: w[0]):
        f()
    for c, cond in sends:
        if cond is None:
            c.wait_send()
        else:
            pl.when(cond)(c.wait_send)
    for i in range(m):
        pltpu.make_async_copy(stages[i], leaves[i].view(outs[i], d, e), out_sem.at[i]).wait()
    assert len(table) <= recv_sem.shape[0], len(table)


def gather(arrays, forms, firsts, n, starts, plain):
    leaves = [Leaf(a.shape, a.dtype, f, o, n) for a, f, o in zip(arrays, forms, firsts)]
    total = 0
    for leaf in leaves:
        plane, line = 6, 2 * (n - 1)
        if leaf.form == "tokens":
            total += 2 * line
            continue
        total += plane if leaf.form == "expert" else plane + 4 * line if leaf.first == "xy" else plane * (2 * n - 1) + line
    m = len(leaves)
    anyspace, vmem = pl.BlockSpec(memory_space=pl.ANY), pl.BlockSpec(memory_space=pltpu.VMEM)
    return pl.pallas_call(
        functools.partial(gather_kernel, leaves, n, starts),
        out_shape=[jax.ShapeDtypeStruct(leaf.out, leaf.dtype) for leaf in leaves] + [
            jax.ShapeDtypeStruct(v.shape[::-1], v.dtype) for v in plain],
        in_specs=[anyspace] * m + [vmem] * 2,
        out_specs=[anyspace] * m + [vmem] * 2,
        scratch_shapes=[pltpu.VMEM(leaf.shape, leaf.dtype) for leaf in leaves] + [
            pltpu.SemaphoreType.DMA((m,)), pltpu.SemaphoreType.DMA((m,)),
            pltpu.SemaphoreType.DMA((total,)), pltpu.SemaphoreType.DMA((total,))],
        compiler_params=pltpu.CompilerParams(
            collective_id=0, has_side_effects=True, vmem_limit_bytes=60 << 20),
    )(*arrays, *plain)


message_rows = 5632
ring_slots = {"x": 4, "y": 4, "z": 6}


def scatter_items(dense, units, n):
    ends = [k // 2 if k % 2 == 0 else n - 1 - k // 2 for k in range(n)]
    items = [("a", k, "", 0) for k in range(4)]
    for i, (_, first) in enumerate(dense):
        names = [("z", t) for t in ends] if first == "z" else []
        names += [("p", s) for s in ("y1", "x1", "x2", "y2")]
        names += [("z", t) for t in ends] if first != "z" else []
        items += [("d", i) + name for name in names] + [("d", i, "out", 0)]
    for u in range(units):
        items += [("e", u, "p", s) for s in ("y1", "x1", "x2", "y2")] + [("e", u, "out", 0)]
    return items


def scatter_uses(item, m):
    kind, i = item[:2]
    if kind == "a":
        return (("hidden", "back", "few", "named", "gain_two", "router", "cot", "normed"),
                ("q", "k", "v", "cos", "sin", "mask"), (), ("inp", "gain_one"))[i]
    if kind == "e":
        return (("ggp", "rows_all"), ("gup", "rows_all"), ("act", "cot_all", "gates"))[i // 2]
    return (("one_t",), ("one_t",), ("one_t",), ("mixed_t",), ("two_t", "gsg"), ("two_t", "gsu"),
            ("sact_t", "cot"), ("normed",))[i]


def scatter_kernel(dense, units, n, order, names, experts, *refs):
    m = len(dense)
    c_ = len(names)
    given = dict(zip(names, refs[:c_]))
    w_out, w_qkv = refs[c_], refs[c_ + 1 : c_ + 4]
    refs = refs[c_ + 4 :]
    box, refs = types.SimpleNamespace(**dict(zip(names, refs[-c_:]))), refs[:-c_]
    (in_sem, logits_t, gq, gk, gv, gattn, extra, gm, wbuf, gh, part, other, rhs, w_sem, pair_send, pair_recv,
     small_out) = refs[-17:]
    refs = refs[:-17]
    own_grads = (gq, gk, gv)
    lefts = (box.one_t,) * 3 + (box.mixed_t, box.two_t, box.two_t, box.sact_t, logits_t)
    rights = own_grads + (gattn, box.gsg, box.gsu, box.cot, box.normed)
    exp_left = (box.ggp, box.gup, box.act)
    rows_all = box.rows_all
    here_yet = set()

    def fetch(name):
        k = names.index(name)
        return pltpu.make_async_copy(given[name], getattr(box, name), in_sem.at[k])

    def need(item):
        for name in scatter_uses(item, m):
            if name not in here_yet:
                here_yet.add(name)
                fetch(name).wait()

    steps = scatter_items(dense, units, n)
    steps = [steps[k] for k in order] if order else steps
    for name in dict.fromkeys(v for it in steps for v in scatter_uses(it, m)):
        fetch(name).start()
    input_out, refs = refs[m + 3], refs[: m + 3] + refs[m + 4 :]
    outs, refs = refs[: m + 3], refs[m + 3 :]
    landed, refs = refs[: 3 * m + 2], refs[3 * m + 2 :]
    bufs = dict(zip("xyz", refs[:3]))
    held, tall, wide = refs[3:6]
    stage_sem, load_sem, recv_sem = refs[6:9]
    send_sems = dict(zip("xyz", refs[9:12]))
    d, e = lax.axis_index("dp"), lax.axis_index("expert")
    dx = d + 1 - 2 * lax.rem(d, 2)
    dy = lax.rem(d + 2, 4)
    dd = lax.rem(dx + 2, 4)
    after, before = e < n - 1, e > 0

    barrier = pltpu.get_barrier_semaphore()
    partner = {"tensor": 1 - lax.axis_index("tensor")}
    for dev in ({"dp": dx}, {"dp": dy}, partner):
        pl.semaphore_signal(barrier, inc=1, device_id=dev, device_id_type=MESH)
    for cond, dev in ((after, {"expert": e + 1}), (before, {"expert": e - 1})):
        @pl.when(cond)
        def _():
            pl.semaphore_signal(barrier, inc=1, device_id=dev, device_id_type=MESH)
    pl.semaphore_wait(barrier, 3 + after.astype(jnp.int32) + before.astype(jnp.int32))
    held[...] = jnp.zeros_like(held)

    def when(cond, f):
        if cond is None:
            f()
        else:
            pl.when(cond)(f)

    sems = {}

    def sem_of(key, count=1):
        if key not in sems:
            sems[key] = sum(c for _, c in sems.values()), count
        return sems[key][0]

    turns = {"x": 0, "y": 0, "z": 0}
    pending = {}

    def slot(side):
        k = turns[side] % ring_slots[side]
        turns[side] += 1
        if (side, k) in pending:
            c, cond = pending.pop((side, k))
            when(cond, c.wait_send)
        return k

    def send(side, k, rows, dst, sem, dev, cond=None):
        c = pltpu.make_async_remote_copy(
            src_ref=bufs[side].at[k, pl.ds(0, rows)], dst_ref=dst,
            send_sem=send_sems[side].at[k], recv_sem=recv_sem.at[sem],
            device_id=dev, device_id_type=MESH)
        when(cond, c.start)
        pending[(side, k)] = (c, cond)

    seen = set()

    def arrived(key, view, sem, cond=None):
        if key in seen:
            return
        seen.add(key)
        c = pltpu.make_async_remote_copy(
            src_ref=view, dst_ref=view, send_sem=recv_sem.at[sem], recv_sem=recv_sem.at[sem],
            device_id={"dp": dx}, device_id_type=MESH)
        when(cond, c.wait_recv)

    class Loads:
        def __init__(self):
            self.list = []

        def add(self, src, k, off, cond=None):
            rows = src.shape[0]
            c = pltpu.make_async_copy(src, held.at[k, pl.ds(off, rows)], load_sem.at[len(self.list)])
            when(cond, c.start)
            self.list.append((c, cond))

        def wait(self):
            for c, cond in self.list:
                when(cond, c.wait)

    def dense_piece(i, d_, e_, half, put):
        kind = dense[i][0]
        block = d_ * n + e_
        if kind == "rows":
            width = rights[i].shape[1]
            r = lefts[i].shape[0] // (4 * n)
            left = lefts[i][pl.ds(pl.multiple_of(block * r + half * (r // 2), r // 2), r // 2), :]
            for c in range(0, width, 256):
                w = min(256, width - c)
                res = jnp.dot(left, rights[i][:, c : c + w], preferred_element_type=F32)
                for k in range(0, w, 128):
                    put((c + k) // 128 * (r // 2), res[:, k : k + 128], c + k)
        else:
            half_rows = lefts[i].shape[0] // 2
            right = rights[i][:, pl.ds(pl.multiple_of(block * 128, 128), 128)]
            step = half_rows // 2
            for r in range(0, half_rows, step):
                left = lefts[i][pl.ds(pl.multiple_of(half * half_rows + r, 16), step), :]
                res = jnp.dot(left, right, preferred_element_type=F32)
                if i == m - 1:
                    at = pl.ds(pl.multiple_of(half * half_rows + r, 16), step)
                    res = res + extra[at, pl.ds(pl.multiple_of(block * 128, 128), 128)]
                put(r, res, 0)

    def half_rows_of(i):
        if dense[i][0] == "rows":
            return lefts[i].shape[0] // (8 * n) * rights[i].shape[1] // 128
        return lefts[i].shape[0] // 2

    def total(value, row, adds):
        rows = value.shape[0]
        for k, off, flag in adds:
            more = held[k, pl.ds(pl.multiple_of(off + row, 16), rows), :].astype(F32)
            value = value + (more if flag is None else jnp.where(flag, more, 0.0))
        return value

    def into(side, k, base, adds):
        def put(row, value, col):
            value = total(value, row, adds)
            start = pl.multiple_of(base + row, 16)
            bufs[side][k, pl.ds(start, value.shape[0]), :] = value.astype(jnp.bfloat16)
        return put

    out_busy = {}

    def out_wait(which):
        if which in out_busy:
            out_busy.pop(which).wait()

    def dense_step(i, stage, arg):
        z_land, first_land, second_land = landed[3 * i : 3 * i + 3]
        z_first = dense[i][1] == "z"
        hb = half_rows_of(i)
        z_rows = (8 if z_first else 2) * hb
        z_sem = sem_of(("z", i), 2 * n)
        groups = 1 if z_first else n
        p_sem = {s: sem_of((s, i)) for s in ("y1", "x1", "x2", "y2")}
        place = {"y1": (first_land, 0, 2), "x1": (first_land, 1, 2), "x2": (second_land, 0, 1), "y2": (second_land, 1, 1)}

        def view(s, g0, gs, sub):
            land, which, pieces = place[s]
            if sub is None:
                return land.at[which, pl.ds(0, groups * pieces * hb)]
            return land.at[which, pl.ds(pl.multiple_of((g0 * pieces + sub) * hb, hb), gs * hb)]

        def plane_arrived(s):
            arrived((s, i), view(s, 0, 0, None), p_sem[s])

        def own_line(ld, k, off, d_, half, rows):
            for side, there in ((0, after), (1, before)):
                arrived(("own", i, side), z_land.at[side, e], z_sem + side * n + e, there)
                src = z_land.at[side, e, pl.ds(pl.multiple_of((2 * d_ + half) * hb, hb), rows)]
                ld.add(src, k + side, off, there)

        def plane_out(ld, g):
            for s in ("y1", "x1", "x2", "y2"):
                plane_arrived(s)
            ld.add(view("y1", g, 1, 1), 2, 0)
            ld.add(view("x1", g, 1, 1), 2, hb)
            ld.add(view("x2", g, 1, 0), 3, 0)
            ld.add(view("y2", g, 1, 0), 3, hb)

        if stage == "z":
            t = arg
            side = 1 - (e + n - t) // n
            more = jnp.logical_or(jnp.logical_and(e > t, after), jnp.logical_and(e < t, before))
            cond = e != t
            k = slot("z")
            def go():
                ld = Loads()
                land = z_land.at[side, t]
                arrived(("pass", i, t), land, z_sem + side * n + t, more)
                ld.add(land, 0, 0, more)
                if not z_first:
                    plane_out(ld, t)
                ld.wait()
                if z_first:
                    def one(h, _):
                        dense_piece(i, h // 2, t, h % 2, into("z", k, h * hb, [(0, h * hb, more)]))
                        return 0
                    lax.fori_loop(0, 8, one, 0)
                else:
                    def one(h, _):
                        dense_piece(i, d, t, h, into("z", k, h * hb, [(0, h * hb, more), (2, h * hb, None), (3, h * hb, None)]))
                        return 0
                    lax.fori_loop(0, 2, one, 0)
            if not z_first:
                for s in ("y1", "x1", "x2", "y2"):
                    plane_arrived(s)
            pl.when(cond)(go)
            send("z", k, z_rows, z_land.at[side, t], z_sem + side * n + t, {"expert": e - 1 + 2 * side}, cond)
        elif stage == "p":
            s = arg
            link = s[0]
            dev = {"dp": dy if link == "y" else dx}
            half = 0 if s in ("y1", "x2") else 1
            k = slot(link)
            ld = Loads()
            if s in ("y1", "x1"):
                owners = (dd, dy if link == "y" else dx)
                if z_first:
                    for q, o in enumerate(owners):
                        own_line(ld, 0, q * hb, o, half, hb)
                    ld.wait()
                    for q, o in enumerate(owners):
                        dense_piece(i, o, e, half, into(link, k, q * hb, [(0, q * hb, after), (1, q * hb, before)]))
                else:
                    def one(g, _):
                        for q, o in enumerate(owners):
                            dense_piece(i, o, g, half, into(link, k, (2 * g + q) * hb, []))
                        return 0
                    lax.fori_loop(0, n, one, 0)
                send(link, k, groups * 2 * hb, view(s, 0, 0, None), p_sem[s], dev)
            else:
                o = dx if link == "x" else dy
                prior = "y1" if s == "x2" else "x1"
                plane_arrived(prior)
                if z_first:
                    own_line(ld, 0, 0, o, half, hb)
                    ld.add(view(prior, 0, 1, 0), 2, 0)
                    ld.wait()
                    dense_piece(i, o, e, half, into(link, k, 0, [(0, 0, after), (1, 0, before), (2, 0, None)]))
                else:
                    ld.add(view(prior, 0, 0, None), 2, 0)
                    ld.wait()
                    def one(g, _):
                        dense_piece(i, o, g, half, into(link, k, g * hb, [(2, 2 * g * hb, None)]))
                        return 0
                    lax.fori_loop(0, n, one, 0)
                send(link, k, groups * hb, view(s, 0, 0, None), p_sem[s], dev)
        else:
            ld = Loads()
            if z_first:
                own_line(ld, 0, 0, d, 0, 2 * hb)
                plane_out(ld, 0)
            else:
                for side, there in ((0, after), (1, before)):
                    arrived(("own", i, side), z_land.at[side, e], z_sem + side * n + e, there)
                    ld.add(z_land.at[side, e], side, 0, there)
                plane_out(ld, e)
            rows = dense[i][0] == "rows"
            which = "wide" if rows else "slim"
            out_wait(which)
            ld.wait()
            def one(h, _):
                adds = [(0, h * hb, after), (1, h * hb, before), (2, h * hb, None), (3, h * hb, None)]
                def put(row, value, col):
                    value = total(value, row, adds)
                    if rows:
                        r = value.shape[0]
                        wide[pl.ds(pl.multiple_of(h * r, r), r), col : col + 128] = value
                    else:
                        small_out[pl.ds(pl.multiple_of(h * hb + row, 16), value.shape[0]), :] = value
                dense_piece(i, d, e, h, put)
                return 0
            lax.fori_loop(0, 2, one, 0)
            if rows:
                src = wide.at[:, pl.ds(0, outs[i].shape[1])]
            else:
                src = small_out.at[pl.ds(0, outs[i].shape[0])]
            c = pltpu.make_async_copy(src, outs[i], stage_sem.at[0 if rows else 3])
            c.start()
            out_busy[which] = c

    first_exp, second_exp = landed[3 * m], landed[3 * m + 1]

    def expert_step(u, stage, s):
        a, q = u // 2, u % 2
        rows, width = exp_left[a].shape[1], outs[m + a].shape[2]
        tiles = width // 128
        piece = rows * tiles
        step = rows // 4
        sem = {s_: sem_of((s_, "e", u)) for s_ in ("y1", "x1", "x2", "y2")}
        place = {"y1": (first_exp, 0, 2), "x1": (first_exp, 1, 2), "x2": (second_exp, 0, 1), "y2": (second_exp, 1, 1)}

        def view(s_, sub=None):
            land, which, pieces = place[s_]
            if sub is None:
                return land.at[u, which]
            return land.at[u, which, pl.ds(sub * piece, piece)]

        def one_piece(j, d_, put):
            if a == 2:
                for r in range(0, rhs.shape[0], 128):
                    gate = box.gates[r : r + 128, :][:, j : j + 1]
                    ct = box.cot_all[r : r + 128, pl.ds(pl.multiple_of(d_ * width, 128), width)]
                    rhs[r : r + 128, :] = (gate * ct.astype(F32)).astype(jnp.bfloat16)
            def body(r, _):
                left = exp_left[a][j, pl.ds(pl.multiple_of(r * step, 16), step), :]
                cols = pl.ds(pl.multiple_of(d_ * width, 128), width)
                right = rhs[...] if a == 2 else rows_all[:, cols]
                res = jnp.dot(left, right, preferred_element_type=F32)
                for c in range(tiles):
                    put(c * rows + r * step, res[:, c * 128 : (c + 1) * 128], (r * step, c * 128))
                return 0
            lax.fori_loop(0, 4, body, 0)

        def get(s_):
            arrived((s_, "e", u), view(s_), sem[s_])

        ld = Loads()
        if stage == "p":
            link = s[0]
            dev = {"dp": dy if link == "y" else dx}
            j = q if s in ("y1", "x2") else q + 2
            k = slot(link)
            if s in ("y1", "x1"):
                for b, o in enumerate((dd, dy if link == "y" else dx)):
                    one_piece(j, o, into(link, k, b * piece, []))
                send(link, k, 2 * piece, view(s), sem[s], dev)
            else:
                prior = "y1" if s == "x2" else "x1"
                get(prior)
                ld.add(view(prior, 0), 0, 0)
                ld.wait()
                one_piece(j, dx if link == "x" else dy, into(link, k, 0, [(0, 0, None)]))
                send(link, k, piece, view(s), sem[s], dev)
        else:
            for b, (j, one, two) in enumerate(((q, "y1", "x2"), (q + 2, "x1", "y2"))):
                get(one)
                get(two)
                ld.add(view(one, 1), 2 * b, 0)
                ld.add(view(two, 0), 2 * b + 1, 0)
            out_wait("tall")
            ld.wait()
            for b, j in enumerate((q, q + 2)):
                adds = [(2 * b, 0, None), (2 * b + 1, 0, None)]
                def put(row, value, at):
                    value = total(value, row, adds)
                    r, c = at
                    tall[b, pl.ds(pl.multiple_of(r, 16), value.shape[0]), c : c + 128] = value
                one_piece(j, d, put)
            cs = [pltpu.make_async_copy(tall.at[b, pl.ds(0, rows), pl.ds(0, width)], outs[m + a].at[q + 2 * b], stage_sem.at[1 + b]) for b in range(2)]
            for c in cs:
                c.start()
            class Both:
                def wait(self):
                    for c in cs:
                        c.wait()
            out_busy["tall"] = Both()

    width_all = gh.shape[1]
    chunk = wbuf.shape[1]
    plan = [w_out.at[:, pl.ds(c * chunk, chunk)] for c in range(width_all // chunk)]
    plan += [w.at[pl.ds(c * chunk, chunk)] for c in range(width_all // chunk) for w in w_qkv]

    def weight(k):
        return pltpu.make_async_copy(plan[k], wbuf.at[k % 2], w_sem.at[k % 2])

    def a_t_b(a, b):
        return lax.dot_general(a, b, (((1,), (1,)), ((), ())), preferred_element_type=F32)

    def attn_step(k):
        if k == 0:
            weight(0).start()
            weight(1).start()
            logits = a_t_b(box.normed[...], box.router[...])
            lane = lax.broadcasted_iota(jnp.int32, logits.shape, 1)
            logits = jnp.where(lane < experts, logits, -1e30)
            ex = jnp.exp(logits - jnp.max(logits, axis=-1, keepdims=True))
            probs = ex / jnp.sum(ex, axis=-1, keepdims=True)
            grads = jnp.where(box.named[...] > 0.0, box.few[...], 0.0)
            grads = probs * (grads - jnp.sum(grads * probs, axis=-1, keepdims=True))
            logits_t[...] = grads.T[: logits_t.shape[0], :].astype(jnp.bfloat16)
            extra[...] = jnp.zeros_like(extra)
            gains = jnp.zeros((1, width_all), F32)
            for r in range(0, gh.shape[0], 32):
                p = slice(r, r + 32)
                low = grads[p].astype(jnp.bfloat16)
                gn = box.back[p, :] + jnp.dot(low, box.router[...], preferred_element_type=F32)
                h = box.hidden[p, :]
                scale = lax.rsqrt(jnp.mean(h * h, axis=-1, keepdims=True) + epsilon)
                gains = gains + jnp.sum(gn * h * scale, axis=0, keepdims=True)
                w = gn * box.gain_two[...]
                g = (box.cot[p, :].astype(F32) + scale * w
                     - h * (scale * scale * scale) * jnp.mean(h * w, axis=-1, keepdims=True))
                gh[p, :] = g
                gattn[p, :] = g.astype(jnp.bfloat16)
            extra[experts + 1 : experts + 2, :] = gains
        elif k == 1:
            count = width_all // chunk
            for c in range(count):
                weight(c).wait()
                piece = a_t_b(gattn[:, c * chunk : (c + 1) * chunk], wbuf[c % 2])
                weight(c + 2).start()
                part[:, : piece.shape[1]] = piece if c == 0 else part[:, : piece.shape[1]] + piece
            gm[...] = part[:, : gm.shape[1]].astype(jnp.bfloat16)
            root = 1.0 / math.sqrt(HD)
            for h in range(gm.shape[1] // HD):
                cols = slice(h * HD, (h + 1) * HD)
                q, kk, v, g = box.q[:, cols], box.k[:, cols], box.v[:, cols], gm[:, cols]
                scores = a_t_b(q, kk) / math.sqrt(HD)
                scores = jnp.where(box.mask[...] > 0.0, scores, masked_score)
                ex = jnp.exp(scores - jnp.max(scores, axis=-1, keepdims=True))
                prob = ex / jnp.sum(ex, axis=-1, keepdims=True)
                gp = a_t_b(g, v)
                gs = prob * (gp - jnp.sum(prob * gp, axis=-1, keepdims=True))
                gv[:, cols] = jnp.dot(prob.T.astype(jnp.bfloat16), g, preferred_element_type=F32).astype(jnp.bfloat16)
                for dst, left, right in ((gq, gs, kk), (gk, gs.T, q)):
                    u = jnp.dot(left.astype(jnp.bfloat16), right, preferred_element_type=F32) * root
                    u = u * box.cos[...] + pltpu.roll(u, HD // 2, 1) * box.sin[...]
                    dst[:, cols] = u.astype(jnp.bfloat16)
        elif k == 2:
            base = width_all // chunk
            for c in range(width_all // chunk):
                cols = slice(c * chunk, (c + 1) * chunk)
                for j in range(3):
                    i = base + 3 * c + j
                    weight(i).wait()
                    piece = a_t_b(own_grads[j][...], wbuf[i % 2])
                    if i + 2 < len(plan):
                        weight(i + 2).start()
                    part[:, cols] = piece if j == 0 else part[:, cols] + piece
            pair_copy().start()
        else:
            pair_copy().wait_recv()
            gains = jnp.zeros((1, width_all), F32)
            for r in range(0, gh.shape[0], 32):
                p = slice(r, r + 32)
                gn = part[p, :] + other[p, :]
                x = box.inp[p, :].astype(F32)
                scale = lax.rsqrt(jnp.mean(x * x, axis=-1, keepdims=True) + epsilon)
                gains = gains + jnp.sum(gn * x * scale, axis=0, keepdims=True)
                w = gn * box.gain_one[...]
                gh[p, :] = (gh[p, :] + scale * w
                            - x * (scale * scale * scale) * jnp.mean(x * w, axis=-1, keepdims=True))
            extra[experts : experts + 1, :] = gains
            c = pltpu.make_async_copy(gh, input_out, stage_sem.at[4])
            c.start()
            out_busy["input"] = c

    def pair_copy():
        return pltpu.make_async_remote_copy(
            src_ref=part, dst_ref=other, send_sem=pair_send, recv_sem=pair_recv,
            device_id=partner, device_id_type=MESH)

    for item in steps:
        kind, i, stage, arg = item
        need(item)
        if kind == "a":
            attn_step(i)
        else:
            (dense_step if kind == "d" else expert_step)(i, stage, arg)
    pair_copy().wait_send()
    for c, cond in pending.values():
        when(cond, c.wait_send)
    for which in list(out_busy):
        out_wait(which)
    assert sum(c for _, c in sems.values()) <= recv_sem.shape[0]


def scatter(dense, given, weights, experts, n, order, cid):
    m, units = len(dense), 6
    bf, dma, vm = jnp.bfloat16, pltpu.SemaphoreType.DMA, pltpu.VMEM
    toks, width = given["hidden"].shape
    heads = given["q"].shape[1]
    room = experts + 2 + (-(experts + 2) % 64)
    left = dict(zip(range(m), ("one_t", "one_t", "one_t", "mixed_t", "two_t", "two_t", "sact_t")))
    outs, landed = [], []
    for i, (kind, first) in enumerate(dense):
        rows = given[left[i]].shape[0] if i in left else room
        if kind == "rows":
            r = rows // (4 * n)
            cols = heads if i < 3 else given["gsg"].shape[1]
            shape, hb = (r, cols), r // 2 * cols // 128
        else:
            shape, hb = (rows, 128), rows // 2
        outs.append(jax.ShapeDtypeStruct(shape, F32))
        g, z = (1, 8) if first == "z" else (n, 2)
        landed += [jax.ShapeDtypeStruct((2, n, z * hb, 128), bf),
                   jax.ShapeDtypeStruct((2, g * 2 * hb, 128), bf),
                   jax.ShapeDtypeStruct((2, g * hb, 128), bf)]
    here, rows = given["act"].shape[:2]
    cut = width // 4
    tall_rows = max(o.shape[0] for o in outs)
    wide_cols = max(o.shape[1] for o in outs)
    outs += [jax.ShapeDtypeStruct((here, rows, cut), F32)] * 3
    outs.append(jax.ShapeDtypeStruct((toks, width), F32))
    piece = rows * cut // 128
    landed += [jax.ShapeDtypeStruct((units, 2, 2 * piece, 128), bf),
               jax.ShapeDtypeStruct((units, 2, piece, 128), bf)]
    anyspace = pl.BlockSpec(memory_space=pl.ANY)
    count = m * (2 * n + 4) + 4 * units
    names = tuple(given)
    res = pl.pallas_call(
        functools.partial(scatter_kernel, dense, units, n, order, names, experts),
        out_shape=outs + landed,
        in_specs=[anyspace] * (len(names) + 4),
        out_specs=[anyspace] * (len(outs) + len(landed)),
        scratch_shapes=[vm((ring_slots[s], message_rows, 128), bf) for s in "xyz"] + [
            vm((4, message_rows, 128), bf), vm((2, rows, cut), F32), vm((128, wide_cols), F32),
            dma((5,)), dma((8,)), dma((count,))] + [dma((ring_slots[s],)) for s in "xyz"] + [
            dma((len(names),)), vm((room, toks), bf)] + [vm((toks, heads), bf)] * 3 + [
            vm((toks, width), bf), vm((room, width), F32), vm((toks, heads), bf),
            vm((2, width // 2, heads), bf), vm((toks, width), F32), vm((toks, width), F32),
            vm((toks, width), F32), vm((n * toks, cut), bf), dma((2,)), dma, dma, vm((tall_rows, 128), F32),
        ] + [vm(v.shape, v.dtype) for v in given.values()],
        compiler_params=pltpu.CompilerParams(
            collective_id=cid, has_side_effects=True, vmem_limit_bytes=67043328),
    )(*given.values(), *weights)
    return res[: m + 4]


def across(a, b):
    return lax.dot_general(a, b, (((1,), (1,)), ((), ())), preferred_element_type=F32)


def times(a, b):
    return jnp.dot(a, b, preferred_element_type=F32)


def middle_items(n, here):
    items = [("join",), ("gates",), ("settle",)]
    for q in range(2):
        items += [("tok", q, k) for k in range(n)] + [("tokend", q)]
    for i in range(3):
        items += [("plane", 12 + i, s) for s in range(4)]
        items += [("line", i, b, k) for b in range(4) for k in range(n)]
    for j in range(here):
        for a in range(3):
            items += [("plane", 3 * j + a, s) for s in range(4)]
        items += [(name, j) for name in ("load", "load_down", "pre", "front", "back", "rows")]
    for v in range(2):
        items += [("shared_load", v), ("shared", v), ("fold_start", v), ("fold_lines", v)]
    return items + [("fold_shared",), ("fold_end",)]


def middle_kernel(n, order, *refs):
    (part, inp, gain, router, named, cot_own, one, mixed, gate_in, up_in, down_in, sg_in, su_in, sd_in) = refs[:14]
    refs = refs[14:]
    (hidden, normed, rows_all, few, gn2, ffn, act_t, ggp_t, gup_t, gates, cot,
     gsg, gsu, sact_t, one_t, two_t, mixed_t) = refs[:17]
    exp_land, sh_land = refs[17:20], refs[20:23]
    refs = refs[23:]
    (other, weights, back, routed, gpre, upre, act, grad, copy_buf, turned, eye,
     sh_stage, dot_sums, fold_other, fold_own, fold_out, fold_in, few_other, few_out, few_in,
     ffn_own, gn_own) = refs[:22]
    (pair_send, pair_recv, row_send, row_recv, plane_send, plane_recv, line_send, line_recv,
     load_sem, out_sem, stage_sem, zsend, zrecv) = refs[22:]
    ins = (gate_in, up_in, down_in)
    sh_ins = (sg_in, su_in, sd_in)
    here, hid, width = gate_in.shape
    toks = inp.shape[0]
    alltoks = n * toks
    D_ = inp.shape[1]
    half = D_ // 2
    d, e, t = lax.axis_index(DP), lax.axis_index(EXPERT), lax.axis_index(TENSOR)
    dx = d + 1 - 2 * lax.rem(d, 2)
    dy = lax.rem(d + 2, 4)
    dd = lax.rem(dx + 2, 4)
    after, before = e < n - 1, e > 0
    near = {"x": {DP: dx}, "y": {DP: dy}, "r": {EXPERT: e + 1}, "l": {EXPERT: e - 1},
            "c": {TENSOR: 1 - t}}
    peers = [lax.rem(e + k, n) for k in range(1, n)]
    mine = pl.ds(pl.multiple_of(t * half, half), half)
    theirs = pl.ds(pl.multiple_of((1 - t) * half, half), half)

    barrier = pltpu.get_barrier_semaphore()
    for dev in [near["x"], near["y"], near["c"]] + [{EXPERT: p} for p in peers]:
        pl.semaphore_signal(barrier, inc=1, device_id=dev, device_id_type=MESH)
    pl.semaphore_wait(barrier, 3 + n - 1)

    def when(cond, f):
        if cond is None:
            f()
        else:
            pl.when(cond)(f)

    sends = []

    def remote(src, dst, ssem, rsem, dev, cond=None, start=True):
        c = pltpu.make_async_remote_copy(
            src_ref=src, dst_ref=dst, send_sem=ssem, recv_sem=rsem, device_id=dev,
            device_id_type=MESH)
        if start:
            when(cond, c.start)
            sends.append((c, cond))
        return c

    def block(p):
        return pl.ds(pl.multiple_of(p * toks, toks), toks)

    first = [remote(part.at[pl.ds(k * (toks // 2), toks // 2)], other.at[pl.ds(k * (toks // 2), toks // 2)],
                    pair_send.at[k], pair_recv.at[k], near["c"]) for k in range(2)]
    for i in range(3):
        pltpu.make_async_copy(sh_ins[i], sh_stage.at[i], stage_sem.at[i]).start()

    def join():
        for k, c in enumerate(first):
            c.wait_recv()
            p = pl.ds(k * (toks // 2), toks // 2)
            h = inp[p, :].astype(F32) + (part[p, :] + other[p, :])
            scale = lax.rsqrt(jnp.mean(h * h, axis=-1, keepdims=True) + epsilon)
            hidden[p, :] = h
            rows = (h * scale * gain[...]).astype(jnp.bfloat16)
            normed[p, :] = rows
            rows_all[pl.ds(pl.multiple_of(e * toks + k * (toks // 2), toks // 2), toks // 2), :] = rows
        two_t[...] = normed[...].astype(F32).T.astype(jnp.bfloat16)

    def along(k):
        return (("r", e - k, e >= k, after, 0), ("l", e + k, e + k < n, before, 1))

    def tok_step(q, k):
        every = (rows_all, cot)[q]
        base = 4 * (n - 1) * q
        if k == 0:
            src = (normed, cot_own)[q]
            for side, has, w in (("r", after, 0), ("l", before, 1)):
                s = base + (n - 1) * w
                remote(src.at[:, mine], every.at[block(e), mine], row_send.at[s], row_recv.at[s], near[side], has)
            return
        for side, o, there, has, w in along(k):
            view = every.at[block(o), mine]
            s = base + (n - 1) * w + k - 1
            when(there, remote(view, view, row_send.at[s], row_recv.at[s], near[side], start=False).wait_recv)
            if k < n - 1:
                remote(view, view, row_send.at[s + 1], row_recv.at[s + 1], near[side], jnp.logical_and(there, has))
            s += 2 * (n - 1)
            remote(view, view, row_send.at[s], row_recv.at[s], near["c"], there)

    def tok_end(q):
        every = (rows_all, cot)[q]
        for k in range(1, n):
            for side, o, there, has, w in along(k):
                view = every.at[block(o), theirs]
                s = 4 * (n - 1) * q + (n - 1) * (2 + w) + k - 1
                when(there, remote(view, view, row_send.at[s], row_recv.at[s], near["c"], start=False).wait_recv)

    def gates_step():
        cot[block(e), :] = cot_own[...]
        one_t[...] = one[...].astype(F32).T.astype(jnp.bfloat16)
        mixed_t[...] = mixed[...].astype(F32).T.astype(jnp.bfloat16)
        logits = across(rows_all[...], router[...])
        lane = lax.broadcasted_iota(jnp.int32, logits.shape, 1)
        logits = jnp.where(lane < 4 * n, logits, -1e30)
        top = jnp.max(logits, axis=-1, keepdims=True)
        ex = jnp.exp(logits - top)
        pr = ex / jnp.sum(ex, axis=-1, keepdims=True)
        gates[...] = pr * named[...].astype(F32)
        back[...] = jnp.zeros_like(back)
        routed[...] = jnp.zeros_like(routed)
        dot_sums[...] = jnp.zeros_like(dot_sums)
        ffn_own[...] = jnp.zeros_like(ffn_own)
        gn_own[...] = jnp.zeros_like(gn_own)
        r = lax.broadcasted_iota(jnp.int32, eye.shape, 0)
        c = lax.broadcasted_iota(jnp.int32, eye.shape, 1)
        eye[...] = jnp.where(r == c, 1.0, 0.0).astype(jnp.bfloat16)

    def plane_view(i, o, h):
        if i < 12:
            k = hid // 2
            return exp_land[i % 3].at[i // 3, pl.ds(h * k, k), pl.ds(pl.multiple_of(o * width, width), width)]
        k = sh_land[i - 12].shape[0] // 2
        return sh_land[i - 12].at[pl.ds(h * k, k), pl.ds(pl.multiple_of((o * n + e) * 128, 128), 128)]

    def plane_own(i, h):
        if i < 12:
            k = hid // 2
            return ins[i % 3].at[i // 3, pl.ds(h * k, k)]
        k = sh_land[i - 12].shape[0] // 2
        return sh_ins[i - 12].at[pl.ds(h * k, k)]

    kinds = ("x0", "y1", "x1", "y0", "f0", "f1")

    def plane_copy(i, o, h, side, kind, own=False, start=True):
        s = 6 * i + kinds.index(kind)
        dst = plane_view(i, o, h)
        return remote(plane_own(i, h) if own else dst, dst, plane_send.at[s], plane_recv.at[s], near[side], start=start)

    def plane_step(i, s):
        if s == 0:
            plane_copy(i, d, 0, "x", "x0", own=True)
            plane_copy(i, d, 1, "y", "y1", own=True)
            plane_copy(i, d, 1, "x", "x1", own=True)
            plane_copy(i, d, 0, "y", "y0", own=True)
        elif s == 1:
            plane_copy(i, dx, 0, "x", "x0", start=False).wait_recv()
            plane_copy(i, dx, 0, "y", "f0")
            plane_copy(i, dy, 1, "x", "y1", start=False).wait_recv()
            plane_copy(i, dy, 1, "x", "f1")
        elif s == 2:
            plane_copy(i, dx, 1, "x", "x1", start=False).wait_recv()
            plane_copy(i, dy, 0, "x", "y0", start=False).wait_recv()
        else:
            plane_copy(i, dd, 0, "x", "f0", start=False).wait_recv()
            plane_copy(i, dd, 1, "x", "f1", start=False).wait_recv()

    def line_view(i, o, eo):
        return sh_land[i].at[:, pl.ds(pl.multiple_of((o * n + eo) * 128, 128), 128)]

    def line_step(i, b, k):
        o = (d, dx, dy, dd)[b]
        base = (i * 4 + b) * 2 * (n - 1)

        def copy(eo, side, hop, own=False, cond=None, start=True):
            s = base + (0 if side == "r" else n - 1) + hop - 1
            dst = line_view(i, o, eo)
            return remote(sh_ins[i] if own else dst, dst, line_send.at[s], line_recv.at[s], near[side], cond, start)

        if k == 0:
            copy(e, "r", 1, b == 0, after)
            copy(e, "l", 1, b == 0, before)
            return
        for side, eo, there, has in (("r", e - k, e >= k, after), ("l", e + k, e + k < n, before)):
            when(there, copy(eo, side, k, start=False).wait_recv)
            if k < n - 1:
                copy(eo, side, k + 1, cond=jnp.logical_and(there, has))

    loads = {}

    def load(j, arrays=(0, 1)):
        cs = []
        for a in arrays:
            for q, o in enumerate((d, dx, dy, dd)):
                cols = pl.ds(pl.multiple_of(o * width, width), width)
                src = ins[a].at[j] if q == 0 else exp_land[a].at[j, :, cols]
                c = pltpu.make_async_copy(src, weights.at[j % 2, a, :, cols], load_sem.at[j % 2, 4 * a + q])
                c.start()
                cs.append(c)
        loads[j, arrays] = cs

    def load_down(j):
        load(j, (2,))

    writes = []
    waiting = {}

    def write(src, dst, k):
        c = pltpu.make_async_copy(src, dst, out_sem.at[k])
        c.start()
        waiting[k] = c

    def free(k):
        if k in waiting:
            waiting.pop(k).wait()

    def ffn_front(rows, count, w):
        step = min(256, count)
        def pre(m, _):
            r = pl.ds(pl.multiple_of(m * step, step), step)
            x = rows[r, :]
            g = across(x, w(0))
            u = across(x, w(1))
            gpre[r, :] = g
            upre[r, :] = u
            act[r, :] = (g * jax.nn.sigmoid(g) * u).astype(jnp.bfloat16)
            return 0
        lax.fori_loop(0, count // step, pre, 0)

    def pre_step(j):
        for c in loads.pop((j, (0, 1))):
            c.wait()
        ffn_front(rows_all, alltoks, lambda a: weights[j % 2, a])

    def front(j):
        for c in loads.pop((j, (2,))):
            c.wait()
        lane = lax.broadcasted_iota(jnp.int32, (256, 128), 1)
        def out(k, _):
            m, c = k // 4, k % 4
            r = pl.ds(pl.multiple_of(m * 256, 256), 256)
            cols = pl.ds(pl.multiple_of(c * 512, 512), 512)
            piece = times(act[r, :], weights[j % 2, 2, :, cols]).astype(jnp.bfloat16).astype(F32)
            gt = gates[r, :][:, j : j + 1]
            ct = cot[r, cols].astype(F32)
            routed[r, cols] += gt * piece
            dot = jnp.sum(piece * ct, axis=-1, keepdims=True)
            dot_sums[r, :] += jnp.where(lane == e * here + j, dot, 0.0)
            copy_buf[r, cols] = (gt * ct).astype(jnp.bfloat16)
            return 0
        lax.fori_loop(0, alltoks // 256 * 4, out, 0)
        free(0)
        turned[0] = across(eye[...], act[...]).astype(jnp.bfloat16)
        write(turned.at[0], act_t.at[j], 0)

    def ffn_back(rows, count, w):
        step = min(256, count)
        def pre(m, _):
            r = pl.ds(pl.multiple_of(m * step, step), step)
            ga = across(rows[r, :], w(2))
            g, u = gpre[r, :], upre[r, :]
            s = jax.nn.sigmoid(g)
            grad[0, r, :] = (ga * u * (s * (1.0 + g * (1.0 - s)))).astype(jnp.bfloat16)
            grad[1, r, :] = (ga * (g * s)).astype(jnp.bfloat16)
            return 0
        lax.fori_loop(0, count // step, pre, 0)

    def back_step(j):
        ffn_back(copy_buf, alltoks, lambda a: weights[j % 2, a])

    def rows_step(j):
        def out(k, _):
            m, c = k // 4, k % 4
            r = pl.ds(pl.multiple_of(m * 256, 256), 256)
            cols = pl.ds(pl.multiple_of(c * 512, 512), 512)
            back[r, cols] += (times(grad[0, r, :], weights[j % 2, 0, :, cols])
                              + times(grad[1, r, :], weights[j % 2, 1, :, cols]))
            return 0
        lax.fori_loop(0, alltoks // 256 * 4, out, 0)
        for q, dst in ((0, ggp_t), (1, gup_t)):
            free(1 + q)
            turned[1 + q] = across(eye[...], grad[q]).astype(jnp.bfloat16)
            write(turned.at[1 + q], dst.at[j], 1 + q)

    def shared_load(v):
        cs = []
        for a in range(3):
            c = pltpu.make_async_copy(sh_land[a].at[pl.ds(v * hid, hid)], weights.at[v, a], load_sem.at[v, a])
            c.start()
            cs.append(c)
        loads["s", v] = cs

    def shared(v):
        for c in loads.pop(("s", v)):
            c.wait()
        w = lambda a: weights[v, a]
        own = block(e)
        ffn_front(normed, toks, w)
        for c in range(4):
            ffn_own[:, c * 512 : (c + 1) * 512] += times(act[0:toks, :], weights[v, 2, :, c * 512 : (c + 1) * 512])
        sact_t[pl.ds(v * hid, hid), :] = across(eye[...], act[0:toks, :]).astype(jnp.bfloat16)
        copy_buf[0:toks, :] = cot[own, :]
        ffn_back(copy_buf, toks, w)
        for c in range(4):
            gn_own[:, c * 512 : (c + 1) * 512] += (
                times(grad[0, 0:toks, :], weights[v, 0, :, c * 512 : (c + 1) * 512])
                + times(grad[1, 0:toks, :], weights[v, 1, :, c * 512 : (c + 1) * 512]))
        gsg[:, v * hid : (v + 1) * hid] = grad[0, 0:toks, :]
        gsu[:, v * hid : (v + 1) * hid] = grad[1, 0:toks, :]

    def settle():
        for i in range(3):
            pltpu.make_async_copy(sh_ins[i], sh_stage.at[i], stage_sem.at[i]).wait()
            pltpu.make_async_copy(sh_stage.at[i], line_view(i, d, e), stage_sem.at[i]).start()
        for i in range(3):
            pltpu.make_async_copy(sh_stage.at[i], line_view(i, d, e), stage_sem.at[i]).wait()

    def fold_start(q):
        src, base = ((back, 2), (routed, 2 + 2 * n))[q]
        for k, p in enumerate(peers + [e]):
            remote(src.at[block(p), theirs], fold_other.at[q, block(p)], pair_send.at[base + k], pair_recv.at[base + k], near["c"])
            if q == 1:
                s = 2 + n + k
                remote(dot_sums.at[block(p)], few_other.at[block(p)], pair_send.at[s], pair_recv.at[s], near["c"])

    def got(view, k):
        remote(view, view, pair_send.at[k], pair_recv.at[k], near["c"], start=False).wait_recv()

    def fold_shared():
        base = 2 + 3 * n
        for q, src in enumerate((gn_own, ffn_own)):
            remote(src.at[:, theirs], fold_own.at[q], pair_send.at[base + q], pair_recv.at[base + q], near["c"])

    def fold_lines(q):
        src, base = ((back, 2), (routed, 2 + 2 * n))[q]
        for k, p in enumerate(peers):
            got(fold_other.at[q, block(p)], base + k)
            fold_out[q, k] = (src[block(p), mine] + fold_other[q, block(p), :]).astype(jnp.bfloat16)
            s = 2 * (n - 1) * q + k
            remote(fold_out.at[q, k], fold_in.at[q, k], zsend.at[s], zrecv.at[s], {EXPERT: p})
            if q == 1:
                got(few_other.at[block(p)], 2 + n + k)
                few_out[k] = (dot_sums[block(p), :] + few_other[block(p), :]).astype(jnp.bfloat16)
                s = n - 1 + k
                remote(few_out.at[k], few_in.at[k], zsend.at[s], zrecv.at[s], {EXPERT: p})

    def fold_end():
        for src, q, base in ((back, 0, 2), (routed, 1, 2 + 2 * n)):
            got(fold_other.at[q, block(e)], base + n - 1)
            got(fold_own.at[q], 2 + 3 * n + q)
            dst, own = ((gn2, gn_own), (ffn, ffn_own))[q]
            dst[:, mine] = (src[block(e), mine] + fold_other[q, block(e), :]) + (own[:, mine] + fold_own[q])
        got(few_other.at[block(e)], 2 + n + n - 1)
        few[...] = dot_sums[block(e), :] + few_other[block(e), :]
        for k in range(n - 1):
            s = n - 1 + k
            remote(few_in.at[k], few_in.at[k], zsend.at[s], zrecv.at[s], near["c"], start=False).wait_recv()
            few[...] += few_in[k].astype(F32)
        for q, dst in ((0, gn2), (1, ffn)):
            for k in range(n - 1):
                s = 2 * (n - 1) * q + k
                remote(fold_in.at[q, k], fold_in.at[q, k], zsend.at[s], zrecv.at[s], near["c"], start=False).wait_recv()
                dst[:, mine] += fold_in[q, k].astype(F32)
            s = 2 + 3 * n + 2 + q
            remote(dst.at[:, mine], dst.at[:, mine], pair_send.at[s], pair_recv.at[s], near["c"])
        for q, dst in ((0, gn2), (1, ffn)):
            got(dst.at[:, theirs], 2 + 3 * n + 2 + q)

    steps = {"join": join, "tok": tok_step, "tokend": tok_end, "gates": gates_step, "plane": plane_step, "line": line_step,
             "load": load, "load_down": load_down, "pre": pre_step, "front": front, "back": back_step, "rows": rows_step, "shared_load": shared_load, "shared": shared,
             "settle": settle, "fold_start": fold_start, "fold_shared": fold_shared, "fold_lines": fold_lines,
             "fold_end": fold_end}
    items = middle_items(n, here)
    for name, *args in [items[k] for k in order]:
        steps[name](*args)
    for k in list(waiting):
        free(k)
    for c, cond in sends:
        when(cond, c.wait_send)


def middle(part, inp, gain, router, named, cot, one, mixed, experts, shared_t, n, order, cid):
    bf, dma, vm = jnp.bfloat16, pltpu.SemaphoreType.DMA, pltpu.VMEM
    toks, width = inp.shape
    here, hid, cut = experts[0].shape
    al = n * toks
    sh = shared_t[0].shape[0]
    S = jax.ShapeDtypeStruct
    vmem, anyspace = pl.BlockSpec(memory_space=pltpu.VMEM), pl.BlockSpec(memory_space=pl.ANY)
    outs = [
        (S((toks, width), F32), vmem), (S((toks, width), bf), vmem), (S((al, width), bf), vmem),
        (S((toks, 128), F32), vmem), (S((toks, width), F32), vmem),
        (S((toks, width), F32), vmem), (S((here, hid, al), bf), anyspace), (S((here, hid, al), bf), anyspace),
        (S((here, hid, al), bf), anyspace), (S((al, 128), F32), vmem), (S((al, width), bf), vmem),
        (S((toks, 2 * hid), bf), vmem), (S((toks, 2 * hid), bf), vmem), (S((2 * hid, toks), bf), vmem),
        (S((width, toks), bf), vmem), (S((width, toks), bf), vmem), (S((mixed.shape[1], toks), bf), vmem),
    ] + [(S((here, hid, width), bf), anyspace)] * 3 + [(S((sh, width), bf), anyspace)] * 3
    scratch = [
        vm((toks, width), F32), vm((2, 3, hid, width), bf), vm((al, width), F32),
        vm((al, width), F32), vm((al, hid), F32), vm((al, hid), F32), vm((al, hid), bf), vm((2, al, hid), bf),
        vm((al, width), bf), vm((3, hid, al), bf), vm((hid, hid), bf), vm((3, sh, 128), bf), vm((al, 128), F32),
        vm((2, al, width // 2), F32), vm((2, toks, width // 2), F32), vm((2, n - 1, toks, width // 2), bf),
        vm((2, n - 1, toks, width // 2), bf), vm((al, 128), F32), vm((n - 1, toks, 128), bf),
        vm((n - 1, toks, 128), bf), vm((toks, width), F32), vm((toks, width), F32),
        dma((6 + 3 * n,)), dma((6 + 3 * n,)), dma((8 * (n - 1),)), dma((8 * (n - 1),)), dma((90,)), dma((90,)),
        dma((24 * (n - 1),)), dma((24 * (n - 1),)), dma((2, 12)), dma((4,)), dma((3,)),
        dma((3 * (n - 1),)), dma((3 * (n - 1),)),
    ]
    res = pl.pallas_call(
        functools.partial(middle_kernel, n, order),
        out_shape=[s for s, _ in outs], out_specs=[b for _, b in outs],
        in_specs=[vmem] * 8 + [anyspace] * 6,
        scratch_shapes=scratch,
        compiler_params=pltpu.CompilerParams(
            collective_id=cid, has_side_effects=True, vmem_limit_bytes=67043328),
    )(part, inp, gain, router, named, cot, one, mixed, *experts, *shared_t)
    return res[:17]


def rms_scale(vector):
    return lax.rsqrt(jnp.mean(vector * vector, axis=-1, keepdims=True) + epsilon)


def rope_tables(count, width):
    half_width = width // 2
    frequency = rope_base ** (-jnp.arange(half_width, dtype=jnp.float32) / half_width)
    angles = jnp.arange(count, dtype=jnp.float32)[:, None] * frequency[None, :]
    return (jnp.cos(angles)[:, None, :], jnp.sin(angles)[:, None, :])


def rotate(vector, cosine, sine_table):
    half_width = vector.shape[-1] // 2
    first_half = vector[..., :half_width]
    second_half = vector[..., half_width:]
    return jnp.concatenate(
        [
            first_half * cosine - second_half * sine_table,
            first_half * sine_table + second_half * cosine,
        ],
        axis=-1,
    )


def unrotate(vector, cosine, sine_table):
    half_width = vector.shape[-1] // 2
    first_half = vector[..., :half_width]
    second_half = vector[..., half_width:]
    return jnp.concatenate(
        [
            first_half * cosine + second_half * sine_table,
            second_half * cosine - first_half * sine_table,
        ],
        axis=-1,
    )


def dots(left, right, *dims):
    return lax.dot_general(left, right, dims, preferred_element_type=F32)


def silu_parts(before):
    sigmoid_val = jax.nn.sigmoid(before)
    return (before * sigmoid_val, sigmoid_val * (1.0 + before * (1.0 - sigmoid_val)))


def masked_scores(query_rot, key_rot, allowed):
    scores = dots(query_rot, key_rot, ((2,), (2,)), ((1,), (1,))) / math.sqrt(query_rot.shape[-1])
    return jnp.where(allowed[None], scores, masked_score)


def turn(array, by, axis):
    return lax.dynamic_slice_in_dim(
        jnp.concatenate([array, array], axis=axis), by, array.shape[axis], axis=axis)


def plain_middle(attn_part, input_f, gain_two, router_rows, named_all, grads_all, cotangent,
                 expert_weights, full_sgate, full_sup, full_sdown):
    here = lax.axis_index(EXPERT)
    local_gate, local_up, local_down = expert_weights
    experts_here = local_gate.shape[0]
    hidden_one = input_f + lax.psum(attn_part, TENSOR)
    normed_two = (hidden_one * rms_scale(hidden_one) * gain_two).astype(BF)
    rows_all = lax.all_gather(normed_two, EXPERT, axis=0, tiled=True)
    probs_all = jax.nn.softmax(dots(rows_all, router_rows, ((1,), (1,)), ((), ())), axis=-1)
    gates_here = lax.dynamic_slice_in_dim(
        probs_all * named_all, here * experts_here, experts_here, axis=1)
    gate_pre = dots(local_gate, rows_all, ((2,), (1,)), ((), ()))
    up_pre = dots(local_up, rows_all, ((2,), (1,)), ((), ()))
    silu_gate, slope_gate = silu_parts(gate_pre)
    act_t = (silu_gate * up_pre).astype(BF)
    part_rows = dots(act_t, local_down, ((1,), (1,)), ((0,), (0,))).astype(BF).astype(F32)
    routed = sum(gates_here[:, j : j + 1] * part_rows[j] for j in range(experts_here))
    grads_wide = grads_all.astype(F32)
    owner_grads = (jnp.transpose(gates_here)[:, :, None] * grads_wide[None]).astype(BF)
    gate_dots = jnp.sum(part_rows * grads_wide[None], axis=-1)
    dots_wide = lax.dynamic_update_slice(
        jnp.zeros_like(probs_all), jnp.transpose(gate_dots), (0, here * experts_here))
    grad_act = dots(local_down, owner_grads, ((2,), (2,)), ((0,), (0,)))
    ggp_t = (grad_act * up_pre * slope_gate).astype(BF)
    gup_t = (grad_act * silu_gate).astype(BF)
    grad_rows = dots(ggp_t, local_gate, ((0, 1), (0, 1)), ((), ()))
    grad_rows = grad_rows + dots(gup_t, local_up, ((0, 1), (0, 1)), ((), ()))
    shared_gpre = jnp.dot(normed_two, full_sgate, preferred_element_type=F32)
    shared_upre = jnp.dot(normed_two, full_sup, preferred_element_type=F32)
    silu_shared, slope_shared = silu_parts(shared_gpre)
    shared_act = (silu_shared * shared_upre).astype(BF)
    shared_part = jnp.dot(shared_act, full_sdown, preferred_element_type=F32)
    grad_sact = dots(cotangent, full_sdown, ((1,), (1,)), ((), ()))
    grad_sgate = (grad_sact * shared_upre * slope_shared).astype(BF)
    grad_sup = (grad_sact * silu_shared).astype(BF)
    own_rows = dots(grad_sgate, full_sgate, ((1,), (1,)), ((), ()))
    own_rows = own_rows + dots(grad_sup, full_sup, ((1,), (1,)), ((), ()))
    back = [lax.psum_scatter(v, EXPERT, scatter_dimension=0, tiled=True)
            for v in (grad_rows, routed, dots_wide)]
    grad_normed_two = lax.psum(back[0] + own_rows, TENSOR)
    ffn_total = lax.psum(back[1] + shared_part, TENSOR)
    dots_sum = lax.psum(back[2], TENSOR)
    router_probs = lax.dynamic_slice_in_dim(
        probs_all, here * normed_two.shape[0], normed_two.shape[0], axis=0)
    return (hidden_one, normed_two, rows_all, router_probs, dots_sum, grad_normed_two, ffn_total,
            act_t, ggp_t, gup_t, owner_grads, grad_sgate, grad_sup, shared_act.T)


def plain_scatter(dense, lefts, rights, extra, exp_left, rows_all, owner_grads):
    sums = []
    for k, ((kind, _), left, right) in enumerate(zip(dense, lefts, rights)):
        part = jnp.dot(left, right, preferred_element_type=F32)
        if k == len(dense) - 1:
            part = part + extra
        dim = 0 if kind == "rows" else 1
        sums.append(lax.psum_scatter(part, BOTH, scatter_dimension=dim, tiled=True))
    for left, right in zip(exp_left, (rows_all, rows_all, owner_grads)):
        dims = (((2,), (0,)), ((), ())) if right.ndim == 2 else (((2,), (1,)), ((0,), (0,)))
        part = dots(left, right, *dims).astype(BF)
        sums.append(lax.psum_scatter(part, DP, scatter_dimension=2, tiled=True).astype(F32))
    return sums


def plain_backward(
    dense, cotangent, block_input, named, router_probs, dots_sum, grad_normed_two, router_rows,
    hidden_one, gain_two, gain_one, full_query, full_key, full_value, full_output, query_rot, key_rot,
    value_rows, allowed, log_total, cosine, sine_table, one_t, two_t, mixed_t, shared_act_t,
    grad_sgate, grad_sup, normed_two, ggp_t, gup_t, act_t, rows_all, owner_grads,
):
    total_experts = router_rows.shape[0]
    seq_len, heads_here = query_rot.shape[:2]
    input_f = block_input.astype(F32)
    scale_one = rms_scale(input_f)
    scale_two = rms_scale(hidden_one)
    grad_out = cotangent.astype(F32)
    grad_rprobs = jnp.where(named, dots_sum, 0.0)
    grad_logits = (
        router_probs * (grad_rprobs - jnp.sum(grad_rprobs * router_probs, axis=-1, keepdims=True))
    ).astype(BF)
    grad_normed_two = grad_normed_two + dots(grad_logits, router_rows, ((1,), (0,)), ((), ()))
    ffn_gain_full = jnp.sum(grad_normed_two * hidden_one * scale_two, axis=0)
    weighted_two = grad_normed_two * gain_two
    cube_two = scale_two * scale_two * scale_two
    grad_hidden = (
        grad_out
        + scale_two * weighted_two
        - hidden_one * cube_two * jnp.mean(hidden_one * weighted_two, axis=-1, keepdims=True)
    )
    grad_attn = grad_hidden.astype(BF)
    grad_mixed = (
        dots(grad_attn, full_output, ((1,), (1,)), ((), ()))
        .astype(BF)
        .reshape(seq_len, heads_here, HD)
    )
    prob_again = jnp.exp(masked_scores(query_rot, key_rot, allowed) - log_total)
    grad_probs = dots(grad_mixed, value_rows, ((2,), (2,)), ((1,), (1,)))
    grad_scores = (
        prob_again * (grad_probs - jnp.sum(prob_again * grad_probs, axis=-1, keepdims=True))
    ).astype(BF)
    value_grad_rows = (
        jnp.transpose(dots(prob_again.astype(BF), grad_mixed, ((1,), (0,)), ((0,), (1,))), (1, 0, 2))
        .astype(BF)
        .reshape(seq_len, heads_here * HD)
    )
    inverse_root = 1.0 / math.sqrt(HD)
    grad_qrot = (
        jnp.transpose(dots(grad_scores, key_rot, ((2,), (0,)), ((0,), (1,))), (1, 0, 2))
        * inverse_root
    )
    grad_krot = (
        jnp.transpose(dots(grad_scores, query_rot, ((1,), (0,)), ((0,), (1,))), (1, 0, 2))
        * inverse_root
    )
    grad_qpre = (
        unrotate(grad_qrot, cosine, sine_table).astype(BF).reshape(seq_len, heads_here * HD)
    )
    grad_kpre = (
        unrotate(grad_krot, cosine, sine_table).astype(BF).reshape(seq_len, heads_here * HD)
    )
    grad_normed_one = dots(grad_qpre, full_query, ((1,), (1,)), ((), ()))
    grad_normed_one = grad_normed_one + dots(grad_kpre, full_key, ((1,), (1,)), ((), ()))
    grad_normed_one = grad_normed_one + dots(value_grad_rows, full_value, ((1,), (1,)), ((), ()))
    grad_normed_one = lax.psum(grad_normed_one, TENSOR)
    attn_gain_full = jnp.sum(grad_normed_one * input_f * scale_one, axis=0)
    weighted_one = grad_normed_one * gain_one
    cube_one = scale_one * scale_one * scale_one
    input_grad = (
        grad_hidden
        + scale_one * weighted_one
        - input_f * cube_one * jnp.mean(input_f * weighted_one, axis=-1, keepdims=True)
    )
    room = total_experts + 2 + (-(total_experts + 2) % 64)
    logits_t = jnp.pad(grad_logits.T, ((0, room - total_experts), (0, 0)))
    extra = jnp.concatenate([
        jnp.zeros((total_experts, D), F32), attn_gain_full[None], ffn_gain_full[None],
        jnp.zeros((room - total_experts - 2, D), F32)])
    lefts = (one_t, one_t, one_t, mixed_t, two_t, two_t, shared_act_t, logits_t)
    rights = (grad_qpre, grad_kpre, value_grad_rows, grad_attn, grad_sgate, grad_sup, cotangent, normed_two)
    exp_left = (ggp_t, gup_t, act_t)
    sums = plain_scatter(dense, lefts, rights, extra, exp_left, rows_all, owner_grads)
    return sums, input_grad


def body(
    block_input,
    attn_gain,
    query_weight,
    key_weight,
    value_weight,
    output_weight,
    ffn_gain,
    router_weight,
    expert_gate,
    expert_up,
    expert_down,
    shared_gate,
    shared_up,
    shared_down,
    segments,
    routes,
    cotangent,
):
    seq_len = block_input.shape[0]
    total_experts = router_weight.shape[1]
    owners, here = lax.axis_size(EXPERT), lax.axis_index(EXPERT)
    kernels = (output_weight.shape[1] % 128 == 0 and lax.axis_size(DP) == 4
               and total_experts <= 128 and seq_len == 128)
    expert_ids = jnp.arange(total_experts, dtype=jnp.int32)
    named = jnp.any(routes[:, :, None] == expert_ids[None, None, :], axis=1)
    small = jnp.concatenate([router_weight, attn_gain[:, None], ffn_gain[:, None]], axis=1).T
    flip_gate, flip_up = jnp.swapaxes(expert_gate, 1, 2), jnp.swapaxes(expert_up, 1, 2)
    named_low = named.astype(BF)
    if kernels:
        small = jnp.pad(small, ((0, -small.shape[0] % 32), (0, 0)))
        named_low = jnp.pad(named_low, ((0, 0), (0, 256 - total_experts)))
        arrays = (query_weight, key_weight, value_weight, output_weight, small, named_low)
        forms = ("rows",) * 3 + ("cols", "cols", "tokens")
        firsts = ("z",) * 3 + ("xy", "z", "xy")
        (full_query, full_key, full_value, full_output, full_small, named_all, sgate_t, sup_t) = gather(
            arrays, forms, firsts, owners, gather_starts, (shared_gate, shared_up))
    else:
        full_small = lax.all_gather(small, BOTH, axis=1, tiled=True)
        full_query = lax.all_gather(query_weight, BOTH, axis=0, tiled=True)
        full_key = lax.all_gather(key_weight, BOTH, axis=0, tiled=True)
        full_value = lax.all_gather(value_weight, BOTH, axis=0, tiled=True)
        full_output = lax.all_gather(output_weight, BOTH, axis=1, tiled=True)
        named_all = lax.all_gather(named_low, EXPERT, axis=0, tiled=True)
    named_all = named_all[:, :total_experts]
    router_rows = full_small[:total_experts]
    gain_one = full_small[total_experts].astype(F32)
    gain_two = full_small[total_experts + 1].astype(F32)
    heads_here = full_query.shape[1] // HD
    input_f = block_input.astype(F32)
    scale_one = rms_scale(input_f)
    normed_one = (input_f * scale_one * gain_one).astype(BF)
    cosine, sine_table = rope_tables(seq_len, HD)
    query_pre = jnp.dot(normed_one, full_query, preferred_element_type=F32).reshape(
        seq_len, heads_here, HD
    )
    key_pre = jnp.dot(normed_one, full_key, preferred_element_type=F32).reshape(
        seq_len, heads_here, HD
    )
    query_rot = rotate(query_pre, cosine, sine_table).astype(BF)
    key_rot = rotate(key_pre, cosine, sine_table).astype(BF)
    value_rows = (
        jnp.dot(normed_one, full_value, preferred_element_type=F32)
        .astype(BF)
        .reshape(seq_len, heads_here, HD)
    )
    position = jnp.arange(seq_len)
    segment_row = segments[0]
    allowed = (position[:, None] >= position[None, :]) & (
        segment_row[:, None] == segment_row[None, :]
    )
    scores = masked_scores(query_rot, key_rot, allowed)
    top_score = jnp.max(scores, axis=-1, keepdims=True)
    shifted = jnp.exp(scores - top_score)
    row_total = jnp.sum(shifted, axis=-1, keepdims=True)
    log_total = top_score + jnp.log(row_total)
    prob_low = (shifted / row_total).astype(BF)
    mixed_rows = (
        jnp.transpose(dots(prob_low, value_rows, ((2,), (0,)), ((0,), (1,))), (1, 0, 2))
        .astype(BF)
        .reshape(seq_len, heads_here * HD)
    )
    attn_part = jnp.dot(mixed_rows, full_output, preferred_element_type=F32)
    experts = (flip_gate, flip_up, expert_down)
    if kernels:
        first = here * expert_gate.shape[0]
        router_pad = jnp.pad(turn(router_rows, first, 0), ((0, 128 - total_experts), (0, 0)))
        named_pad = jnp.pad(turn(named_all, first, 1), ((0, 0), (0, 128 - total_experts)))
        (hidden_one, normed_two, rows_all, dots_sum, back, ffn_total, act_t, ggp_t, gup_t, gates, cot_all,
         grad_sgate, grad_sup, shared_act_t, one_t, two_t, mixed_t) = middle(
            attn_part, block_input, gain_two[None], router_pad, named_pad, cotangent, normed_one,
            mixed_rows, experts, (sgate_t, sup_t, shared_down), owners, middle_order, 2)
    else:
        (hidden_one, normed_two, rows_all, router_probs, dots_sum, grad_normed_two, ffn_total, act_t, ggp_t, gup_t,
         owner_grads, grad_sgate, grad_sup, shared_act_t) = plain_middle(
            attn_part, input_f, gain_two, router_rows, named_all.astype(F32),
            lax.all_gather(cotangent, EXPERT, axis=0, tiled=True), cotangent,
            tuple(lax.all_gather(w, DP, axis=2, tiled=True) for w in experts),
            lax.all_gather(shared_gate, BOTH, axis=0, tiled=True),
            lax.all_gather(shared_up, BOTH, axis=0, tiled=True),
            lax.all_gather(shared_down, BOTH, axis=1, tiled=True))
        one_t, two_t, mixed_t = normed_one.T, normed_two.T, mixed_rows.T
    block_output = (hidden_one + ffn_total).astype(BF)
    dense = ((("rows", "z"),) + (("rows", "p"),) * 2
             + (("cols", "p"),) + (("rows", "z"),) * 2 + (("cols", "z"),) * 2)
    if kernels:
        pair = lambda first, last: jnp.concatenate([first, last], axis=-1)[:, 0]
        flat = lambda v: v.reshape(seq_len, heads_here * HD)
        given = dict(
            one_t=one_t, mixed_t=mixed_t, two_t=two_t, sact_t=shared_act_t, gsg=grad_sgate, gsu=grad_sup,
            cot=cotangent, normed=normed_two, ggp=ggp_t, gup=gup_t, act=act_t, rows_all=rows_all,
            cot_all=cot_all, gates=gates, hidden=hidden_one, back=back, few=dots_sum,
            named=jnp.pad(named.astype(F32), ((0, 0), (0, 128 - total_experts))),
            gain_two=gain_two[None], gain_one=gain_one[None], inp=block_input,
            q=flat(query_rot), k=flat(key_rot), v=flat(value_rows), cos=pair(cosine, cosine),
            sin=pair(sine_table, -sine_table), mask=allowed.astype(F32),
            router=jnp.pad(router_rows, ((0, 128 - total_experts), (0, 0))))
        *sums, input_grad = scatter(
            dense, given, (full_output, full_query, full_key, full_value), total_experts, owners,
            scatter_order, 1)
    else:
        sums, input_grad = plain_backward(
            dense, cotangent, block_input, named, router_probs, dots_sum, grad_normed_two, router_rows,
            hidden_one, gain_two, gain_one, full_query, full_key, full_value, full_output, query_rot, key_rot,
            value_rows, allowed, log_total, cosine, sine_table, one_t, two_t, mixed_t, shared_act_t,
            grad_sgate, grad_sup, normed_two, ggp_t, gup_t, act_t, rows_all, owner_grads)
    (query_grad, key_grad, value_grad, output_grad, shared_gate_grad, shared_up_grad,
     shared_down_grad, small_grad, expert_gate_grad, expert_up_grad, expert_down_grad) = sums
    return (
        block_output,
        input_grad,
        small_grad[total_experts],
        query_grad,
        key_grad,
        value_grad,
        output_grad,
        small_grad[total_experts + 1],
        small_grad[:total_experts].T,
        jnp.swapaxes(expert_gate_grad, 1, 2),
        jnp.swapaxes(expert_up_grad, 1, 2),
        expert_down_grad,
        shared_gate_grad,
        shared_up_grad,
        shared_down_grad,
    )


def solution(mesh):
    return jax.shard_map(
        body,
        mesh=mesh,
        in_specs=(
            P((DP, EXPERT), None),
            P((DP, EXPERT)),
            P((DP, EXPERT), TENSOR),
            P((DP, EXPERT), TENSOR),
            P((DP, EXPERT), TENSOR),
            P(TENSOR, (DP, EXPERT)),
            P((DP, EXPERT)),
            P((DP, EXPERT), None),
            P(EXPERT, DP, TENSOR),
            P(EXPERT, DP, TENSOR),
            P(EXPERT, TENSOR, DP),
            P((DP, EXPERT), TENSOR),
            P((DP, EXPERT), TENSOR),
            P(TENSOR, (DP, EXPERT)),
            P((DP, EXPERT), None),
            P((DP, EXPERT), None),
            P((DP, EXPERT), None),
        ),
        out_specs=(
            P((DP, EXPERT), None),
            P((DP, EXPERT), None),
            P((DP, EXPERT)),
            P((DP, EXPERT), TENSOR),
            P((DP, EXPERT), TENSOR),
            P((DP, EXPERT), TENSOR),
            P(TENSOR, (DP, EXPERT)),
            P((DP, EXPERT)),
            P((DP, EXPERT), None),
            P(EXPERT, DP, TENSOR),
            P(EXPERT, DP, TENSOR),
            P(EXPERT, TENSOR, DP),
            P((DP, EXPERT), TENSOR),
            P((DP, EXPERT), TENSOR),
            P(TENSOR, (DP, EXPERT)),
        ),
        check_vma=False,
    )
```
